256 devices in a mesh: grp: 32 (over z, y), mem: 8 (over x, core).
Axes of the slice: x: 4, y: 4, z: 8, core: 2. Of those that a mesh axis runs over, the one named last changes fastest.
Arguments:
- potential: float32 [512, 512, 512], P(('grp', 'mem')), may hold values from -6 to 6
- source: float32 [512, 512, 512], P(('grp', 'mem')), may hold values from -20 to 20
- side_faces: float32 [256, 4, 256], P(('grp', 'mem')), may hold values from -6 to 6
- end_faces: float32 [2, 256, 256], replicated, may hold values from -6 to 6
Outputs:
- corrected: float32 [512, 512, 512], P(('grp', 'mem'))
- correction: float32 [256, 256, 256], P(('grp', 'mem'))
The draws below stay inside these ranges and needn't reach their ends.
All inputs are finite; a program needn't handle non-finite values.
Results may differ from the reference program's by a relative error of at most 0.00002.
Values sent between devices are 32-bit elements; how exact they have to be, the bound alone decides.
A program may use at most 64 MiB of HBM per device.

```python
import jax
import jax.numpy as jnp
from jax import lax

NF = 512
SWEEPS = 8
NC = 256
NZ = 512
NZC = 256


def draw_source(key, part):
    first_key = jax.random.fold_in(jax.random.fold_in(key, 11), 0)
    values = jax.random.normal(first_key, (NZ, NF, NF), jnp.float32)
    return jnp.clip(values, -20.0, 20.0)


def steps_of(own_key, extent, pieces, least, top_value):
    gain = 1.0
    for axis_at, blocks in pieces:
        steps = jax.random.uniform(jax.random.fold_in(jax.random.fold_in(own_key, 6), axis_at), (blocks,), jnp.float32, least / len(pieces), top_value / len(pieces))
        gain = gain * jnp.repeat(jnp.exp(steps), extent[axis_at] // blocks).reshape((-1,) + (1,) * (len(extent) - 1 - axis_at))
    return gain


def gaussian(rng, shape, scale, most, pieces=(), held_as=jnp.bfloat16):
    array = jax.random.normal(rng, shape, jnp.float32) * scale
    if len(pieces) > 0:
        array = steps_of(rng, shape, pieces, -0.22, 0.18) * array
    return jnp.clip(array, min=-most, max=most).astype(held_as)


def setup_inputs(seed: int = 0) -> dict:
    streams_of = jax.random.split(jax.random.key(seed), 5)
    return {
        "potential": gaussian(streams_of[0], (NZ, NF, NF), 1.0, 6.0, ((0, 256),), jnp.float32),
        "source": draw_source(jax.random.fold_in(streams_of[4], 71), 0),
        "side_faces": gaussian(streams_of[2], (NZC, 4, NC), 1.0, 6.0, ((0, 256),), jnp.float32),
        "end_faces": gaussian(streams_of[3], (2, NC, NC), 1.0, 6.0, (), jnp.float32),
    }


def fine_operator(padded):
    center = padded[1:-1, 1:-1, 1:-1]
    beside = padded[2:, 1:-1, 1:-1] + padded[:-2, 1:-1, 1:-1]
    beside = beside + padded[1:-1, 2:, 1:-1] + padded[1:-1, :-2, 1:-1]
    beside = beside + padded[1:-1, 1:-1, 2:] + padded[1:-1, 1:-1, :-2]
    return 4.0 * (6.0 * center - beside)


def restrict_axis(values, direction, before):
    even_part = lax.slice_in_dim(values, 0, None, 2, direction)
    odd_part = lax.slice_in_dim(values, 1, None, 2, direction)
    length = odd_part.shape[direction]
    earlier = jnp.concatenate([before, lax.slice_in_dim(odd_part, 0, length - 1, 1, direction)], direction)
    return 0.5 * even_part + 0.25 * (odd_part + earlier)


def zero_slice(values, direction):
    return jnp.zeros_like(lax.slice_in_dim(values, 0, 1, 1, direction))


def prolong_axis(values, direction, beyond):
    length = values.shape[direction]
    following = jnp.concatenate([lax.slice_in_dim(values, 1, length, 1, direction), beyond], direction)
    middle = 0.5 * (values + following)
    paired = jnp.stack([values, middle], direction + 1)
    new_shape = list(values.shape)
    new_shape[direction] = 2 * length
    return paired.reshape(new_shape)


def last_slice(values, direction):
    length = values.shape[direction]
    return lax.slice_in_dim(values, length - 1, length, 1, direction)


def side_sum(values, side_faces):
    front_face = side_faces[:, 0:1, :]
    back_face = side_faces[:, 1:2, :]
    left_face = side_faces[:, 2, :][:, :, None]
    right_face = side_faces[:, 3, :][:, :, None]
    front_cells = jnp.concatenate([front_face, values[:, :-1, :]], 1)
    back_cells = jnp.concatenate([values[:, 1:, :], back_face], 1)
    left_cells = jnp.concatenate([left_face, values[:, :, :-1]], 2)
    right_cells = jnp.concatenate([values[:, :, 1:], right_face], 2)
    return (front_cells + back_cells) + (left_cells + right_cells)


def smooth_red_black(forcing, side_faces, end_faces, offset, at_first, at_last, neighbour_fn):
    planes = forcing.shape[0]
    depth_ids = offset + lax.broadcasted_iota(jnp.int32, forcing.shape, 0)
    row_ids = lax.broadcasted_iota(jnp.int32, forcing.shape, 1)
    col_ids = lax.broadcasted_iota(jnp.int32, forcing.shape, 2)
    parity = (depth_ids + row_ids + col_ids) % 2

    def one_sweep(counter, values):
        for colour in (0, 1):
            padded = neighbour_fn(values)
            lower_face = jnp.where(at_first, end_faces[0], padded[0])
            upper_face = jnp.where(at_last, end_faces[1], padded[-1])
            under_plane = jnp.concatenate([lower_face[None], padded[1:planes]], 0)
            over_plane = jnp.concatenate([padded[2:planes + 1], upper_face[None]], 0)
            neighbours = (under_plane + over_plane) + side_sum(values, side_faces)
            values = jnp.where(parity == colour, (forcing + neighbours) / 6.0, values)
        return values

    return lax.fori_loop(0, SWEEPS, one_sweep, jnp.zeros_like(forcing))


def pad_depth(values):
    return jnp.pad(values, ((1, 1), (0, 0), (0, 0)))


def reference(potential, source, side_faces, end_faces):
    residual = source - fine_operator(jnp.pad(potential, 1))
    forcing = residual
    for direction in (0, 1, 2):
        forcing = restrict_axis(forcing, direction, zero_slice(forcing, direction))
    correction = smooth_red_black(forcing, side_faces, end_faces, 0, True, True, pad_depth)
    refined = correction
    for direction in (0, 1, 2):
        refined = prolong_axis(refined, direction, last_slice(refined, direction))
    return potential + refined, correction
```

```python
import functools

import jax
import jax.numpy as jnp
from jax import lax
from jax.experimental import pallas as pl
from jax.experimental.pallas import tpu as pltpu
from jax.sharding import PartitionSpec as P

F32 = jnp.float32
BF16 = jnp.bfloat16
MESH = pl.DeviceIdType.MESH

NF = 512
NC = 256
MEM = 8
ROWS = NC // MEM
HALO = 8
SLOTS = MEM + 2 * HALO
FROWS = ROWS + 2 * HALO
VROWS = FROWS + 16
CHUNKS = 4
CROWS = NC // CHUNKS
FINE = 2 * CROWS


def iota(shape, dim):
    return lax.broadcasted_iota(jnp.int32, shape, dim)


def split3(x):
    high = x.astype(BF16)
    rest = x - high.astype(F32)
    middle = rest.astype(BF16)
    low = (rest - middle.astype(F32)).astype(BF16)
    return high, middle, low


def dot_exact(x, weights):
    rows = x.shape[0]
    parts = jnp.concatenate(split3(x), axis=0)
    out = jnp.dot(parts, weights, preferred_element_type=F32)
    return out[:rows] + (out[rows : 2 * rows] + out[2 * rows :])


def coarse_column(shape, dim):
    n = iota(shape, dim)
    return jnp.where(n < NC // 2, 2 * n, 2 * n - (NC - 1))


def restrict_kernel(p_hbm, s_hbm, side, end_hbm, out, pb, sb, eb, w_rc, w_lr, w_perm, sems, end_sem):
    groups = lax.axis_size("grp")
    device = lax.axis_index("grp") * MEM + lax.axis_index("mem")
    is_first = device == 0
    is_last = device == groups * MEM - 1

    copies = []
    for c in range(CHUNKS):
        row = []
        for t in range(4):
            for a, (src, dst) in enumerate(((p_hbm, pb), (s_hbm, sb))):
                row.append(
                    pltpu.make_async_copy(
                        src.at[:, pl.ds(FINE * c, FINE), pl.ds(128 * t, 128)],
                        dst.at[:, t, pl.ds(8 + FINE * c, FINE), :],
                        sems.at[c, t, a],
                    )
                )
        copies.append(row)
    for row in copies:
        for copy in row:
            copy.start()
    end_copy = pltpu.make_async_copy(
        end_hbm.at[jnp.where(is_last, 1, 0)], eb, end_sem
    )
    at_end = jnp.logical_or(is_first, is_last)

    @pl.when(at_end)
    def _():
        end_copy.start()

    zeros = jnp.zeros((2, 4, 8, 128), F32)
    pb[:, :, 0:8, :] = zeros
    pb[:, :, 8 + NF : 16 + NF, :] = zeros
    sb[:, :, 0:8, :] = zeros

    column = coarse_column((NF, NC), 1)
    step = jnp.abs(iota((NF, NC), 0) - 2 * column)
    w_rc[...] = jnp.where(step == 0, 0.5, jnp.where(step == 1, 0.25, 0.0)).astype(BF16)
    near = jnp.where(step == 0, jnp.where(column == 0, 0.25, 0.5), 0.5)
    w_lr[...] = jnp.where(step <= 1, near, jnp.where(step == 2, 0.25, 0.0)).astype(BF16)
    square = coarse_column((NC, NC), 1)
    w_perm[...] = jnp.where(iota((NC, NC), 0) == square, 1.0, 0.0).astype(BF16)

    front = dot_exact(jnp.broadcast_to(side[0, 0:1, :], (8, NC)), w_perm[...])[0:1]
    back = dot_exact(jnp.broadcast_to(side[0, 1:2, :], (8, NC)), w_perm[...])[0:1]
    own_weight = jnp.where(is_first, 0.25, 0.5)

    def store(field, c, value):
        row = CROWS * c + iota((CROWS, 128), 0)
        even = lax.rem(row + device + (field > 0), 2) == 0
        left, right = value[:, :128], value[:, 128:]
        red = jnp.where(even, left, right)
        black = jnp.where(even, right, left)
        for b in range(CROWS // ROWS):
            q = c * (CROWS // ROWS) + b
            out[field, q, 0] = red[ROWS * b : ROWS * (b + 1)]
            out[field, q, 1] = black[ROWS * b : ROWS * (b + 1)]

    for copy in copies[0]:
        copy.wait()
    for c in range(CHUNKS):
        if c + 1 < CHUNKS:
            for copy in copies[c + 1]:
                copy.wait()
        fields = [[], [], [], [], []]
        for t in range(4):

            def load(ref, plane, shift):
                return ref[plane, t, pl.ds(8 + FINE * c + shift, CROWS, stride=2), :]

            a, b = [], []
            for plane in (0, 1):
                p_before, p_here, p_after = (load(pb, plane, k) for k in (-1, 0, 1))
                outer = load(pb, plane, -2) + load(pb, plane, 2)
                odd = p_before + p_after
                s_part = 0.5 * load(sb, plane, 0) + 0.25 * (load(sb, plane, -1) + load(sb, plane, 1))
                value = s_part + (outer - 4.0 * odd - 10.0 * p_here)
                if c == 0:
                    value = value - jnp.where(iota(value.shape, 0) == 0, p_here, 0.0)
                a.append(value)
                b.append(2.0 * p_here + odd)
            up = 0.25 * a[1] + 0.5 * b[1]
            fields[0].append(0.5 * a[0] + up + own_weight * b[0])
            fields[1].append(up + 0.25 * b[0])
            fields[2].append(0.25 * b[0])
            fields[3].append(0.5 * b[0] + 0.25 * b[1])
            fields[4].append(0.25 * b[1])
        wide = [jnp.concatenate(f, axis=1) for f in fields]
        plain = dot_exact(jnp.concatenate(wide[:3], axis=0), w_rc[...])
        cross = dot_exact(jnp.concatenate(wide[3:], axis=0), w_lr[...])
        local = plain[:CROWS] + cross[:CROWS]
        above = plain[CROWS : 2 * CROWS] + cross[CROWS:]
        below = plain[2 * CROWS :]
        row = iota((CROWS, NC), 0)
        lane = iota((CROWS, NC), 1)
        diagonal = lane == row + CROWS * c
        left = jnp.sum(jnp.where(diagonal, side[0, 2:3, :], 0.0), axis=1, keepdims=True)
        right = jnp.sum(jnp.where(diagonal, side[0, 3:4, :], 0.0), axis=1, keepdims=True)
        local = local + jnp.where(lane == 0, left, jnp.where(lane == NC - 1, right, 0.0))
        if c == 0:
            local = local + jnp.where(row == 0, front, 0.0)
        if c == CHUNKS - 1:
            local = local + jnp.where(row == CROWS - 1, back, 0.0)
        store(0, c, local)
        store(1, c, above)
        store(2, c, below)

    @pl.when(at_end)
    def _():
        end_copy.wait()
        for c in range(CHUNKS):
            rows = pl.ds(CROWS * c, CROWS)
            face = dot_exact(eb[rows, :], w_perm[...])
            row = CROWS * c + iota((CROWS, 128), 0)
            even = lax.rem(row + device, 2) == 0
            red = jnp.where(even, face[:, :128], face[:, 128:])
            black = jnp.where(even, face[:, 128:], face[:, :128])
            for b in range(CROWS // ROWS):
                q = c * (CROWS // ROWS) + b
                out[0, q, 0] = out[0, q, 0] + red[ROWS * b : ROWS * (b + 1)]
                out[0, q, 1] = out[0, q, 1] + black[ROWS * b : ROWS * (b + 1)]


def restrict(potential, source, side_faces, end_faces):
    anyspace = pl.BlockSpec(memory_space=pl.ANY)
    return pl.pallas_call(
        restrict_kernel,
        out_shape=jax.ShapeDtypeStruct((3, MEM, 2, ROWS, 128), F32),
        in_specs=[anyspace, anyspace, pl.BlockSpec(memory_space=pltpu.VMEM), anyspace],
        out_specs=pl.BlockSpec(memory_space=pltpu.VMEM),
        scratch_shapes=[
            pltpu.VMEM((2, 4, NF + 16, 128), F32),
            pltpu.VMEM((2, 4, NF + 16, 128), F32),
            pltpu.VMEM((NC, NC), F32),
            pltpu.VMEM((NF, NC), BF16),
            pltpu.VMEM((NF, NC), BF16),
            pltpu.VMEM((NC, NC), BF16),
            pltpu.SemaphoreType.DMA((CHUNKS, 4, 2)),
            pltpu.SemaphoreType.DMA,
        ],
        name="restrict",
    )(potential, source, side_faces, end_faces)


DIRECTIONS = tuple((dg, dm) for dg in (-1, 0, 1) for dm in (-1, 0, 1) if (dg, dm) != (0, 0))


def smooth_kernel(
    fields, e_out, partner, summed, fb, xb, vr, vk, vk2,
    partner_sems, f_send, f_recv, x_send, x_recv, h_send, h_recv, b_send, b_recv, e_send, e_recv, e_local,
):
    groups = lax.axis_size("grp")
    g = lax.axis_index("grp")
    m = lax.axis_index("mem")

    def remote(src, dst, send, recv, tg, tm):
        return pltpu.make_async_remote_copy(
            src_ref=src, dst_ref=dst, send_sem=send, recv_sem=recv,
            device_id={"grp": tg, "mem": tm}, device_id_type=MESH,
        )

    vr[...] = jnp.zeros_like(vr)
    vk[...] = jnp.zeros_like(vk)
    vk2[...] = jnp.zeros_like(vk2)
    fb[...] = jnp.zeros_like(fb)
    xb[...] = jnp.zeros_like(xb)

    barrier = pltpu.get_barrier_semaphore()
    for dg in (-1, 0, 1):
        exists = jnp.logical_and(g + dg >= 0, g + dg < groups)

        @pl.when(exists)
        def _():
            for i in range(1 if dg == 0 else 0, MEM):
                pl.semaphore_signal(
                    barrier, inc=1,
                    device_id={"grp": g + dg, "mem": lax.rem(m + i, MEM)}, device_id_type=MESH,
                )
    count = (MEM - 1) + jnp.where(g > 0, MEM, 0) + jnp.where(g < groups - 1, MEM, 0)
    pl.semaphore_wait(barrier, count)

    odd = lax.rem(m, 2)
    to_partner = remote(
        fields.at[1 + odd], partner, partner_sems.at[0], partner_sems.at[1], g, m + 1 - 2 * odd
    )
    to_partner.start()

    x_group = g - jnp.where(m == 0, 1, 0) + jnp.where(m == MEM - 1, 1, 0)
    x_plane = lax.rem(m + jnp.where(odd == 1, 1, MEM - 1), MEM)
    x_field = 2 - odd
    x_valid = jnp.logical_and(x_group >= 0, x_group < groups)
    x_home = x_group == g
    x_copies = []
    for i in range(MEM):
        q = lax.rem(m + i, MEM)
        copy = remote(fields.at[x_field, q], xb.at[x_plane], x_send.at[i], x_recv.at[x_plane], x_group, q)
        sends = jnp.logical_and(x_valid, jnp.logical_not(x_home)) if i == 0 else x_valid
        x_copies.append((copy, sends))

        @pl.when(sends)
        def _():
            copy.start()

    @pl.when(x_home)
    def _():
        xb[x_plane] = fields[x_field, m]

    to_partner.wait_recv()
    summed[...] = fields[0] + partner[...]
    own_rows = pl.ds(HALO, ROWS)
    f_copies = []
    for i in range(1, MEM):
        q = lax.rem(m + i, MEM)
        copy = remote(summed.at[q], fb.at[HALO + m, :, own_rows], f_send.at[i], f_recv.at[m], g, q)
        copy.start()
        f_copies.append(copy)
    fb[HALO + m, :, HALO : HALO + ROWS, :] = summed[m]

    for k in range(MEM):
        @pl.when(m != k)
        def _():
            remote(summed.at[0], fb.at[HALO + k, :, own_rows], f_send.at[0], f_recv.at[k], g, k).wait_recv()

        arrives = jnp.logical_not(jnp.logical_and(x_home, x_plane == k))
        if k == 0:
            arrives = jnp.logical_and(arrives, g > 0)
        if k == MEM - 1:
            arrives = jnp.logical_and(arrives, g < groups - 1)

        @pl.when(arrives)
        def _():
            remote(fields.at[0, 0], xb.at[k], x_send.at[0], x_recv.at[k], g, k).wait_recv()

        fb[HALO + k, :, HALO : HALO + ROWS, :] = fb[HALO + k, :, HALO : HALO + ROWS, :] + xb[k]

    def inside(dg, dm):
        ok = None
        for test in (
            (g + dg >= 0) if dg < 0 else (g + dg < groups) if dg > 0 else None,
            (m + dm >= 0) if dm < 0 else (m + dm < MEM) if dm > 0 else None,
        ):
            if test is not None:
                ok = test if ok is None else jnp.logical_and(ok, test)
        return ok

    def exchange(make):
        copies = []
        for o, (dg, dm) in enumerate(DIRECTIONS):
            copy = make(o, dg, dm)
            copies.append(copy)

            @pl.when(inside(dg, dm))
            def _():
                copy.start()
        return copies

    def arrive(copies):
        for o, (dg, dm) in enumerate(DIRECTIONS):
            @pl.when(inside(-dg, -dm))
            def _():
                copies[o].wait_recv()

    def row_parts(dm, base):
        if dm < 0:
            return pl.ds(base, HALO), pl.ds(base + ROWS, HALO)
        if dm > 0:
            return pl.ds(base + ROWS - HALO, HALO), pl.ds(base - HALO, HALO)
        return pl.ds(base, ROWS), pl.ds(base, ROWS)

    def plane_parts(dg, depth):
        if dg < 0:
            return pl.ds(HALO, depth), pl.ds(HALO + MEM, depth)
        if dg > 0:
            return pl.ds(HALO + MEM - depth, depth), pl.ds(HALO - depth, depth)
        return pl.ds(HALO, MEM), pl.ds(HALO, MEM)

    def forcing_copy(o, dg, dm):
        src_rows, dst_rows = row_parts(dm, HALO)
        src_planes, dst_planes = plane_parts(dg, HALO - 1)
        return remote(
            fb.at[src_planes, :, src_rows], fb.at[dst_planes, :, dst_rows],
            h_send.at[o], h_recv.at[o], g + dg, m + dm,
        )

    def black_copy(o, dg, dm):
        src_rows, dst_rows = row_parts(dm, HALO + 8)
        src_planes, dst_planes = plane_parts(dg, HALO)
        return remote(
            vk2.at[src_planes, src_rows], vk2.at[dst_planes, dst_rows],
            b_send.at[o], b_recv.at[o], g + dg, m + dm,
        )

    h_copies = exchange(forcing_copy)
    arrive(h_copies)

    lane = iota((8, 128), 1)
    row_parity = lax.rem(iota((8, 128), 0), 2)
    sixth = jnp.float32(1.0 / 6.0)
    top_scale = jnp.where(m == 0, jnp.float32(0.0), sixth)
    bottom_scale = jnp.where(m == MEM - 1, jnp.float32(0.0), sixth)

    def half_sweep(colour, low, high, target, source, tiles):
        def plane(slot, carry):
            out = jnp.logical_or(
                jnp.logical_and(slot < HALO, g == 0),
                jnp.logical_and(slot >= HALO + MEM, g == groups - 1),
            )
            flip = lax.rem(slot + colour, 2)
            from_left = row_parity == flip
            keep_left = jnp.logical_and(from_left, lane != 0)
            keep_right = jnp.logical_and(jnp.logical_not(from_left), lane != 127)
            for r in tiles:
                at = 8 + 8 * r
                centre = source[slot, at : at + 8, :]
                beside = jnp.where(
                    keep_left, pltpu.roll(centre, 1, 1),
                    jnp.where(keep_right, pltpu.roll(centre, 127, 1), 0.0),
                )
                rows = source[slot, at - 1 : at + 7, :] + source[slot, at + 1 : at + 9, :]
                depth = source[slot - 1, at : at + 8, :] + source[slot + 1, at : at + 8, :]
                scale = top_scale if r == 0 else bottom_scale if r == FROWS // 8 - 1 else sixth
                scale = jnp.where(out, jnp.float32(0.0), scale)
                total = fb[slot, colour, 8 * r : 8 * r + 8, :] + (depth + (rows + (centre + beside)))
                target[slot, at : at + 8, :] = total * scale
            return carry

        lax.fori_loop(low, high, plane, 0)

    all_tiles = tuple(range(FROWS // 8))
    own_tiles = tuple(range(1, 1 + ROWS // 8))

    def pair(black):
        def body(i, carry):
            half_sweep(0, 1 + 2 * i, SLOTS - 1 - 2 * i, vr, black, all_tiles)
            half_sweep(1, 2 + 2 * i, SLOTS - 2 - 2 * i, black, vr, all_tiles)
            return carry
        return body

    lax.fori_loop(0, 3, pair(vk), 0)
    half_sweep(0, 7, SLOTS - 7, vr, vk, all_tiles)
    half_sweep(1, 8, SLOTS - 8, vk2, vr, own_tiles)
    b_copies = exchange(black_copy)
    arrive(b_copies)
    for o, (dg, dm) in enumerate(DIRECTIONS):
        @pl.when(inside(dg, dm))
        def _():
            b_copies[o].wait_send()
    lax.fori_loop(0, 3, pair(vk2), 0)
    half_sweep(0, 7, SLOTS - 7, vr, vk2, all_tiles)

    v_rows = pl.ds(HALO + 8, ROWS)
    e_copies = []

    def send_back(colour, values):
        for i in range(MEM):
            tm = lax.rem(m + i, MEM)
            if i == 0:
                pltpu.make_async_copy(values.at[HALO + m, v_rows], e_out.at[0, m, colour], e_local.at[0, colour]).start()
            else:
                copy = remote(
                    values.at[HALO + tm, v_rows], e_out.at[0, m, colour],
                    e_send.at[0, colour, i], e_recv.at[0, colour, m], g, tm,
                )
                copy.start()
                e_copies.append((copy, None))
            wraps = tm == MEM - 1
            plane = HALO + jnp.where(wraps, 0, tm + 1)
            tg = g - jnp.where(wraps, 1, 0)
            copy = remote(
                values.at[plane, v_rows], e_out.at[1, m, colour],
                e_send.at[1, colour, i], e_recv.at[1, colour, m], tg, tm,
            )
            if i == 0:
                sends = jnp.logical_and(wraps, g > 0)

                @pl.when(jnp.logical_not(wraps))
                def _():
                    pltpu.make_async_copy(values.at[plane, v_rows], e_out.at[1, m, colour], e_local.at[1, colour]).start()
            else:
                sends = jnp.logical_not(jnp.logical_and(wraps, g == 0))
            e_copies.append((copy, sends))

            @pl.when(sends)
            def _():
                copy.start()

    send_back(0, vr)
    half_sweep(1, 8, SLOTS - 8, vk2, vr, own_tiles)
    send_back(1, vk2)

    to_partner.wait_send()
    for copy, sends in x_copies:
        @pl.when(sends)
        def _():
            copy.wait_send()
    for copy in f_copies:
        copy.wait_send()
    for o, (dg, dm) in enumerate(DIRECTIONS):
        @pl.when(inside(dg, dm))
        def _():
            h_copies[o].wait_send()
    for colour, values in ((0, vr), (1, vk2)):
        pltpu.make_async_copy(values.at[HALO, v_rows], e_out.at[0, m, colour], e_local.at[0, colour]).wait()

        @pl.when(m != MEM - 1)
        def _():
            pltpu.make_async_copy(values.at[HALO, v_rows], e_out.at[1, m, colour], e_local.at[1, colour]).wait()

        for q in range(MEM):
            def wait_for(part):
                remote(
                    values.at[HALO, v_rows], e_out.at[part, q, colour],
                    e_send.at[part, colour, 0], e_recv.at[part, colour, q], g, q,
                ).wait_recv()

            @pl.when(m != q)
            def _():
                wait_for(0)

            last = m == MEM - 1
            arrives = jnp.logical_or(
                jnp.logical_and(jnp.logical_not(last), m != q), jnp.logical_and(last, g < groups - 1)
            )

            @pl.when(arrives)
            def _():
                wait_for(1)
    for copy, sends in e_copies:
        if sends is None:
            copy.wait_send()
        else:
            @pl.when(sends)
            def _():
                copy.wait_send()


def smooth(fields):
    dma = pltpu.SemaphoreType.DMA
    return pl.pallas_call(
        smooth_kernel,
        out_shape=jax.ShapeDtypeStruct((2, MEM, 2, ROWS, 128), F32),
        in_specs=[pl.BlockSpec(memory_space=pltpu.VMEM)],
        out_specs=pl.BlockSpec(memory_space=pl.ANY),
        scratch_shapes=[
            pltpu.VMEM((MEM, 2, ROWS, 128), F32),
            pltpu.VMEM((MEM, 2, ROWS, 128), F32),
            pltpu.VMEM((SLOTS, 2, FROWS, 128), F32),
            pltpu.VMEM((MEM, 2, ROWS, 128), F32),
            pltpu.VMEM((SLOTS, VROWS, 128), F32),
            pltpu.VMEM((SLOTS, VROWS, 128), F32),
            pltpu.VMEM((SLOTS, VROWS, 128), F32),
            dma((2,)),
            dma((MEM,)),
            dma((MEM,)),
            dma((MEM,)),
            dma((MEM,)),
            dma((8,)),
            dma((8,)),
            dma((8,)),
            dma((8,)),
            dma((2, 2, MEM)),
            dma((2, 2, MEM)),
            dma((2, 2)),
        ],
        compiler_params=pltpu.CompilerParams(collective_id=0, has_side_effects=True),
        name="smooth",
    )(fields)


def prolong_kernel(e, p, corrected, correction, w_fine, w_plain):
    groups = lax.axis_size("grp")
    device = lax.axis_index("grp") * MEM + lax.axis_index("mem")
    is_last = device == groups * MEM - 1
    c = pl.program_id(0)
    blocks = CROWS // ROWS

    @pl.when(c == 0)
    def _():
        column = coarse_column((NC, NF), 0)
        fine = iota((NC, NF), 1)
        step = fine - 2 * column
        whole = jnp.logical_or(step == 0, jnp.logical_and(step == 1, column == NC - 1))
        half = jnp.logical_or(step == 1, step == -1)
        w_fine[...] = jnp.where(whole, 1.0, jnp.where(half, 0.5, 0.0)).astype(BF16)
        w_plain[...] = jnp.where(
            iota((NC, NC), 1) == coarse_column((NC, NC), 0), 1.0, 0.0
        ).astype(BF16)

    def by_column(part, shift, red, black):
        row = iota(red.shape, 0)
        even = lax.rem(row + shift + device, 2) == 0
        return jnp.concatenate([jnp.where(even, red, black), jnp.where(even, black, red)], axis=1)

    def rows_of(part):
        here = [by_column(part, part, e[part, c * blocks + b, 0], e[part, c * blocks + b, 1]) for b in range(blocks)]
        q = jnp.minimum(c * blocks + blocks, MEM - 1)
        after = by_column(part, part, e[part, q, 0, 0:8, :], e[part, q, 1, 0:8, :])
        return jnp.concatenate(here, axis=0), after

    here, after = rows_of(0)
    here_up, after_up = rows_of(1)
    at_bottom = c == CHUNKS - 1

    r = iota((FINE, CROWS), 0)
    k = iota((FINE, CROWS), 1)
    last_row = jnp.logical_and(jnp.logical_and(r == FINE - 1, k == CROWS - 1), at_bottom)
    take = jnp.where(
        jnp.logical_or(r == 2 * k, last_row), 1.0,
        jnp.where(jnp.logical_or(r == 2 * k + 1, r == 2 * k - 1), 0.5, 0.0),
    ).astype(BF16)

    def down(x, next_rows):
        parts = jnp.concatenate(split3(x), axis=1)
        out = jnp.dot(take, parts, preferred_element_type=F32)
        out = out[:, :NC] + (out[:, NC : 2 * NC] + out[:, 2 * NC :])
        carry = jnp.where(at_bottom, 0.0, 0.5 * next_rows[0:1, :])
        return out + jnp.where(iota((FINE, NC), 0) == FINE - 1, carry, 0.0)

    above = jnp.where(is_last, here, 0.5 * (here + here_up))
    above_after = jnp.where(is_last, after, 0.5 * (after + after_up))
    corrected[0] = p[0] + dot_exact(down(here, after), w_fine[...])
    corrected[1] = p[1] + dot_exact(down(above, above_after), w_fine[...])
    correction[0] = dot_exact(here, w_plain[...])


def prolong(e, potential):
    return pl.pallas_call(
        prolong_kernel,
        grid=(CHUNKS,),
        out_shape=(
            jax.ShapeDtypeStruct((2, NF, NF), F32),
            jax.ShapeDtypeStruct((1, NC, NC), F32),
        ),
        in_specs=[
            pl.BlockSpec((2, MEM, 2, ROWS, 128), lambda c: (0, 0, 0, 0, 0)),
            pl.BlockSpec((2, FINE, NF), lambda c: (0, c, 0)),
        ],
        out_specs=(
            pl.BlockSpec((2, FINE, NF), lambda c: (0, c, 0)),
            pl.BlockSpec((1, CROWS, NC), lambda c: (0, c, 0)),
        ),
        scratch_shapes=[pltpu.VMEM((NC, NF), BF16), pltpu.VMEM((NC, NC), BF16)],
        name="prolong",
    )(e, potential)


def per_device(potential, source, side_faces, end_faces):
    fields = restrict(potential, source, side_faces, end_faces)
    e = smooth(fields)
    return prolong(e, potential)


def solution(mesh):
    placed = P(("grp", "mem"), None, None)
    return jax.shard_map(
        per_device,
        mesh=mesh,
        in_specs=(placed, placed, placed, P()),
        out_specs=(placed, placed),
        check_vma=False,
    )
```

```python
import functools

import jax
import jax.numpy as jnp
from jax import lax
from jax.experimental import pallas as pl
from jax.experimental.pallas import tpu as pltpu
from jax.sharding import PartitionSpec as P

F32 = jnp.float32
BF16 = jnp.bfloat16
MESH = pl.DeviceIdType.MESH

NF = 512
NC = 256
MEM = 8
ROWS = NC // MEM
HALO = 8
SLOTS = MEM + 2 * HALO
FROWS = ROWS + 2 * HALO
VROWS = FROWS + 16
CHUNKS = 4
CROWS = NC // CHUNKS
FINE = 2 * CROWS


def iota(shape, dim):
    return lax.broadcasted_iota(jnp.int32, shape, dim)


def split3(x):
    high = x.astype(BF16)
    rest = x - high.astype(F32)
    middle = rest.astype(BF16)
    low = (rest - middle.astype(F32)).astype(BF16)
    return high, middle, low


def dot_exact(x, weights):
    rows = x.shape[0]
    parts = jnp.concatenate(split3(x), axis=0)
    out = jnp.dot(parts, weights, preferred_element_type=F32)
    return out[:rows] + (out[rows : 2 * rows] + out[2 * rows :])


def coarse_column(shape, dim):
    n = iota(shape, dim)
    return jnp.where(n < NC // 2, 2 * n, 2 * n - (NC - 1))


def restrict_kernel(p_hbm, s_hbm, side, end_hbm, out, pb, sb, eb, w_rc, w_lr, w_perm, sems, end_sem):
    groups = lax.axis_size("grp")
    device = lax.axis_index("grp") * MEM + lax.axis_index("mem")
    is_first = device == 0
    is_last = device == groups * MEM - 1

    copies = []
    for c in range(CHUNKS):
        row = []
        for t in range(4):
            for a, (src, dst) in enumerate(((p_hbm, pb), (s_hbm, sb))):
                row.append(
                    pltpu.make_async_copy(
                        src.at[:, pl.ds(FINE * c, FINE), pl.ds(128 * t, 128)],
                        dst.at[:, t, pl.ds(8 + FINE * c, FINE), :],
                        sems.at[c, t, a],
                    )
                )
        copies.append(row)
    for row in copies:
        for copy in row:
            copy.start()
    end_copy = pltpu.make_async_copy(
        end_hbm.at[jnp.where(is_last, 1, 0)], eb, end_sem
    )
    at_end = jnp.logical_or(is_first, is_last)

    @pl.when(at_end)
    def _():
        end_copy.start()

    zeros = jnp.zeros((2, 4, 8, 128), F32)
    pb[:, :, 0:8, :] = zeros
    pb[:, :, 8 + NF : 16 + NF, :] = zeros
    sb[:, :, 0:8, :] = zeros

    column = coarse_column((NF, NC), 1)
    step = jnp.abs(iota((NF, NC), 0) - 2 * column)
    w_rc[...] = jnp.where(step == 0, 0.5, jnp.where(step == 1, 0.25, 0.0)).astype(BF16)
    near = jnp.where(step == 0, jnp.where(column == 0, 0.25, 0.5), 0.5)
    w_lr[...] = jnp.where(step <= 1, near, jnp.where(step == 2, 0.25, 0.0)).astype(BF16)
    square = coarse_column((NC, NC), 1)
    w_perm[...] = jnp.where(iota((NC, NC), 0) == square, 1.0, 0.0).astype(BF16)

    front = dot_exact(jnp.broadcast_to(side[0, 0:1, :], (8, NC)), w_perm[...])[0:1]
    back = dot_exact(jnp.broadcast_to(side[0, 1:2, :], (8, NC)), w_perm[...])[0:1]
    own_weight = jnp.where(is_first, 0.25, 0.5)

    def store(field, c, value):
        row = CROWS * c + iota((CROWS, 128), 0)
        even = lax.rem(row + device + (field > 0), 2) == 0
        left, right = value[:, :128], value[:, 128:]
        red = jnp.where(even, left, right)
        black = jnp.where(even, right, left)
        for b in range(CROWS // ROWS):
            q = c * (CROWS // ROWS) + b
            out[field, q, 0] = red[ROWS * b : ROWS * (b + 1)]
            out[field, q, 1] = black[ROWS * b : ROWS * (b + 1)]

    for copy in copies[0]:
        copy.wait()
    for c in range(CHUNKS):
        if c + 1 < CHUNKS:
            for copy in copies[c + 1]:
                copy.wait()
        fields = [[], [], [], [], []]
        for t in range(4):

            def load(ref, plane, shift):
                return ref[plane, t, pl.ds(8 + FINE * c + shift, CROWS, stride=2), :]

            a, b = [], []
            for plane in (0, 1):
                p_before, p_here, p_after = (load(pb, plane, k) for k in (-1, 0, 1))
                outer = load(pb, plane, -2) + load(pb, plane, 2)
                odd = p_before + p_after
                s_part = 0.5 * load(sb, plane, 0) + 0.25 * (load(sb, plane, -1) + load(sb, plane, 1))
                value = s_part + (outer - 4.0 * odd - 10.0 * p_here)
                if c == 0:
                    value = value - jnp.where(iota(value.shape, 0) == 0, p_here, 0.0)
                a.append(value)
                b.append(2.0 * p_here + odd)
            up = 0.25 * a[1] + 0.5 * b[1]
            fields[0].append(0.5 * a[0] + up + own_weight * b[0])
            fields[1].append(up + 0.25 * b[0])
            fields[2].append(0.25 * b[0])
            fields[3].append(0.5 * b[0] + 0.25 * b[1])
            fields[4].append(0.25 * b[1])
        wide = [jnp.concatenate(f, axis=1) for f in fields]
        plain = dot_exact(jnp.concatenate(wide[:3], axis=0), w_rc[...])
        cross = dot_exact(jnp.concatenate(wide[3:], axis=0), w_lr[...])
        local = plain[:CROWS] + cross[:CROWS]
        above = plain[CROWS : 2 * CROWS] + cross[CROWS:]
        below = plain[2 * CROWS :]
        row = iota((CROWS, NC), 0)
        lane = iota((CROWS, NC), 1)
        diagonal = lane == row + CROWS * c
        left = jnp.sum(jnp.where(diagonal, side[0, 2:3, :], 0.0), axis=1, keepdims=True)
        right = jnp.sum(jnp.where(diagonal, side[0, 3:4, :], 0.0), axis=1, keepdims=True)
        local = local + jnp.where(lane == 0, left, jnp.where(lane == NC - 1, right, 0.0))
        if c == 0:
            local = local + jnp.where(row == 0, front, 0.0)
        if c == CHUNKS - 1:
            local = local + jnp.where(row == CROWS - 1, back, 0.0)
        store(0, c, local)
        store(1, c, above)
        store(2, c, below)

    @pl.when(at_end)
    def _():
        end_copy.wait()
        for c in range(CHUNKS):
            rows = pl.ds(CROWS * c, CROWS)
            face = dot_exact(eb[rows, :], w_perm[...])
            row = CROWS * c + iota((CROWS, 128), 0)
            even = lax.rem(row + device, 2) == 0
            red = jnp.where(even, face[:, :128], face[:, 128:])
            black = jnp.where(even, face[:, 128:], face[:, :128])
            for b in range(CROWS // ROWS):
                q = c * (CROWS // ROWS) + b
                out[0, q, 0] = out[0, q, 0] + red[ROWS * b : ROWS * (b + 1)]
                out[0, q, 1] = out[0, q, 1] + black[ROWS * b : ROWS * (b + 1)]


def restrict(potential, source, side_faces, end_faces):
    anyspace = pl.BlockSpec(memory_space=pl.ANY)
    return pl.pallas_call(
        restrict_kernel,
        out_shape=jax.ShapeDtypeStruct((3, MEM, 2, ROWS, 128), F32),
        in_specs=[anyspace, anyspace, pl.BlockSpec(memory_space=pltpu.VMEM), anyspace],
        out_specs=pl.BlockSpec(memory_space=pltpu.VMEM),
        scratch_shapes=[
            pltpu.VMEM((2, 4, NF + 16, 128), F32),
            pltpu.VMEM((2, 4, NF + 16, 128), F32),
            pltpu.VMEM((NC, NC), F32),
            pltpu.VMEM((NF, NC), BF16),
            pltpu.VMEM((NF, NC), BF16),
            pltpu.VMEM((NC, NC), BF16),
            pltpu.SemaphoreType.DMA((CHUNKS, 4, 2)),
            pltpu.SemaphoreType.DMA,
        ],
        name="restrict",
    )(potential, source, side_faces, end_faces)


DIRECTIONS = tuple((dg, dm) for dg in (-1, 0, 1) for dm in (-1, 0, 1) if (dg, dm) != (0, 0))


def smooth_kernel(
    fields, e_out, partner, summed, fb, xb, vr, vk, vk2, scales,
    partner_sems, f_send, f_recv, x_send, x_recv, h_send, h_recv, b_send, b_recv, e_send, e_recv, e_local,
):
    groups = lax.axis_size("grp")
    g = lax.axis_index("grp")
    m = lax.axis_index("mem")

    def remote(src, dst, send, recv, tg, tm):
        return pltpu.make_async_remote_copy(
            src_ref=src, dst_ref=dst, send_sem=send, recv_sem=recv,
            device_id={"grp": tg, "mem": tm}, device_id_type=MESH,
        )

    vr[...] = jnp.zeros_like(vr)
    vk[...] = jnp.zeros_like(vk)
    vk2[...] = jnp.zeros_like(vk2)
    fb[...] = jnp.zeros_like(fb)
    xb[...] = jnp.zeros_like(xb)

    row = m * ROWS - HALO + iota((FROWS, 128), 0)
    inner = jnp.where(jnp.logical_and(row >= 0, row < NC), 1.0 / 6.0, 0.0)
    scales[0] = jnp.where(g > 0, inner, 0.0)
    scales[1] = inner
    scales[2] = jnp.where(g < groups - 1, inner, 0.0)

    barrier = pltpu.get_barrier_semaphore()
    for dg in (-1, 0, 1):
        exists = jnp.logical_and(g + dg >= 0, g + dg < groups)

        @pl.when(exists)
        def _():
            for i in range(1 if dg == 0 else 0, MEM):
                pl.semaphore_signal(
                    barrier, inc=1,
                    device_id={"grp": g + dg, "mem": lax.rem(m + i, MEM)}, device_id_type=MESH,
                )
    count = (MEM - 1) + jnp.where(g > 0, MEM, 0) + jnp.where(g < groups - 1, MEM, 0)
    pl.semaphore_wait(barrier, count)

    odd = lax.rem(m, 2)
    to_partner = remote(
        fields.at[1 + odd], partner, partner_sems.at[0], partner_sems.at[1], g, m + 1 - 2 * odd
    )
    to_partner.start()

    x_group = g - jnp.where(m == 0, 1, 0) + jnp.where(m == MEM - 1, 1, 0)
    x_plane = lax.rem(m + jnp.where(odd == 1, 1, MEM - 1), MEM)
    x_field = 2 - odd
    x_valid = jnp.logical_and(x_group >= 0, x_group < groups)
    x_home = x_group == g
    x_copies = []
    for i in range(MEM):
        q = lax.rem(m + i, MEM)
        copy = remote(fields.at[x_field, q], xb.at[x_plane], x_send.at[i], x_recv.at[x_plane], x_group, q)
        sends = jnp.logical_and(x_valid, jnp.logical_not(x_home)) if i == 0 else x_valid
        x_copies.append((copy, sends))

        @pl.when(sends)
        def _():
            copy.start()

    @pl.when(x_home)
    def _():
        xb[x_plane] = fields[x_field, m]

    to_partner.wait_recv()
    summed[...] = fields[0] + partner[...]
    own_rows = pl.ds(HALO, ROWS)
    f_copies = []
    for i in range(1, MEM):
        q = lax.rem(m + i, MEM)
        copy = remote(summed.at[q], fb.at[HALO + m, :, own_rows], f_send.at[i], f_recv.at[m], g, q)
        copy.start()
        f_copies.append(copy)
    fb[HALO + m, :, HALO : HALO + ROWS, :] = summed[m]

    for k in range(MEM):
        @pl.when(m != k)
        def _():
            remote(summed.at[0], fb.at[HALO + k, :, own_rows], f_send.at[0], f_recv.at[k], g, k).wait_recv()

        arrives = jnp.logical_not(jnp.logical_and(x_home, x_plane == k))
        if k == 0:
            arrives = jnp.logical_and(arrives, g > 0)
        if k == MEM - 1:
            arrives = jnp.logical_and(arrives, g < groups - 1)

        @pl.when(arrives)
        def _():
            remote(fields.at[0, 0], xb.at[k], x_send.at[0], x_recv.at[k], g, k).wait_recv()

        fb[HALO + k, :, HALO : HALO + ROWS, :] = fb[HALO + k, :, HALO : HALO + ROWS, :] + xb[k]

    def inside(dg, dm):
        ok = None
        for test in (
            (g + dg >= 0) if dg < 0 else (g + dg < groups) if dg > 0 else None,
            (m + dm >= 0) if dm < 0 else (m + dm < MEM) if dm > 0 else None,
        ):
            if test is not None:
                ok = test if ok is None else jnp.logical_and(ok, test)
        return ok

    def exchange(make):
        copies = []
        for o, (dg, dm) in enumerate(DIRECTIONS):
            copy = make(o, dg, dm)
            copies.append(copy)

            @pl.when(inside(dg, dm))
            def _():
                copy.start()
        return copies

    def arrive(copies):
        for o, (dg, dm) in enumerate(DIRECTIONS):
            @pl.when(inside(-dg, -dm))
            def _():
                copies[o].wait_recv()

    def row_parts(dm, base):
        if dm < 0:
            return pl.ds(base, HALO), pl.ds(base + ROWS, HALO)
        if dm > 0:
            return pl.ds(base + ROWS - HALO, HALO), pl.ds(base - HALO, HALO)
        return pl.ds(base, ROWS), pl.ds(base, ROWS)

    def plane_parts(dg, depth):
        if dg < 0:
            return pl.ds(HALO, depth), pl.ds(HALO + MEM, depth)
        if dg > 0:
            return pl.ds(HALO + MEM - depth, depth), pl.ds(HALO - depth, depth)
        return pl.ds(HALO, MEM), pl.ds(HALO, MEM)

    def forcing_copy(o, dg, dm):
        src_rows, dst_rows = row_parts(dm, HALO)
        src_planes, dst_planes = plane_parts(dg, HALO - 1)
        return remote(
            fb.at[src_planes, :, src_rows], fb.at[dst_planes, :, dst_rows],
            h_send.at[o], h_recv.at[o], g + dg, m + dm,
        )

    def black_copy(o, dg, dm):
        src_rows, dst_rows = row_parts(dm, HALO + 8)
        src_planes, dst_planes = plane_parts(dg, HALO)
        return remote(
            vk2.at[src_planes, src_rows], vk2.at[dst_planes, dst_rows],
            b_send.at[o], b_recv.at[o], g + dg, m + dm,
        )

    h_copies = exchange(forcing_copy)
    arrive(h_copies)

    lane = iota((8, 128), 1)
    row_parity = lax.rem(iota((8, 128), 0), 2)
    from_left = [
        (jnp.logical_and(row_parity == flip, lane != 0), jnp.logical_and(row_parity != flip, lane != 127))
        for flip in (0, 1)
    ]

    def half_sweep(colour, t, target, source, first=0, tiles=FROWS // 8):
        at, n = 8 + 8 * first, 8 * tiles
        shape = (tiles, 8, 128)
        for slot in range(t, SLOTS - t):
            centre = source[slot, at : at + n, :].reshape(shape)
            keep_left, keep_right = from_left[(slot + colour) % 2]
            beside = jnp.where(
                jnp.broadcast_to(keep_left, shape), pltpu.roll(centre, 1, 2),
                jnp.where(jnp.broadcast_to(keep_right, shape), pltpu.roll(centre, 127, 2), 0.0),
            )
            rows = source[slot, at - 1 : at - 1 + n, :] + source[slot, at + 1 : at + 1 + n, :]
            depth = source[slot - 1, at : at + n, :] + source[slot + 1, at : at + n, :]
            side = 0 if slot < HALO else 2 if slot >= HALO + MEM else 1
            near = (depth + rows).reshape(shape) + (centre + beside)
            total = fb[slot, colour, 8 * first : 8 * first + n, :].reshape(shape) + near
            total = total * scales[side, 8 * first : 8 * first + n, :].reshape(shape)
            target[slot, at : at + n, :] = total.reshape(n, 128)

    def sweeps(black):
        for t in (1, 3, 5):
            half_sweep(0, t, vr, black)
            half_sweep(1, t + 1, black, vr)
        half_sweep(0, 7, vr, black)

    sweeps(vk)
    half_sweep(1, 8, vk2, vr, 1, ROWS // 8)
    b_copies = exchange(black_copy)
    arrive(b_copies)
    for o, (dg, dm) in enumerate(DIRECTIONS):
        @pl.when(inside(dg, dm))
        def _():
            b_copies[o].wait_send()
    sweeps(vk2)

    v_rows = pl.ds(HALO + 8, ROWS)
    e_copies = []

    def send_back(colour, values):
        for i in range(MEM):
            tm = lax.rem(m + i, MEM)
            if i == 0:
                pltpu.make_async_copy(values.at[HALO + m, v_rows], e_out.at[0, m, colour], e_local.at[0, colour]).start()
            else:
                copy = remote(
                    values.at[HALO + tm, v_rows], e_out.at[0, m, colour],
                    e_send.at[0, colour, i], e_recv.at[0, colour, m], g, tm,
                )
                copy.start()
                e_copies.append((copy, None))
            wraps = tm == MEM - 1
            plane = HALO + jnp.where(wraps, 0, tm + 1)
            tg = g - jnp.where(wraps, 1, 0)
            copy = remote(
                values.at[plane, v_rows], e_out.at[1, m, colour],
                e_send.at[1, colour, i], e_recv.at[1, colour, m], tg, tm,
            )
            if i == 0:
                sends = jnp.logical_and(wraps, g > 0)

                @pl.when(jnp.logical_not(wraps))
                def _():
                    pltpu.make_async_copy(values.at[plane, v_rows], e_out.at[1, m, colour], e_local.at[1, colour]).start()
            else:
                sends = jnp.logical_not(jnp.logical_and(wraps, g == 0))
            e_copies.append((copy, sends))

            @pl.when(sends)
            def _():
                copy.start()

    send_back(0, vr)
    half_sweep(1, 8, vk2, vr, 1, ROWS // 8)
    send_back(1, vk2)

    to_partner.wait_send()
    for copy, sends in x_copies:
        @pl.when(sends)
        def _():
            copy.wait_send()
    for copy in f_copies:
        copy.wait_send()
    for o, (dg, dm) in enumerate(DIRECTIONS):
        @pl.when(inside(dg, dm))
        def _():
            h_copies[o].wait_send()
    for colour, values in ((0, vr), (1, vk2)):
        pltpu.make_async_copy(values.at[HALO, v_rows], e_out.at[0, m, colour], e_local.at[0, colour]).wait()

        @pl.when(m != MEM - 1)
        def _():
            pltpu.make_async_copy(values.at[HALO, v_rows], e_out.at[1, m, colour], e_local.at[1, colour]).wait()

        for q in range(MEM):
            def wait_for(part):
                remote(
                    values.at[HALO, v_rows], e_out.at[part, q, colour],
                    e_send.at[part, colour, 0], e_recv.at[part, colour, q], g, q,
                ).wait_recv()

            @pl.when(m != q)
            def _():
                wait_for(0)

            last = m == MEM - 1
            arrives = jnp.logical_or(
                jnp.logical_and(jnp.logical_not(last), m != q), jnp.logical_and(last, g < groups - 1)
            )

            @pl.when(arrives)
            def _():
                wait_for(1)
    for copy, sends in e_copies:
        if sends is None:
            copy.wait_send()
        else:
            @pl.when(sends)
            def _():
                copy.wait_send()


def smooth(fields):
    dma = pltpu.SemaphoreType.DMA
    return pl.pallas_call(
        smooth_kernel,
        out_shape=jax.ShapeDtypeStruct((2, MEM, 2, ROWS, 128), F32),
        in_specs=[pl.BlockSpec(memory_space=pltpu.VMEM)],
        out_specs=pl.BlockSpec(memory_space=pl.ANY),
        scratch_shapes=[
            pltpu.VMEM((MEM, 2, ROWS, 128), F32),
            pltpu.VMEM((MEM, 2, ROWS, 128), F32),
            pltpu.VMEM((SLOTS, 2, FROWS, 128), F32),
            pltpu.VMEM((MEM, 2, ROWS, 128), F32),
            pltpu.VMEM((SLOTS, VROWS, 128), F32),
            pltpu.VMEM((SLOTS, VROWS, 128), F32),
            pltpu.VMEM((SLOTS, VROWS, 128), F32),
            pltpu.VMEM((3, FROWS, 128), F32),
            dma((2,)),
            dma((MEM,)),
            dma((MEM,)),
            dma((MEM,)),
            dma((MEM,)),
            dma((8,)),
            dma((8,)),
            dma((8,)),
            dma((8,)),
            dma((2, 2, MEM)),
            dma((2, 2, MEM)),
            dma((2, 2)),
        ],
        compiler_params=pltpu.CompilerParams(collective_id=0, has_side_effects=True),
        name="smooth",
    )(fields)


def prolong_kernel(e, p, corrected, correction, w_fine, w_plain):
    groups = lax.axis_size("grp")
    device = lax.axis_index("grp") * MEM + lax.axis_index("mem")
    is_last = device == groups * MEM - 1
    c = pl.program_id(0)
    blocks = CROWS // ROWS

    @pl.when(c == 0)
    def _():
        column = coarse_column((NC, NF), 0)
        fine = iota((NC, NF), 1)
        step = fine - 2 * column
        whole = jnp.logical_or(step == 0, jnp.logical_and(step == 1, column == NC - 1))
        half = jnp.logical_or(step == 1, step == -1)
        w_fine[...] = jnp.where(whole, 1.0, jnp.where(half, 0.5, 0.0)).astype(BF16)
        w_plain[...] = jnp.where(
            iota((NC, NC), 1) == coarse_column((NC, NC), 0), 1.0, 0.0
        ).astype(BF16)

    def by_column(part, shift, red, black):
        row = iota(red.shape, 0)
        even = lax.rem(row + shift + device, 2) == 0
        return jnp.concatenate([jnp.where(even, red, black), jnp.where(even, black, red)], axis=1)

    def rows_of(part):
        here = [by_column(part, part, e[part, c * blocks + b, 0], e[part, c * blocks + b, 1]) for b in range(blocks)]
        q = jnp.minimum(c * blocks + blocks, MEM - 1)
        after = by_column(part, part, e[part, q, 0, 0:8, :], e[part, q, 1, 0:8, :])
        return jnp.concatenate(here, axis=0), after

    here, after = rows_of(0)
    here_up, after_up = rows_of(1)
    at_bottom = c == CHUNKS - 1

    r = iota((FINE, CROWS), 0)
    k = iota((FINE, CROWS), 1)
    last_row = jnp.logical_and(jnp.logical_and(r == FINE - 1, k == CROWS - 1), at_bottom)
    take = jnp.where(
        jnp.logical_or(r == 2 * k, last_row), 1.0,
        jnp.where(jnp.logical_or(r == 2 * k + 1, r == 2 * k - 1), 0.5, 0.0),
    ).astype(BF16)

    def down(x, next_rows):
        parts = jnp.concatenate(split3(x), axis=1)
        out = jnp.dot(take, parts, preferred_element_type=F32)
        out = out[:, :NC] + (out[:, NC : 2 * NC] + out[:, 2 * NC :])
        carry = jnp.where(at_bottom, 0.0, 0.5 * next_rows[0:1, :])
        return out + jnp.where(iota((FINE, NC), 0) == FINE - 1, carry, 0.0)

    above = jnp.where(is_last, here, 0.5 * (here + here_up))
    above_after = jnp.where(is_last, after, 0.5 * (after + after_up))
    corrected[0] = p[0] + dot_exact(down(here, after), w_fine[...])
    corrected[1] = p[1] + dot_exact(down(above, above_after), w_fine[...])
    correction[0] = dot_exact(here, w_plain[...])


def prolong(e, potential):
    return pl.pallas_call(
        prolong_kernel,
        grid=(CHUNKS,),
        out_shape=(
            jax.ShapeDtypeStruct((2, NF, NF), F32),
            jax.ShapeDtypeStruct((1, NC, NC), F32),
        ),
        in_specs=[
            pl.BlockSpec((2, MEM, 2, ROWS, 128), lambda c: (0, 0, 0, 0, 0)),
            pl.BlockSpec((2, FINE, NF), lambda c: (0, c, 0)),
        ],
        out_specs=(
            pl.BlockSpec((2, FINE, NF), lambda c: (0, c, 0)),
            pl.BlockSpec((1, CROWS, NC), lambda c: (0, c, 0)),
        ),
        scratch_shapes=[pltpu.VMEM((NC, NF), BF16), pltpu.VMEM((NC, NC), BF16)],
        name="prolong",
    )(e, potential)


def per_device(potential, source, side_faces, end_faces):
    fields = restrict(potential, source, side_faces, end_faces)
    e = smooth(fields)
    return prolong(e, potential)


def solution(mesh):
    placed = P(("grp", "mem"), None, None)
    return jax.shard_map(
        per_device,
        mesh=mesh,
        in_specs=(placed, placed, placed, P()),
        out_specs=(placed, placed),
        check_vma=False,
    )
```

```python
import jax
import jax.numpy as jnp
from jax import lax
from jax.experimental import pallas as pl
from jax.experimental.pallas import tpu as pltpu
from jax.sharding import PartitionSpec as P

F32 = jnp.float32
BF16 = jnp.bfloat16
MESH = pl.DeviceIdType.MESH

NF = 512
NC = 256
MEM = 8
ROWS = NC // MEM
HALO = 8
SLOTS = MEM + 2 * HALO
FROWS = ROWS + 2 * HALO
VROWS = FROWS + 16
CHUNKS = 4
CROWS = NC // CHUNKS
FINE = 2 * CROWS


def iota(shape, dim):
    return lax.broadcasted_iota(jnp.int32, shape, dim)


def split3(x):
    high = x.astype(BF16)
    rest = x - high.astype(F32)
    middle = rest.astype(BF16)
    low = (rest - middle.astype(F32)).astype(BF16)
    return high, middle, low


def dot_exact(x, weights):
    rows = x.shape[0]
    parts = jnp.concatenate(split3(x), axis=0)
    out = jnp.dot(parts, weights, preferred_element_type=F32)
    return out[:rows] + (out[rows : 2 * rows] + out[2 * rows :])


def coarse_column(shape, dim):
    n = iota(shape, dim)
    return jnp.where(n < NC // 2, 2 * n, 2 * n - (NC - 1))


DIRECTIONS = tuple((dg, dm) for dg in (-1, 0, 1) for dm in (-1, 0, 1) if (dg, dm) != (0, 0))


def smooth_kernel(
    p_hbm, s_hbm, side, end_hbm, e_out,
    pb, sb, eb, w_rc, w_lr, w_perm, fields, partner, summed, fb, xb, vr, vk, vk2, scales,
    in_sems, end_sem, p_send, p_recv, f_send, f_recv, x_send, x_recv, h_send, h_recv, b_send, b_recv,
    e_send, e_recv, e_local,
):
    groups = lax.axis_size("grp")
    g = lax.axis_index("grp")
    m = lax.axis_index("mem")
    device = g * MEM + m
    is_first = device == 0
    is_last = device == groups * MEM - 1
    at_end = jnp.logical_or(is_first, is_last)

    def remote(src, dst, send, recv, tg, tm):
        return pltpu.make_async_remote_copy(
            src_ref=src, dst_ref=dst, send_sem=send, recv_sem=recv,
            device_id={"grp": tg, "mem": tm}, device_id_type=MESH,
        )

    in_copies = []
    for t in range(4):
        for a, (src, dst) in enumerate(((p_hbm, pb), (s_hbm, sb))):
            in_copies.append(
                pltpu.make_async_copy(
                    src.at[:, :, pl.ds(128 * t, 128)], dst.at[:, t, pl.ds(8, NF), :], in_sems.at[t, a]
                )
            )
    for copy in in_copies:
        copy.start()
    end_copy = pltpu.make_async_copy(end_hbm.at[jnp.where(is_last, 1, 0)], eb, end_sem)

    @pl.when(at_end)
    def _():
        end_copy.start()

    vk2[...] = jnp.zeros_like(vk2)
    fb[...] = jnp.zeros_like(fb)
    xb[...] = jnp.zeros_like(xb)

    barrier = pltpu.get_barrier_semaphore()
    for dg in (-1, 0, 1):
        exists = jnp.logical_and(g + dg >= 0, g + dg < groups)

        @pl.when(exists)
        def _():
            for i in range(1 if dg == 0 else 0, MEM):
                pl.semaphore_signal(
                    barrier, inc=1,
                    device_id={"grp": g + dg, "mem": lax.rem(m + i, MEM)}, device_id_type=MESH,
                )

    vr[...] = jnp.zeros_like(vr)
    vk[...] = jnp.zeros_like(vk)
    row = m * ROWS - HALO + iota((FROWS, 128), 0)
    inner = jnp.where(jnp.logical_and(row >= 0, row < NC), 1.0 / 6.0, 0.0)
    scales[0] = jnp.where(g > 0, inner, 0.0)
    scales[1] = inner
    scales[2] = jnp.where(g < groups - 1, inner, 0.0)

    zeros = jnp.zeros((2, 4, 8, 128), F32)
    pb[:, :, 0:8, :] = zeros
    pb[:, :, 8 + NF : 16 + NF, :] = zeros
    sb[:, :, 0:8, :] = zeros

    column = coarse_column((NF, NC), 1)
    step = jnp.abs(iota((NF, NC), 0) - 2 * column)
    w_rc[...] = jnp.where(step == 0, 0.5, jnp.where(step == 1, 0.25, 0.0)).astype(BF16)
    near = jnp.where(step == 0, jnp.where(column == 0, 0.25, 0.5), 0.5)
    w_lr[...] = jnp.where(step <= 1, near, jnp.where(step == 2, 0.25, 0.0)).astype(BF16)
    square = coarse_column((NC, NC), 1)
    w_perm[...] = jnp.where(iota((NC, NC), 0) == square, 1.0, 0.0).astype(BF16)

    front = dot_exact(jnp.broadcast_to(side[0, 0:1, :], (8, NC)), w_perm[...])[0:1]
    back = dot_exact(jnp.broadcast_to(side[0, 1:2, :], (8, NC)), w_perm[...])[0:1]
    own_weight = jnp.where(is_first, 0.25, 0.5)
    for copy in in_copies:
        copy.wait()

    blocks = CROWS // ROWS

    def by_colour(value, shift):
        even = lax.rem(iota((CROWS, 128), 0) + device + shift, 2) == 0
        left, right = value[:, :128], value[:, 128:]
        return jnp.where(even, left, right), jnp.where(even, right, left)

    def restrict(c):
        lists = [[], [], [], [], []]
        row = CROWS * c + iota((CROWS, 128), 0)
        for t in range(4):

            def load(ref, plane, shift):
                return ref[plane, t, pl.ds(8 + FINE * c + shift, CROWS, stride=2), :]

            a, b = [], []
            for plane in (0, 1):
                p_before, p_here, p_after = (load(pb, plane, k) for k in (-1, 0, 1))
                outer = load(pb, plane, -2) + load(pb, plane, 2)
                odd = p_before + p_after
                s_part = 0.5 * load(sb, plane, 0) + 0.25 * (load(sb, plane, -1) + load(sb, plane, 1))
                value = s_part + (outer - 4.0 * odd - 10.0 * p_here)
                a.append(value - jnp.where(row == 0, p_here, 0.0))
                b.append(2.0 * p_here + odd)
            up = 0.25 * a[1] + 0.5 * b[1]
            lists[0].append(0.5 * a[0] + up + own_weight * b[0])
            lists[1].append(up + 0.25 * b[0])
            lists[2].append(0.25 * b[0])
            lists[3].append(0.5 * b[0] + 0.25 * b[1])
            lists[4].append(0.25 * b[1])
        wide = [jnp.concatenate(f, axis=1) for f in lists]
        plain = dot_exact(jnp.concatenate(wide[:3], axis=0), w_rc[...])
        cross = dot_exact(jnp.concatenate(wide[3:], axis=0), w_lr[...])
        local = plain[:CROWS] + cross[:CROWS]
        above = plain[CROWS : 2 * CROWS] + cross[CROWS:]
        below = plain[2 * CROWS :]
        row = CROWS * c + iota((CROWS, NC), 0)
        lane = iota((CROWS, NC), 1)
        left = jnp.sum(jnp.where(lane == row, side[0, 2:3, :], 0.0), axis=1, keepdims=True)
        right = jnp.sum(jnp.where(lane == row, side[0, 3:4, :], 0.0), axis=1, keepdims=True)
        local = local + jnp.where(lane == 0, left, jnp.where(lane == NC - 1, right, 0.0))
        local = local + jnp.where(row == 0, front, jnp.where(row == NC - 1, back, 0.0))
        for field, value in ((0, local), (1, above), (2, below)):
            for colour, part in enumerate(by_colour(value, int(field > 0))):
                for b in range(blocks):
                    fields[field, c * blocks + b, colour] = part[ROWS * b : ROWS * (b + 1)]

    def add_end_face(c):
        face = dot_exact(eb[pl.ds(pl.multiple_of(CROWS * c, CROWS), CROWS), :], w_perm[...])
        for colour, part in enumerate(by_colour(face, 0)):
            for b in range(blocks):
                q = c * blocks + b
                fields[0, q, colour] = fields[0, q, colour] + part[ROWS * b : ROWS * (b + 1)]

    odd = lax.rem(m, 2)
    x_group = g - jnp.where(m == 0, 1, 0) + jnp.where(m == MEM - 1, 1, 0)
    x_plane = lax.rem(m + jnp.where(odd == 1, 1, MEM - 1), MEM)
    x_field = 2 - odd
    x_valid = jnp.logical_and(x_group >= 0, x_group < groups)
    x_home = x_group == g
    own_rows = pl.ds(HALO, ROWS)
    sent = []

    def send_if(condition, copy):
        sent.append((condition, copy))

        @pl.when(condition)
        def _():
            copy.start()

    def send_fields(i, c):
        part = pl.ds(c * blocks, blocks)
        copy = remote(
            fields.at[1 + odd, part], partner.at[part], p_send.at[i], p_recv.at[i], g, m + 1 - 2 * odd
        )
        copy.start()
        for b in range(blocks):
            q = c * blocks + b
            home = jnp.logical_and(x_home, q == m)
            send_if(
                jnp.logical_and(x_valid, jnp.logical_not(home)),
                remote(
                    fields.at[x_field, q], xb.at[x_plane], x_send.at[i, b], x_recv.at[x_plane], x_group, q
                ),
            )

            @pl.when(home)
            def _():
                xb[x_plane] = fields[x_field, q]
        return copy

    def send_sums(i, c, to_partner):
        to_partner.wait_recv()
        for b in range(blocks):
            q = c * blocks + b
            summed[q] = fields[0, q] + partner[q]
            send_if(
                q != m,
                remote(summed.at[q], fb.at[HALO + m, :, own_rows], f_send.at[i, b], f_recv.at[m], g, q),
            )

            @pl.when(q == m)
            def _():
                fb[HALO + m, :, HALO : HALO + ROWS, :] = summed[q]

    @pl.when(at_end)
    def _():
        end_copy.wait()

    partners = []
    for i in range(CHUNKS):
        c = lax.rem(m // blocks + 1 + i, CHUNKS)
        restrict(c)

        @pl.when(at_end)
        def _():
            add_end_face(c)

        if i == 0:
            count = (MEM - 1) + jnp.where(g > 0, MEM, 0) + jnp.where(g < groups - 1, MEM, 0)
            pl.semaphore_wait(barrier, count)
        partners.append(send_fields(i, c))
        if i > 0:
            send_sums(i - 1, lax.rem(m // blocks + i, CHUNKS), partners[i - 1])
    send_sums(CHUNKS - 1, m // blocks, partners[-1])

    def inside(dg, dm):
        ok = None
        for test in (
            (g + dg >= 0) if dg < 0 else (g + dg < groups) if dg > 0 else None,
            (m + dm >= 0) if dm < 0 else (m + dm < MEM) if dm > 0 else None,
        ):
            if test is not None:
                ok = test if ok is None else jnp.logical_and(ok, test)
        return ok

    def exchange(make):
        copies = []
        for o, (dg, dm) in enumerate(DIRECTIONS):
            copy = make(o, dg, dm)
            copies.append(copy)

            @pl.when(inside(dg, dm))
            def _():
                copy.start()
        return copies

    def arrive(copies):
        for o, (dg, dm) in enumerate(DIRECTIONS):
            @pl.when(inside(-dg, -dm))
            def _():
                copies[o].wait_recv()

    def row_parts(dm, base):
        if dm < 0:
            return pl.ds(base, HALO), pl.ds(base + ROWS, HALO)
        if dm > 0:
            return pl.ds(base + ROWS - HALO, HALO), pl.ds(base - HALO, HALO)
        return pl.ds(base, ROWS), pl.ds(base, ROWS)

    def plane_parts(dg, depth):
        if dg < 0:
            return pl.ds(HALO, depth), pl.ds(HALO + MEM, depth)
        if dg > 0:
            return pl.ds(HALO + MEM - depth, depth), pl.ds(HALO - depth, depth)
        return pl.ds(HALO, MEM), pl.ds(HALO, MEM)

    def forcing_copy(o, dg, dm, k=None):
        src_rows, dst_rows = row_parts(dm, HALO)
        if k is None:
            src, dst = plane_parts(dg, HALO - 1 - abs(dm))
        else:
            src, dst = HALO + k, HALO + k - MEM * dg
        return remote(
            fb.at[src, :, src_rows], fb.at[dst, :, dst_rows], h_send.at[o], h_recv.at[o], g + dg, m + dm
        )

    def receive(n, carry):
        k = lax.rem(m // blocks * blocks + 2 * MEM - blocks * (1 + n // blocks) + lax.rem(n, blocks), MEM)

        @pl.when(m != k)
        def _():
            remote(summed.at[0], fb.at[HALO + k, :, own_rows], f_send.at[0, 0], f_recv.at[k], g, k).wait_recv()

        arrives = jnp.logical_not(jnp.logical_and(x_home, x_plane == k))
        arrives = jnp.logical_and(arrives, jnp.logical_or(k > 0, g > 0))
        arrives = jnp.logical_and(arrives, jnp.logical_or(k < MEM - 1, g < groups - 1))

        @pl.when(arrives)
        def _():
            remote(fields.at[0, 0], xb.at[k], x_send.at[0, 0], x_recv.at[k], g, k).wait_recv()

        fb[HALO + k, :, HALO : HALO + ROWS, :] = fb[HALO + k, :, HALO : HALO + ROWS, :] + xb[k]
        for o, (dg, dm) in enumerate(DIRECTIONS):
            depth = HALO - 1 - abs(dm)
            needed = inside(dg, dm)
            if dg < 0:
                needed = jnp.logical_and(needed, k < depth)
            if dg > 0:
                needed = jnp.logical_and(needed, k >= MEM - depth)

            @pl.when(needed)
            def _():
                forcing_copy(o, dg, dm, k).start()
        return carry

    def black_copy(o, dg, dm):
        src_rows, dst_rows = row_parts(dm, HALO + 8)
        src_planes, dst_planes = plane_parts(dg, HALO - abs(dm))
        return remote(
            vk2.at[src_planes, src_rows], vk2.at[dst_planes, dst_rows],
            b_send.at[o], b_recv.at[o], g + dg, m + dm,
        )

    lax.fori_loop(0, MEM, receive, 0)
    h_copies = [forcing_copy(o, dg, dm) for o, (dg, dm) in enumerate(DIRECTIONS)]
    arrive(h_copies)

    lane = iota((8, 128), 1)
    row_parity = lax.rem(iota((8, 128), 0), 2)
    from_left = [
        (jnp.logical_and(row_parity == flip, lane != 0), jnp.logical_and(row_parity != flip, lane != 127))
        for flip in (0, 1)
    ]

    def half_sweep(colour, t, target, source, first=0, tiles=FROWS // 8):
        at, n = 8 + 8 * first, 8 * tiles
        shape = (tiles, 8, 128)
        for slot in range(t, SLOTS - t):
            centre = source[slot, at : at + n, :].reshape(shape)
            keep_left, keep_right = from_left[(slot + colour) % 2]
            beside = jnp.where(
                jnp.broadcast_to(keep_left, shape), pltpu.roll(centre, 1, 2),
                jnp.where(jnp.broadcast_to(keep_right, shape), pltpu.roll(centre, 127, 2), 0.0),
            )
            rows = source[slot, at - 1 : at - 1 + n, :] + source[slot, at + 1 : at + 1 + n, :]
            depth = source[slot - 1, at : at + n, :] + source[slot + 1, at : at + n, :]
            side = 0 if slot < HALO else 2 if slot >= HALO + MEM else 1
            near = (depth + rows).reshape(shape) + (centre + beside)
            total = fb[slot, colour, 8 * first : 8 * first + n, :].reshape(shape) + near
            total = total * scales[side, 8 * first : 8 * first + n, :].reshape(shape)
            target[slot, at : at + n, :] = total.reshape(n, 128)

    def sweeps(black):
        for t in (1, 3, 5):
            half_sweep(0, t, vr, black)
            half_sweep(1, t + 1, black, vr)
        half_sweep(0, 7, vr, black)

    sweeps(vk)
    half_sweep(1, 8, vk2, vr, 1, ROWS // 8)
    b_copies = exchange(black_copy)
    arrive(b_copies)
    for o, (dg, dm) in enumerate(DIRECTIONS):
        @pl.when(inside(dg, dm))
        def _():
            b_copies[o].wait_send()
    sweeps(vk2)

    v_rows = pl.ds(HALO + 8, ROWS)
    e_copies = []

    def send_back(colour, values):
        for i in range(MEM):
            tm = lax.rem(m + i, MEM)
            if i == 0:
                pltpu.make_async_copy(values.at[HALO + m, v_rows], e_out.at[0, m, colour], e_local.at[0, colour]).start()
            else:
                copy = remote(
                    values.at[HALO + tm, v_rows], e_out.at[0, m, colour],
                    e_send.at[0, colour, i], e_recv.at[0, colour, m], g, tm,
                )
                copy.start()
                e_copies.append((copy, None))
            wraps = tm == MEM - 1
            plane = HALO + jnp.where(wraps, 0, tm + 1)
            tg = g - jnp.where(wraps, 1, 0)
            copy = remote(
                values.at[plane, v_rows], e_out.at[1, m, colour],
                e_send.at[1, colour, i], e_recv.at[1, colour, m], tg, tm,
            )
            if i == 0:
                sends = jnp.logical_and(wraps, g > 0)

                @pl.when(jnp.logical_not(wraps))
                def _():
                    pltpu.make_async_copy(values.at[plane, v_rows], e_out.at[1, m, colour], e_local.at[1, colour]).start()
            else:
                sends = jnp.logical_not(jnp.logical_and(wraps, g == 0))
            e_copies.append((copy, sends))

            @pl.when(sends)
            def _():
                copy.start()

    send_back(0, vr)
    half_sweep(1, 8, vk2, vr, 1, ROWS // 8)
    send_back(1, vk2)

    for copy in partners:
        copy.wait_send()
    for condition, copy in sent:
        @pl.when(condition)
        def _():
            copy.wait_send()
    for o, (dg, dm) in enumerate(DIRECTIONS):
        @pl.when(inside(dg, dm))
        def _():
            h_copies[o].wait_send()
    for colour, values in ((0, vr), (1, vk2)):
        pltpu.make_async_copy(values.at[HALO, v_rows], e_out.at[0, m, colour], e_local.at[0, colour]).wait()

        @pl.when(m != MEM - 1)
        def _():
            pltpu.make_async_copy(values.at[HALO, v_rows], e_out.at[1, m, colour], e_local.at[1, colour]).wait()

        for q in range(MEM):
            def wait_for(part):
                remote(
                    values.at[HALO, v_rows], e_out.at[part, q, colour],
                    e_send.at[part, colour, 0], e_recv.at[part, colour, q], g, q,
                ).wait_recv()

            @pl.when(m != q)
            def _():
                wait_for(0)

            last = m == MEM - 1
            arrives = jnp.logical_or(
                jnp.logical_and(jnp.logical_not(last), m != q), jnp.logical_and(last, g < groups - 1)
            )

            @pl.when(arrives)
            def _():
                wait_for(1)
    for copy, sends in e_copies:
        if sends is None:
            copy.wait_send()
        else:
            @pl.when(sends)
            def _():
                copy.wait_send()


def smooth(potential, source, side_faces, end_faces):
    dma = pltpu.SemaphoreType.DMA
    anyspace = pl.BlockSpec(memory_space=pl.ANY)
    return pl.pallas_call(
        smooth_kernel,
        out_shape=jax.ShapeDtypeStruct((2, MEM, 2, ROWS, 128), F32),
        in_specs=[anyspace, anyspace, pl.BlockSpec(memory_space=pltpu.VMEM), anyspace],
        out_specs=anyspace,
        scratch_shapes=[
            pltpu.VMEM((2, 4, NF + 16, 128), F32),
            pltpu.VMEM((2, 4, NF + 16, 128), F32),
            pltpu.VMEM((NC, NC), F32),
            pltpu.VMEM((NF, NC), BF16),
            pltpu.VMEM((NF, NC), BF16),
            pltpu.VMEM((NC, NC), BF16),
            pltpu.VMEM((3, MEM, 2, ROWS, 128), F32),
            pltpu.VMEM((MEM, 2, ROWS, 128), F32),
            pltpu.VMEM((MEM, 2, ROWS, 128), F32),
            pltpu.VMEM((SLOTS, 2, FROWS, 128), F32),
            pltpu.VMEM((MEM, 2, ROWS, 128), F32),
            pltpu.VMEM((SLOTS, VROWS, 128), F32),
            pltpu.VMEM((SLOTS, VROWS, 128), F32),
            pltpu.VMEM((SLOTS, VROWS, 128), F32),
            pltpu.VMEM((3, FROWS, 128), F32),
            dma((4, 2)),
            dma,
            dma((CHUNKS,)),
            dma((CHUNKS,)),
            dma((CHUNKS, 2)),
            dma((MEM,)),
            dma((CHUNKS, 2)),
            dma((MEM,)),
            dma((8,)),
            dma((8,)),
            dma((8,)),
            dma((8,)),
            dma((2, 2, MEM)),
            dma((2, 2, MEM)),
            dma((2, 2)),
        ],
        compiler_params=pltpu.CompilerParams(collective_id=0, has_side_effects=True),
        name="smooth",
    )(potential, source, side_faces, end_faces)


def prolong_kernel(e, p, corrected, correction, w_fine, w_plain):
    groups = lax.axis_size("grp")
    device = lax.axis_index("grp") * MEM + lax.axis_index("mem")
    is_last = device == groups * MEM - 1
    c = pl.program_id(0)
    blocks = CROWS // ROWS

    @pl.when(c == 0)
    def _():
        column = coarse_column((NC, NF), 0)
        fine = iota((NC, NF), 1)
        step = fine - 2 * column
        whole = jnp.logical_or(step == 0, jnp.logical_and(step == 1, column == NC - 1))
        half = jnp.logical_or(step == 1, step == -1)
        w_fine[...] = jnp.where(whole, 1.0, jnp.where(half, 0.5, 0.0)).astype(BF16)
        w_plain[...] = jnp.where(
            iota((NC, NC), 1) == coarse_column((NC, NC), 0), 1.0, 0.0
        ).astype(BF16)

    def by_column(part, shift, red, black):
        row = iota(red.shape, 0)
        even = lax.rem(row + shift + device, 2) == 0
        return jnp.concatenate([jnp.where(even, red, black), jnp.where(even, black, red)], axis=1)

    def rows_of(part):
        here = [by_column(part, part, e[part, c * blocks + b, 0], e[part, c * blocks + b, 1]) for b in range(blocks)]
        q = jnp.minimum(c * blocks + blocks, MEM - 1)
        after = by_column(part, part, e[part, q, 0, 0:8, :], e[part, q, 1, 0:8, :])
        return jnp.concatenate(here, axis=0), after

    here, after = rows_of(0)
    here_up, after_up = rows_of(1)
    at_bottom = c == CHUNKS - 1

    r = iota((FINE, CROWS), 0)
    k = iota((FINE, CROWS), 1)
    last_row = jnp.logical_and(jnp.logical_and(r == FINE - 1, k == CROWS - 1), at_bottom)
    take = jnp.where(
        jnp.logical_or(r == 2 * k, last_row), 1.0,
        jnp.where(jnp.logical_or(r == 2 * k + 1, r == 2 * k - 1), 0.5, 0.0),
    ).astype(BF16)

    def down(x, next_rows):
        parts = jnp.concatenate(split3(x), axis=1)
        out = jnp.dot(take, parts, preferred_element_type=F32)
        out = out[:, :NC] + (out[:, NC : 2 * NC] + out[:, 2 * NC :])
        carry = jnp.where(at_bottom, 0.0, 0.5 * next_rows[0:1, :])
        return out + jnp.where(iota((FINE, NC), 0) == FINE - 1, carry, 0.0)

    above = jnp.where(is_last, here, 0.5 * (here + here_up))
    above_after = jnp.where(is_last, after, 0.5 * (after + after_up))
    corrected[0] = p[0] + dot_exact(down(here, after), w_fine[...])
    corrected[1] = p[1] + dot_exact(down(above, above_after), w_fine[...])
    correction[0] = dot_exact(here, w_plain[...])


def prolong(e, potential):
    return pl.pallas_call(
        prolong_kernel,
        grid=(CHUNKS,),
        out_shape=(
            jax.ShapeDtypeStruct((2, NF, NF), F32),
            jax.ShapeDtypeStruct((1, NC, NC), F32),
        ),
        in_specs=[
            pl.BlockSpec((2, MEM, 2, ROWS, 128), lambda c: (0, 0, 0, 0, 0)),
            pl.BlockSpec((2, FINE, NF), lambda c: (0, c, 0)),
        ],
        out_specs=(
            pl.BlockSpec((2, FINE, NF), lambda c: (0, c, 0)),
            pl.BlockSpec((1, CROWS, NC), lambda c: (0, c, 0)),
        ),
        scratch_shapes=[pltpu.VMEM((NC, NF), BF16), pltpu.VMEM((NC, NC), BF16)],
        name="prolong",
    )(e, potential)


def per_device(potential, source, side_faces, end_faces):
    e = smooth(potential, source, side_faces, end_faces)
    return prolong(e, potential)


def solution(mesh):
    placed = P(("grp", "mem"), None, None)
    return jax.shard_map(
        per_device,
        mesh=mesh,
        in_specs=(placed, placed, placed, P()),
        out_specs=(placed, placed),
        check_vma=False,
    )
```

```python
import jax
import jax.numpy as jnp
from jax import lax
from jax.experimental import pallas as pl
from jax.experimental.pallas import tpu as pltpu
from jax.sharding import PartitionSpec as P

F32 = jnp.float32
BF16 = jnp.bfloat16
MESH = pl.DeviceIdType.MESH

NF = 512
NC = 256
MEM = 8
ROWS = NC // MEM
HALO = 8
SLOTS = MEM + 2 * HALO
FROWS = ROWS + 2 * HALO
VROWS = FROWS + 16
CHUNKS = 4
CROWS = NC // CHUNKS
FINE = 2 * CROWS


def iota(shape, dim):
    return lax.broadcasted_iota(jnp.int32, shape, dim)


def split3(x):
    high = x.astype(BF16)
    rest = x - high.astype(F32)
    middle = rest.astype(BF16)
    low = (rest - middle.astype(F32)).astype(BF16)
    return high, middle, low


def dot_exact(x, weights):
    rows = x.shape[0]
    parts = jnp.concatenate(split3(x), axis=0)
    out = jnp.dot(parts, weights, preferred_element_type=F32)
    return out[:rows] + (out[rows : 2 * rows] + out[2 * rows :])


def coarse_column(shape, dim):
    n = iota(shape, dim)
    return jnp.where(n < NC // 2, 2 * n, 2 * n - (NC - 1))


DIRECTIONS = tuple((dg, dm) for dg in (-1, 0, 1) for dm in (-1, 0, 1) if (dg, dm) != (0, 0))


def smooth_kernel(
    p_hbm, s_hbm, side, end_hbm, e_out, pb,
    sb, eb, w_rc, w_lr, w_perm, fields, partner, summed, fb, xb, vr, vk, vk2, scales,
    in_sems, end_sem, p_send, p_recv, f_send, f_recv, x_send, x_recv, h_send, h_recv, b_send, b_recv,
    e_send, e_recv,
):
    groups = lax.axis_size("grp")
    g = lax.axis_index("grp")
    m = lax.axis_index("mem")
    device = g * MEM + m
    is_first = device == 0
    is_last = device == groups * MEM - 1
    at_end = jnp.logical_or(is_first, is_last)

    def remote(src, dst, send, recv, tg, tm):
        return pltpu.make_async_remote_copy(
            src_ref=src, dst_ref=dst, send_sem=send, recv_sem=recv,
            device_id={"grp": tg, "mem": tm}, device_id_type=MESH,
        )

    in_copies = []
    for t in range(4):
        for a, (src, dst) in enumerate(((p_hbm, pb), (s_hbm, sb))):
            in_copies.append(
                pltpu.make_async_copy(
                    src.at[:, :, pl.ds(128 * t, 128)], dst.at[:, t, pl.ds(8, NF), :], in_sems.at[t, a]
                )
            )
    for copy in in_copies:
        copy.start()
    end_copy = pltpu.make_async_copy(end_hbm.at[jnp.where(is_last, 1, 0)], eb, end_sem)

    @pl.when(at_end)
    def _():
        end_copy.start()

    vk2[...] = jnp.zeros_like(vk2)
    fb[...] = jnp.zeros_like(fb)
    xb[...] = jnp.zeros_like(xb)

    barrier = pltpu.get_barrier_semaphore()
    for dg in (-1, 0, 1):
        exists = jnp.logical_and(g + dg >= 0, g + dg < groups)

        @pl.when(exists)
        def _():
            for i in range(1 if dg == 0 else 0, MEM):
                pl.semaphore_signal(
                    barrier, inc=1,
                    device_id={"grp": g + dg, "mem": lax.rem(m + i, MEM)}, device_id_type=MESH,
                )

    vr[...] = jnp.zeros_like(vr)
    vk[...] = jnp.zeros_like(vk)
    row = m * ROWS - HALO + iota((FROWS, 128), 0)
    inner = jnp.where(jnp.logical_and(row >= 0, row < NC), 1.0 / 6.0, 0.0)
    scales[0] = jnp.where(g > 0, inner, 0.0)
    scales[1] = inner
    scales[2] = jnp.where(g < groups - 1, inner, 0.0)

    zeros = jnp.zeros((2, 4, 8, 128), F32)
    pb[:, :, 0:8, :] = zeros
    pb[:, :, 8 + NF : 16 + NF, :] = zeros
    sb[:, :, 0:8, :] = zeros

    column = coarse_column((NF, NC), 1)
    step = jnp.abs(iota((NF, NC), 0) - 2 * column)
    w_rc[...] = jnp.where(step == 0, 0.5, jnp.where(step == 1, 0.25, 0.0)).astype(BF16)
    near = jnp.where(step == 0, jnp.where(column == 0, 0.25, 0.5), 0.5)
    w_lr[...] = jnp.where(step <= 1, near, jnp.where(step == 2, 0.25, 0.0)).astype(BF16)
    square = coarse_column((NC, NC), 1)
    w_perm[...] = jnp.where(iota((NC, NC), 0) == square, 1.0, 0.0).astype(BF16)

    front = dot_exact(jnp.broadcast_to(side[0, 0:1, :], (8, NC)), w_perm[...])[0:1]
    back = dot_exact(jnp.broadcast_to(side[0, 1:2, :], (8, NC)), w_perm[...])[0:1]
    own_weight = jnp.where(is_first, 0.25, 0.5)
    for copy in in_copies:
        copy.wait()

    blocks = CROWS // ROWS

    def by_colour(value, shift):
        even = lax.rem(iota((CROWS, 128), 0) + device + shift, 2) == 0
        left, right = value[:, :128], value[:, 128:]
        return jnp.where(even, left, right), jnp.where(even, right, left)

    def restrict(c):
        lists = [[], [], [], [], []]
        row = CROWS * c + iota((CROWS, 128), 0)
        for t in range(4):

            def load(ref, plane, shift):
                return ref[plane, t, pl.ds(8 + FINE * c + shift, CROWS, stride=2), :]

            a, b = [], []
            for plane in (0, 1):
                p_before, p_here, p_after = (load(pb, plane, k) for k in (-1, 0, 1))
                outer = load(pb, plane, -2) + load(pb, plane, 2)
                odd = p_before + p_after
                s_part = 0.5 * load(sb, plane, 0) + 0.25 * (load(sb, plane, -1) + load(sb, plane, 1))
                value = s_part + (outer - 4.0 * odd - 10.0 * p_here)
                a.append(value - jnp.where(row == 0, p_here, 0.0))
                b.append(2.0 * p_here + odd)
            up = 0.25 * a[1] + 0.5 * b[1]
            lists[0].append(0.5 * a[0] + up + own_weight * b[0])
            lists[1].append(up + 0.25 * b[0])
            lists[2].append(0.25 * b[0])
            lists[3].append(0.5 * b[0] + 0.25 * b[1])
            lists[4].append(0.25 * b[1])
        wide = [jnp.concatenate(f, axis=1) for f in lists]
        plain = dot_exact(jnp.concatenate(wide[:3], axis=0), w_rc[...])
        cross = dot_exact(jnp.concatenate(wide[3:], axis=0), w_lr[...])
        local = plain[:CROWS] + cross[:CROWS]
        above = plain[CROWS : 2 * CROWS] + cross[CROWS:]
        below = plain[2 * CROWS :]
        row = CROWS * c + iota((CROWS, NC), 0)
        lane = iota((CROWS, NC), 1)
        left = jnp.sum(jnp.where(lane == row, side[0, 2:3, :], 0.0), axis=1, keepdims=True)
        right = jnp.sum(jnp.where(lane == row, side[0, 3:4, :], 0.0), axis=1, keepdims=True)
        local = local + jnp.where(lane == 0, left, jnp.where(lane == NC - 1, right, 0.0))
        local = local + jnp.where(row == 0, front, jnp.where(row == NC - 1, back, 0.0))
        for field, value in ((0, local), (1, above), (2, below)):
            for colour, part in enumerate(by_colour(value, int(field > 0))):
                for b in range(blocks):
                    fields[field, c * blocks + b, colour] = part[ROWS * b : ROWS * (b + 1)]

    def add_end_face(c):
        face = dot_exact(eb[pl.ds(pl.multiple_of(CROWS * c, CROWS), CROWS), :], w_perm[...])
        for colour, part in enumerate(by_colour(face, 0)):
            for b in range(blocks):
                q = c * blocks + b
                fields[0, q, colour] = fields[0, q, colour] + part[ROWS * b : ROWS * (b + 1)]

    odd = lax.rem(m, 2)
    x_group = g - jnp.where(m == 0, 1, 0) + jnp.where(m == MEM - 1, 1, 0)
    x_plane = lax.rem(m + jnp.where(odd == 1, 1, MEM - 1), MEM)
    x_field = 2 - odd
    x_valid = jnp.logical_and(x_group >= 0, x_group < groups)
    x_home = x_group == g
    own_rows = pl.ds(HALO, ROWS)
    sent = []

    def send_if(condition, copy):
        sent.append((condition, copy))

        @pl.when(condition)
        def _():
            copy.start()

    def send_fields(i, c):
        part = pl.ds(c * blocks, blocks)
        copy = remote(
            fields.at[1 + odd, part], partner.at[part], p_send.at[i], p_recv.at[i], g, m + 1 - 2 * odd
        )
        copy.start()
        for b in range(blocks):
            q = c * blocks + b
            home = jnp.logical_and(x_home, q == m)
            send_if(
                jnp.logical_and(x_valid, jnp.logical_not(home)),
                remote(
                    fields.at[x_field, q], xb.at[x_plane], x_send.at[i, b], x_recv.at[x_plane], x_group, q
                ),
            )

            @pl.when(home)
            def _():
                xb[x_plane] = fields[x_field, q]
        return copy

    def send_sums(i, c, to_partner):
        to_partner.wait_recv()
        for b in range(blocks):
            q = c * blocks + b
            summed[q] = fields[0, q] + partner[q]
            send_if(
                q != m,
                remote(summed.at[q], fb.at[HALO + m, :, own_rows], f_send.at[i, b], f_recv.at[m], g, q),
            )

            @pl.when(q == m)
            def _():
                fb[HALO + m, :, HALO : HALO + ROWS, :] = summed[q]

    @pl.when(at_end)
    def _():
        end_copy.wait()

    partners = []
    for i in range(CHUNKS):
        c = lax.rem(m // blocks + 1 + i, CHUNKS)
        restrict(c)

        @pl.when(at_end)
        def _():
            add_end_face(c)

        if i == 0:
            count = (MEM - 1) + jnp.where(g > 0, MEM, 0) + jnp.where(g < groups - 1, MEM, 0)
            pl.semaphore_wait(barrier, count)
        partners.append(send_fields(i, c))
        if i > 0:
            send_sums(i - 1, lax.rem(m // blocks + i, CHUNKS), partners[i - 1])
    send_sums(CHUNKS - 1, m // blocks, partners[-1])

    def inside(dg, dm):
        ok = None
        for test in (
            (g + dg >= 0) if dg < 0 else (g + dg < groups) if dg > 0 else None,
            (m + dm >= 0) if dm < 0 else (m + dm < MEM) if dm > 0 else None,
        ):
            if test is not None:
                ok = test if ok is None else jnp.logical_and(ok, test)
        return ok

    def exchange(make):
        copies = []
        for o, (dg, dm) in enumerate(DIRECTIONS):
            copy = make(o, dg, dm)
            copies.append(copy)

            @pl.when(inside(dg, dm))
            def _():
                copy.start()
        return copies

    def arrive(copies):
        for o, (dg, dm) in enumerate(DIRECTIONS):
            @pl.when(inside(-dg, -dm))
            def _():
                copies[o].wait_recv()

    def row_parts(dm, base):
        if dm < 0:
            return pl.ds(base, HALO), pl.ds(base + ROWS, HALO)
        if dm > 0:
            return pl.ds(base + ROWS - HALO, HALO), pl.ds(base - HALO, HALO)
        return pl.ds(base, ROWS), pl.ds(base, ROWS)

    def plane_parts(dg, depth):
        if dg < 0:
            return pl.ds(HALO, depth), pl.ds(HALO + MEM, depth)
        if dg > 0:
            return pl.ds(HALO + MEM - depth, depth), pl.ds(HALO - depth, depth)
        return pl.ds(HALO, MEM), pl.ds(HALO, MEM)

    def forcing_copy(o, dg, dm, k=None):
        src_rows, dst_rows = row_parts(dm, HALO)
        if k is None:
            src, dst = plane_parts(dg, HALO - 1 - abs(dm))
        else:
            src, dst = HALO + k, HALO + k - MEM * dg
        return remote(
            fb.at[src, :, src_rows], fb.at[dst, :, dst_rows], h_send.at[o], h_recv.at[o], g + dg, m + dm
        )

    def receive(n, carry):
        back = jnp.where(n == 0, 1, jnp.where(n < 3, 2, jnp.where(n < 5, 3, jnp.where(n < 7, 0, 1))))
        second = jnp.where(n < 7, jnp.where(n < 5, lax.rem(n, 2) == 1, n == 6), True)
        k = lax.rem(m // blocks + CHUNKS - back, CHUNKS) * blocks + jnp.where(second, 1, 0)

        @pl.when(m != k)
        def _():
            remote(summed.at[0], fb.at[HALO + k, :, own_rows], f_send.at[0, 0], f_recv.at[k], g, k).wait_recv()

        arrives = jnp.logical_not(jnp.logical_and(x_home, x_plane == k))
        arrives = jnp.logical_and(arrives, jnp.logical_or(k > 0, g > 0))
        arrives = jnp.logical_and(arrives, jnp.logical_or(k < MEM - 1, g < groups - 1))

        @pl.when(arrives)
        def _():
            remote(fields.at[0, 0], xb.at[k], x_send.at[0, 0], x_recv.at[k], g, k).wait_recv()

        fb[HALO + k, :, HALO : HALO + ROWS, :] = fb[HALO + k, :, HALO : HALO + ROWS, :] + xb[k]
        for o, (dg, dm) in enumerate(DIRECTIONS):
            depth = HALO - 1 - abs(dm)
            needed = inside(dg, dm)
            if dg < 0:
                needed = jnp.logical_and(needed, k < depth)
            if dg > 0:
                needed = jnp.logical_and(needed, k >= MEM - depth)

            @pl.when(needed)
            def _():
                forcing_copy(o, dg, dm, k).start()
        return carry

    def black_copy(o, dg, dm):
        src_rows, dst_rows = row_parts(dm, HALO + 8)
        src_planes, dst_planes = plane_parts(dg, HALO - abs(dm))
        return remote(
            vk2.at[src_planes, src_rows], vk2.at[dst_planes, dst_rows],
            b_send.at[o], b_recv.at[o], g + dg, m + dm,
        )

    lax.fori_loop(0, MEM, receive, 0)
    h_copies = [forcing_copy(o, dg, dm) for o, (dg, dm) in enumerate(DIRECTIONS)]
    arrive(h_copies)

    lane = iota((8, 128), 1)
    row_parity = lax.rem(iota((8, 128), 0), 2)
    from_left = [
        (jnp.logical_and(row_parity == flip, lane != 0), jnp.logical_and(row_parity != flip, lane != 127))
        for flip in (0, 1)
    ]

    def half_sweep(colour, t, target, source, first=0, tiles=FROWS // 8):
        at, n = 8 + 8 * first, 8 * tiles
        shape = (tiles, 8, 128)
        for slot in range(t, SLOTS - t):
            centre = source[slot, at : at + n, :].reshape(shape)
            keep_left, keep_right = from_left[(slot + colour) % 2]
            beside = jnp.where(
                jnp.broadcast_to(keep_left, shape), pltpu.roll(centre, 1, 2),
                jnp.where(jnp.broadcast_to(keep_right, shape), pltpu.roll(centre, 127, 2), 0.0),
            )
            rows = source[slot, at - 1 : at - 1 + n, :] + source[slot, at + 1 : at + 1 + n, :]
            depth = source[slot - 1, at : at + n, :] + source[slot + 1, at : at + n, :]
            side = 0 if slot < HALO else 2 if slot >= HALO + MEM else 1
            near = (depth + rows).reshape(shape) + (centre + beside)
            total = fb[slot, colour, 8 * first : 8 * first + n, :].reshape(shape) + near
            total = total * scales[side, 8 * first : 8 * first + n, :].reshape(shape)
            target[slot, at : at + n, :] = total.reshape(n, 128)

    def sweeps(black):
        for t in (1, 3, 5):
            half_sweep(0, t, vr, black)
            half_sweep(1, t + 1, black, vr)
        half_sweep(0, 7, vr, black)

    sweeps(vk)
    half_sweep(1, 8, vk2, vr, 1, ROWS // 8)
    b_copies = exchange(black_copy)
    arrive(b_copies)
    for o, (dg, dm) in enumerate(DIRECTIONS):
        @pl.when(inside(dg, dm))
        def _():
            b_copies[o].wait_send()
    sweeps(vk2)

    v_rows = pl.ds(HALO + 8, ROWS)
    e_copies = []

    def send_back(colour, values):
        for i in range(MEM):
            tm = lax.rem(m + i, MEM)
            if i == 0:
                e_out[0, m, colour] = values[HALO + m, HALO + 8 : HALO + 8 + ROWS, :]
            else:
                copy = remote(
                    values.at[HALO + tm, v_rows], e_out.at[0, m, colour],
                    e_send.at[0, colour, i], e_recv.at[0, colour, m], g, tm,
                )
                copy.start()
                e_copies.append((copy, None))
            wraps = tm == MEM - 1
            plane = HALO + jnp.where(wraps, 0, tm + 1)
            tg = g - jnp.where(wraps, 1, 0)
            copy = remote(
                values.at[plane, v_rows], e_out.at[1, m, colour],
                e_send.at[1, colour, i], e_recv.at[1, colour, m], tg, tm,
            )
            if i == 0:
                sends = jnp.logical_and(wraps, g > 0)

                @pl.when(jnp.logical_not(wraps))
                def _():
                    e_out[1, m, colour] = values[plane, HALO + 8 : HALO + 8 + ROWS, :]
            else:
                sends = jnp.logical_not(jnp.logical_and(wraps, g == 0))
            e_copies.append((copy, sends))

            @pl.when(sends)
            def _():
                copy.start()

    send_back(0, vr)
    half_sweep(1, 8, vk2, vr, 1, ROWS // 8)
    send_back(1, vk2)

    for copy in partners:
        copy.wait_send()
    for condition, copy in sent:
        @pl.when(condition)
        def _():
            copy.wait_send()
    for o, (dg, dm) in enumerate(DIRECTIONS):
        @pl.when(inside(dg, dm))
        def _():
            h_copies[o].wait_send()
    for colour, values in ((0, vr), (1, vk2)):
        for q in range(MEM):
            def wait_for(part):
                remote(
                    values.at[HALO, v_rows], e_out.at[part, q, colour],
                    e_send.at[part, colour, 0], e_recv.at[part, colour, q], g, q,
                ).wait_recv()

            @pl.when(m != q)
            def _():
                wait_for(0)

            last = m == MEM - 1
            arrives = jnp.logical_or(
                jnp.logical_and(jnp.logical_not(last), m != q), jnp.logical_and(last, g < groups - 1)
            )

            @pl.when(arrives)
            def _():
                wait_for(1)
    for copy, sends in e_copies:
        if sends is None:
            copy.wait_send()
        else:
            @pl.when(sends)
            def _():
                copy.wait_send()


def smooth(potential, source, side_faces, end_faces):
    dma = pltpu.SemaphoreType.DMA
    anyspace = pl.BlockSpec(memory_space=pltpu.HBM)
    return pl.pallas_call(
        smooth_kernel,
        out_shape=(pltpu.VMEM((2, MEM, 2, ROWS, 128), F32), pltpu.VMEM((2, 4, NF + 16, 128), F32)),
        in_specs=[anyspace, anyspace, pl.BlockSpec(memory_space=pltpu.VMEM), anyspace],
        out_specs=(pl.BlockSpec(memory_space=pltpu.VMEM), pl.BlockSpec(memory_space=pltpu.VMEM)),
        scratch_shapes=[
            pltpu.VMEM((2, 4, NF + 16, 128), F32),
            pltpu.VMEM((NC, NC), F32),
            pltpu.VMEM((NF, NC), BF16),
            pltpu.VMEM((NF, NC), BF16),
            pltpu.VMEM((NC, NC), BF16),
            pltpu.VMEM((3, MEM, 2, ROWS, 128), F32),
            pltpu.VMEM((MEM, 2, ROWS, 128), F32),
            pltpu.VMEM((MEM, 2, ROWS, 128), F32),
            pltpu.VMEM((SLOTS, 2, FROWS, 128), F32),
            pltpu.VMEM((MEM, 2, ROWS, 128), F32),
            pltpu.VMEM((SLOTS, VROWS, 128), F32),
            pltpu.VMEM((SLOTS, VROWS, 128), F32),
            pltpu.VMEM((SLOTS, VROWS, 128), F32),
            pltpu.VMEM((3, FROWS, 128), F32),
            dma((4, 2)),
            dma,
            dma((CHUNKS,)),
            dma((CHUNKS,)),
            dma((CHUNKS, 2)),
            dma((MEM,)),
            dma((CHUNKS, 2)),
            dma((MEM,)),
            dma((8,)),
            dma((8,)),
            dma((8,)),
            dma((8,)),
            dma((2, 2, MEM)),
            dma((2, 2, MEM)),
        ],
        compiler_params=pltpu.CompilerParams(collective_id=0, has_side_effects=True),
        name="smooth",
    )(potential, source, side_faces, end_faces)


def prolong_kernel(e, p, corrected, correction, w_fine, w_plain, fine, coarse, sems):
    groups = lax.axis_size("grp")
    device = lax.axis_index("grp") * MEM + lax.axis_index("mem")
    is_last = device == groups * MEM - 1
    blocks = CROWS // ROWS

    column = coarse_column((NC, NF), 0)
    step = iota((NC, NF), 1) - 2 * column
    whole = jnp.logical_or(step == 0, jnp.logical_and(step == 1, column == NC - 1))
    half = jnp.logical_or(step == 1, step == -1)
    w_fine[...] = jnp.where(whole, 1.0, jnp.where(half, 0.5, 0.0)).astype(BF16)
    w_plain[...] = jnp.where(iota((NC, NC), 1) == coarse_column((NC, NC), 0), 1.0, 0.0).astype(BF16)

    def by_column(part, red, black):
        even = lax.rem(iota(red.shape, 0) + part + device, 2) == 0
        return jnp.concatenate([jnp.where(even, red, black), jnp.where(even, black, red)], axis=1)

    def rows_of(part, c):
        here = [by_column(part, e[part, c * blocks + b, 0], e[part, c * blocks + b, 1]) for b in range(blocks)]
        q = min(c * blocks + blocks, MEM - 1)
        after = by_column(part, e[part, q, 0, 0:8, :], e[part, q, 1, 0:8, :])
        return jnp.concatenate(here, axis=0), after

    r = iota((FINE, CROWS), 0)
    k = iota((FINE, CROWS), 1)
    halves = jnp.logical_or(r == 2 * k + 1, r == 2 * k - 1)
    copies = []
    for c in range(CHUNKS):
        at_bottom = c == CHUNKS - 1
        wholes = r == 2 * k
        if at_bottom:
            wholes = jnp.logical_or(wholes, jnp.logical_and(r == FINE - 1, k == CROWS - 1))
        take = jnp.where(wholes, 1.0, jnp.where(halves, 0.5, 0.0)).astype(BF16)

        def down(x, next_rows):
            parts = jnp.concatenate(split3(x), axis=1)
            out = jnp.dot(take, parts, preferred_element_type=F32)
            out = out[:, :NC] + (out[:, NC : 2 * NC] + out[:, 2 * NC :])
            if at_bottom:
                return out
            return out + jnp.where(iota((FINE, NC), 0) == FINE - 1, 0.5 * next_rows[0:1, :], 0.0)

        here, after = rows_of(0, c)
        here_up, after_up = rows_of(1, c)
        above = jnp.where(is_last, here, 0.5 * (here + here_up))
        above_after = jnp.where(is_last, after, 0.5 * (after + after_up))
        rows = pl.ds(FINE * c, FINE)
        for plane, (x, next_rows) in enumerate(((here, after), (above, above_after))):
            refined = dot_exact(down(x, next_rows), w_fine[...])
            for t in range(4):
                lanes = slice(128 * t, 128 * t + 128)
                fine[plane, rows, lanes] = p[plane, t, pl.ds(8 + FINE * c, FINE), :] + refined[:, lanes]
            copy = pltpu.make_async_copy(fine.at[plane, rows], corrected.at[plane, rows], sems.at[c, plane])
            copy.start()
            copies.append(copy)
        rows = pl.ds(CROWS * c, CROWS)
        coarse[rows, :] = dot_exact(here, w_plain[...])
        copy = pltpu.make_async_copy(coarse.at[rows], correction.at[0, rows], sems.at[c, 2])
        copy.start()
        copies.append(copy)
    for copy in copies:
        copy.wait()


def prolong(e, potential):
    vmem = pl.BlockSpec(memory_space=pltpu.VMEM)
    anyspace = pl.BlockSpec(memory_space=pl.ANY)
    return pl.pallas_call(
        prolong_kernel,
        out_shape=(
            jax.ShapeDtypeStruct((2, NF, NF), F32),
            jax.ShapeDtypeStruct((1, NC, NC), F32),
        ),
        in_specs=[vmem, vmem],
        out_specs=(anyspace, anyspace),
        scratch_shapes=[
            pltpu.VMEM((NC, NF), BF16),
            pltpu.VMEM((NC, NC), BF16),
            pltpu.VMEM((2, NF, NF), F32),
            pltpu.VMEM((NC, NC), F32),
            pltpu.SemaphoreType.DMA((CHUNKS, 3)),
        ],
        compiler_params=pltpu.CompilerParams(vmem_limit_bytes=24 * 2**20),
        name="prolong",
    )(*(pltpu.with_memory_space_constraint(x, pltpu.VMEM) for x in (e, potential)))


def per_device(potential, source, side_faces, end_faces):
    e, kept = smooth(potential, source, side_faces, end_faces)
    return prolong(e, kept)


def solution(mesh):
    placed = P(("grp", "mem"), None, None)
    return jax.shard_map(
        per_device,
        mesh=mesh,
        in_specs=(placed, placed, placed, P()),
        out_specs=(placed, placed),
        check_vma=False,
    )
```

```python
import jax
import jax.numpy as jnp
from jax import lax
from jax.experimental import pallas as pl
from jax.experimental.pallas import tpu as pltpu
from jax.sharding import PartitionSpec as P

F32 = jnp.float32
BF16 = jnp.bfloat16
MESH = pl.DeviceIdType.MESH

NF = 512
NC = 256
MEM = 8
ROWS = NC // MEM
HALO = 8
SLOTS = MEM + 2 * HALO
FROWS = ROWS + 2 * HALO
VROWS = FROWS + 16
CHUNKS = 4
CROWS = NC // CHUNKS
FINE = 2 * CROWS


def iota(shape, dim):
    return lax.broadcasted_iota(jnp.int32, shape, dim)


def split3(x):
    high = x.astype(BF16)
    rest = x - high.astype(F32)
    middle = rest.astype(BF16)
    low = (rest - middle.astype(F32)).astype(BF16)
    return high, middle, low


def dot_exact(x, weights):
    rows = x.shape[0]
    parts = jnp.concatenate(split3(x), axis=0)
    out = jnp.dot(parts, weights, preferred_element_type=F32)
    return out[:rows] + (out[rows : 2 * rows] + out[2 * rows :])


def coarse_column(shape, dim):
    n = iota(shape, dim)
    return jnp.where(n < NC // 2, 2 * n, 2 * n - (NC - 1))


DIRECTIONS = tuple((dg, dm) for dg in (-1, 0, 1) for dm in (-1, 0, 1) if (dg, dm) != (0, 0))


def smooth_kernel(
    p_hbm, s_hbm, side, end_hbm, e_out, pb, w_fine, w_plain,
    sb, eb, w_rc, w_lr, w_perm, fields, partner, summed, fb, xb, vr, vk, vk2, scales,
    in_sems, end_sem, p_send, p_recv, f_send, f_recv, x_send, x_recv, h_send, h_recv, b_send, b_recv,
    e_send, e_recv,
):
    groups = lax.axis_size("grp")
    g = lax.axis_index("grp")
    m = lax.axis_index("mem")
    device = g * MEM + m
    is_first = device == 0
    is_last = device == groups * MEM - 1
    at_end = jnp.logical_or(is_first, is_last)

    def remote(src, dst, send, recv, tg, tm):
        return pltpu.make_async_remote_copy(
            src_ref=src, dst_ref=dst, send_sem=send, recv_sem=recv,
            device_id={"grp": tg, "mem": tm}, device_id_type=MESH,
        )

    in_copies = []
    for t in range(4):
        for a, (src, dst) in enumerate(((p_hbm, pb), (s_hbm, sb))):
            in_copies.append(
                pltpu.make_async_copy(
                    src.at[:, :, pl.ds(128 * t, 128)], dst.at[:, t, pl.ds(8, NF), :], in_sems.at[t, a]
                )
            )
    for copy in in_copies:
        copy.start()
    end_copy = pltpu.make_async_copy(end_hbm.at[jnp.where(is_last, 1, 0)], eb, end_sem)

    @pl.when(at_end)
    def _():
        end_copy.start()

    vk2[...] = jnp.zeros_like(vk2)
    fb[...] = jnp.zeros_like(fb)
    xb[...] = jnp.zeros_like(xb)

    barrier = pltpu.get_barrier_semaphore()
    for dg in (-1, 0, 1):
        exists = jnp.logical_and(g + dg >= 0, g + dg < groups)

        @pl.when(exists)
        def _():
            for i in range(1 if dg == 0 else 0, MEM):
                pl.semaphore_signal(
                    barrier, inc=1,
                    device_id={"grp": g + dg, "mem": lax.rem(m + i, MEM)}, device_id_type=MESH,
                )

    vr[...] = jnp.zeros_like(vr)
    vk[...] = jnp.zeros_like(vk)
    row = m * ROWS - HALO + iota((FROWS, 128), 0)
    inner = jnp.where(jnp.logical_and(row >= 0, row < NC), 1.0 / 6.0, 0.0)
    scales[0] = jnp.where(g > 0, inner, 0.0)
    scales[1] = inner
    scales[2] = jnp.where(g < groups - 1, inner, 0.0)

    zeros = jnp.zeros((2, 4, 8, 128), F32)
    pb[:, :, 0:8, :] = zeros
    pb[:, :, 8 + NF : 16 + NF, :] = zeros
    sb[:, :, 0:8, :] = zeros

    column = coarse_column((NF, NC), 1)
    step = jnp.abs(iota((NF, NC), 0) - 2 * column)
    w_rc[...] = jnp.where(step == 0, 0.5, jnp.where(step == 1, 0.25, 0.0)).astype(BF16)
    near = jnp.where(step == 0, jnp.where(column == 0, 0.25, 0.5), 0.5)
    w_lr[...] = jnp.where(step <= 1, near, jnp.where(step == 2, 0.25, 0.0)).astype(BF16)
    square = coarse_column((NC, NC), 1)
    w_perm[...] = jnp.where(iota((NC, NC), 0) == square, 1.0, 0.0).astype(BF16)

    front = dot_exact(jnp.broadcast_to(side[0, 0:1, :], (8, NC)), w_perm[...])[0:1]
    back = dot_exact(jnp.broadcast_to(side[0, 1:2, :], (8, NC)), w_perm[...])[0:1]
    own_weight = jnp.where(is_first, 0.25, 0.5)
    for copy in in_copies:
        copy.wait()

    blocks = CROWS // ROWS

    def by_colour(value, shift):
        even = lax.rem(iota((CROWS, 128), 0) + device + shift, 2) == 0
        left, right = value[:, :128], value[:, 128:]
        return jnp.where(even, left, right), jnp.where(even, right, left)

    def restrict(c):
        lists = [[], [], [], [], []]
        row = CROWS * c + iota((CROWS, 128), 0)
        for t in range(4):

            def load(ref, plane, shift):
                return ref[plane, t, pl.ds(8 + FINE * c + shift, CROWS, stride=2), :]

            a, b = [], []
            for plane in (0, 1):
                p_before, p_here, p_after = (load(pb, plane, k) for k in (-1, 0, 1))
                outer = load(pb, plane, -2) + load(pb, plane, 2)
                odd = p_before + p_after
                s_part = 0.5 * load(sb, plane, 0) + 0.25 * (load(sb, plane, -1) + load(sb, plane, 1))
                value = s_part + (outer - 4.0 * odd - 10.0 * p_here)
                a.append(value - jnp.where(row == 0, p_here, 0.0))
                b.append(2.0 * p_here + odd)
            up = 0.25 * a[1] + 0.5 * b[1]
            lists[0].append(0.5 * a[0] + up + own_weight * b[0])
            lists[1].append(up + 0.25 * b[0])
            lists[2].append(0.25 * b[0])
            lists[3].append(0.5 * b[0] + 0.25 * b[1])
            lists[4].append(0.25 * b[1])
        wide = [jnp.concatenate(f, axis=1) for f in lists]
        plain = dot_exact(jnp.concatenate(wide[:3], axis=0), w_rc[...])
        cross = dot_exact(jnp.concatenate(wide[3:], axis=0), w_lr[...])
        local = plain[:CROWS] + cross[:CROWS]
        above = plain[CROWS : 2 * CROWS] + cross[CROWS:]
        below = plain[2 * CROWS :]
        row = CROWS * c + iota((CROWS, NC), 0)
        lane = iota((CROWS, NC), 1)
        left = jnp.sum(jnp.where(lane == row, side[0, 2:3, :], 0.0), axis=1, keepdims=True)
        right = jnp.sum(jnp.where(lane == row, side[0, 3:4, :], 0.0), axis=1, keepdims=True)
        local = local + jnp.where(lane == 0, left, jnp.where(lane == NC - 1, right, 0.0))
        local = local + jnp.where(row == 0, front, jnp.where(row == NC - 1, back, 0.0))
        for field, value in ((0, local), (1, above), (2, below)):
            for colour, part in enumerate(by_colour(value, int(field > 0))):
                for b in range(blocks):
                    fields[field, c * blocks + b, colour] = part[ROWS * b : ROWS * (b + 1)]

    def add_end_face(c):
        face = dot_exact(eb[pl.ds(pl.multiple_of(CROWS * c, CROWS), CROWS), :], w_perm[...])
        for colour, part in enumerate(by_colour(face, 0)):
            for b in range(blocks):
                q = c * blocks + b
                fields[0, q, colour] = fields[0, q, colour] + part[ROWS * b : ROWS * (b + 1)]

    odd = lax.rem(m, 2)
    x_group = g - jnp.where(m == 0, 1, 0) + jnp.where(m == MEM - 1, 1, 0)
    x_plane = lax.rem(m + jnp.where(odd == 1, 1, MEM - 1), MEM)
    x_field = 2 - odd
    x_valid = jnp.logical_and(x_group >= 0, x_group < groups)
    x_home = x_group == g
    own_rows = pl.ds(HALO, ROWS)
    sent = []

    def send_if(condition, copy):
        sent.append((condition, copy))

        @pl.when(condition)
        def _():
            copy.start()

    def send_fields(i, c):
        part = pl.ds(c * blocks, blocks)
        copy = remote(
            fields.at[1 + odd, part], partner.at[part], p_send.at[i], p_recv.at[i], g, m + 1 - 2 * odd
        )
        copy.start()
        for b in range(blocks):
            q = c * blocks + b
            home = jnp.logical_and(x_home, q == m)
            send_if(
                jnp.logical_and(x_valid, jnp.logical_not(home)),
                remote(
                    fields.at[x_field, q], xb.at[x_plane], x_send.at[i, b], x_recv.at[x_plane], x_group, q
                ),
            )

            @pl.when(home)
            def _():
                xb[x_plane] = fields[x_field, q]
        return copy

    def send_sums(i, c, to_partner):
        to_partner.wait_recv()
        for b in range(blocks):
            q = c * blocks + b
            summed[q] = fields[0, q] + partner[q]
            send_if(
                q != m,
                remote(summed.at[q], fb.at[HALO + m, :, own_rows], f_send.at[i, b], f_recv.at[m], g, q),
            )

            @pl.when(q == m)
            def _():
                fb[HALO + m, :, HALO : HALO + ROWS, :] = summed[q]

    @pl.when(at_end)
    def _():
        end_copy.wait()

    order = [lax.rem(m // blocks + k, CHUNKS) for k in (1, 3, 0, 2)]
    partners = []
    for i, c in enumerate(order):
        restrict(c)

        @pl.when(at_end)
        def _():
            add_end_face(c)

        if i == 0:
            count = (MEM - 1) + jnp.where(g > 0, MEM, 0) + jnp.where(g < groups - 1, MEM, 0)
            pl.semaphore_wait(barrier, count)
        partners.append(send_fields(i, c))
        if i > 0:
            send_sums(i - 1, order[i - 1], partners[i - 1])
    send_sums(CHUNKS - 1, order[-1], partners[-1])

    def inside(dg, dm):
        ok = None
        for test in (
            (g + dg >= 0) if dg < 0 else (g + dg < groups) if dg > 0 else None,
            (m + dm >= 0) if dm < 0 else (m + dm < MEM) if dm > 0 else None,
        ):
            if test is not None:
                ok = test if ok is None else jnp.logical_and(ok, test)
        return ok

    def exchange(make):
        copies = []
        for o, (dg, dm) in enumerate(DIRECTIONS):
            copy = make(o, dg, dm)
            copies.append(copy)

            @pl.when(inside(dg, dm))
            def _():
                copy.start()
        return copies

    def arrive(copies):
        for o, (dg, dm) in enumerate(DIRECTIONS):
            @pl.when(inside(-dg, -dm))
            def _():
                copies[o].wait_recv()

    def row_parts(dm, base):
        if dm < 0:
            return pl.ds(base, HALO), pl.ds(base + ROWS, HALO)
        if dm > 0:
            return pl.ds(base + ROWS - HALO, HALO), pl.ds(base - HALO, HALO)
        return pl.ds(base, ROWS), pl.ds(base, ROWS)

    def plane_parts(dg, depth):
        if dg < 0:
            return pl.ds(HALO, depth), pl.ds(HALO + MEM, depth)
        if dg > 0:
            return pl.ds(HALO + MEM - depth, depth), pl.ds(HALO - depth, depth)
        return pl.ds(HALO, MEM), pl.ds(HALO, MEM)

    def forcing_copy(o, dg, dm, k=None):
        src_rows, dst_rows = row_parts(dm, HALO)
        if k is None:
            src, dst = plane_parts(dg, HALO - 1 - abs(dm))
        else:
            src, dst = HALO + k, HALO + k - MEM * dg
        return remote(
            fb.at[src, :, src_rows], fb.at[dst, :, dst_rows], h_send.at[o], h_recv.at[o], g + dg, m + dm
        )

    def receive(n, carry):
        offset = jnp.where(n < 4, n - 1, jnp.where(n == 4, -2, n - 2))
        k = lax.rem(m // blocks * blocks + offset + MEM, MEM)

        @pl.when(m != k)
        def _():
            remote(summed.at[0], fb.at[HALO + k, :, own_rows], f_send.at[0, 0], f_recv.at[k], g, k).wait_recv()

        arrives = jnp.logical_not(jnp.logical_and(x_home, x_plane == k))
        arrives = jnp.logical_and(arrives, jnp.logical_or(k > 0, g > 0))
        arrives = jnp.logical_and(arrives, jnp.logical_or(k < MEM - 1, g < groups - 1))

        @pl.when(arrives)
        def _():
            remote(fields.at[0, 0], xb.at[k], x_send.at[0, 0], x_recv.at[k], g, k).wait_recv()

        fb[HALO + k, :, HALO : HALO + ROWS, :] = fb[HALO + k, :, HALO : HALO + ROWS, :] + xb[k]
        for o, (dg, dm) in enumerate(DIRECTIONS):
            depth = HALO - 1 - abs(dm)
            needed = inside(dg, dm)
            if dg < 0:
                needed = jnp.logical_and(needed, k < depth)
            if dg > 0:
                needed = jnp.logical_and(needed, k >= MEM - depth)

            @pl.when(needed)
            def _():
                forcing_copy(o, dg, dm, k).start()
        return carry

    def black_copy(o, dg, dm):
        src_rows, dst_rows = row_parts(dm, HALO + 8)
        src_planes, dst_planes = plane_parts(dg, HALO - abs(dm))
        return remote(
            vk2.at[src_planes, src_rows], vk2.at[dst_planes, dst_rows],
            b_send.at[o], b_recv.at[o], g + dg, m + dm,
        )

    lax.fori_loop(0, MEM, receive, 0)
    column = coarse_column((NC, NF), 0)
    step = iota((NC, NF), 1) - 2 * column
    whole = jnp.logical_or(step == 0, jnp.logical_and(step == 1, column == NC - 1))
    half = jnp.abs(step) == 1
    w_fine[...] = jnp.where(whole, 1.0, jnp.where(half, 0.5, 0.0)).astype(BF16)
    w_plain[...] = jnp.where(iota((NC, NC), 1) == coarse_column((NC, NC), 0), 1.0, 0.0).astype(BF16)

    h_copies = [forcing_copy(o, dg, dm) for o, (dg, dm) in enumerate(DIRECTIONS)]
    arrive(h_copies)

    lane = iota((8, 128), 1)
    row_parity = lax.rem(iota((8, 128), 0), 2)
    from_left = [
        (jnp.logical_and(row_parity == flip, lane != 0), jnp.logical_and(row_parity != flip, lane != 127))
        for flip in (0, 1)
    ]

    def half_sweep(colour, t, target, source, first=0, tiles=FROWS // 8):
        at, n = 8 + 8 * first, 8 * tiles
        shape = (tiles, 8, 128)
        for slot in range(t, SLOTS - t):
            centre = source[slot, at : at + n, :].reshape(shape)
            keep_left, keep_right = from_left[(slot + colour) % 2]
            beside = jnp.where(
                jnp.broadcast_to(keep_left, shape), pltpu.roll(centre, 1, 2),
                jnp.where(jnp.broadcast_to(keep_right, shape), pltpu.roll(centre, 127, 2), 0.0),
            )
            rows = source[slot, at - 1 : at - 1 + n, :] + source[slot, at + 1 : at + 1 + n, :]
            depth = source[slot - 1, at : at + n, :] + source[slot + 1, at : at + n, :]
            side = 0 if slot < HALO else 2 if slot >= HALO + MEM else 1
            near = (depth + rows).reshape(shape) + (centre + beside)
            total = fb[slot, colour, 8 * first : 8 * first + n, :].reshape(shape) + near
            total = total * scales[side, 8 * first : 8 * first + n, :].reshape(shape)
            target[slot, at : at + n, :] = total.reshape(n, 128)

    def sweeps(black):
        for t in (1, 3, 5):
            half_sweep(0, t, vr, black)
            half_sweep(1, t + 1, black, vr)
        half_sweep(0, 7, vr, black)

    sweeps(vk)
    half_sweep(1, 8, vk2, vr, 1, ROWS // 8)
    b_copies = exchange(black_copy)
    arrive(b_copies)
    for o, (dg, dm) in enumerate(DIRECTIONS):
        @pl.when(inside(dg, dm))
        def _():
            b_copies[o].wait_send()
    sweeps(vk2)

    v_rows = pl.ds(HALO + 8, ROWS)
    e_copies = []

    def send_back(colour, values):
        for i in range(MEM):
            tm = lax.rem(m + i, MEM)
            if i == 0:
                e_out[0, m, colour] = values[HALO + m, HALO + 8 : HALO + 8 + ROWS, :]
            else:
                copy = remote(
                    values.at[HALO + tm, v_rows], e_out.at[0, m, colour],
                    e_send.at[0, colour, i], e_recv.at[0, colour, m], g, tm,
                )
                copy.start()
                e_copies.append((copy, None))
            wraps = tm == MEM - 1
            plane = HALO + jnp.where(wraps, 0, tm + 1)
            tg = g - jnp.where(wraps, 1, 0)
            copy = remote(
                values.at[plane, v_rows], e_out.at[1, m, colour],
                e_send.at[1, colour, i], e_recv.at[1, colour, m], tg, tm,
            )
            if i == 0:
                sends = jnp.logical_and(wraps, g > 0)

                @pl.when(jnp.logical_not(wraps))
                def _():
                    e_out[1, m, colour] = values[plane, HALO + 8 : HALO + 8 + ROWS, :]
            else:
                sends = jnp.logical_not(jnp.logical_and(wraps, g == 0))
            e_copies.append((copy, sends))

            @pl.when(sends)
            def _():
                copy.start()

    send_back(0, vr)
    half_sweep(1, 8, vk2, vr, 1, ROWS // 8)
    send_back(1, vk2)

    for copy in partners:
        copy.wait_send()
    for condition, copy in sent:
        @pl.when(condition)
        def _():
            copy.wait_send()
    for o, (dg, dm) in enumerate(DIRECTIONS):
        @pl.when(inside(dg, dm))
        def _():
            h_copies[o].wait_send()
    for colour, values in ((0, vr), (1, vk2)):
        for q in range(MEM):
            def wait_for(part):
                remote(
                    values.at[HALO, v_rows], e_out.at[part, q, colour],
                    e_send.at[part, colour, 0], e_recv.at[part, colour, q], g, q,
                ).wait_recv()

            @pl.when(m != q)
            def _():
                wait_for(0)

            last = m == MEM - 1
            arrives = jnp.logical_or(
                jnp.logical_and(jnp.logical_not(last), m != q), jnp.logical_and(last, g < groups - 1)
            )

            @pl.when(arrives)
            def _():
                wait_for(1)
    for copy, sends in e_copies:
        if sends is None:
            copy.wait_send()
        else:
            @pl.when(sends)
            def _():
                copy.wait_send()


def smooth(potential, source, side_faces, end_faces):
    dma = pltpu.SemaphoreType.DMA
    anyspace = pl.BlockSpec(memory_space=pltpu.HBM)
    return pl.pallas_call(
        smooth_kernel,
        out_shape=(
            pltpu.VMEM((2, MEM, 2, ROWS, 128), F32),
            pltpu.VMEM((2, 4, NF + 16, 128), F32),
            pltpu.VMEM((NC, NF), BF16),
            pltpu.VMEM((NC, NC), BF16),
        ),
        in_specs=[anyspace, anyspace, pl.BlockSpec(memory_space=pltpu.VMEM), anyspace],
        out_specs=(pl.BlockSpec(memory_space=pltpu.VMEM),) * 4,
        scratch_shapes=[
            pltpu.VMEM((2, 4, NF + 16, 128), F32),
            pltpu.VMEM((NC, NC), F32),
            pltpu.VMEM((NF, NC), BF16),
            pltpu.VMEM((NF, NC), BF16),
            pltpu.VMEM((NC, NC), BF16),
            pltpu.VMEM((3, MEM, 2, ROWS, 128), F32),
            pltpu.VMEM((MEM, 2, ROWS, 128), F32),
            pltpu.VMEM((MEM, 2, ROWS, 128), F32),
            pltpu.VMEM((SLOTS, 2, FROWS, 128), F32),
            pltpu.VMEM((MEM, 2, ROWS, 128), F32),
            pltpu.VMEM((SLOTS, VROWS, 128), F32),
            pltpu.VMEM((SLOTS, VROWS, 128), F32),
            pltpu.VMEM((SLOTS, VROWS, 128), F32),
            pltpu.VMEM((3, FROWS, 128), F32),
            dma((4, 2)),
            dma,
            dma((CHUNKS,)),
            dma((CHUNKS,)),
            dma((CHUNKS, 2)),
            dma((MEM,)),
            dma((CHUNKS, 2)),
            dma((MEM,)),
            dma((8,)),
            dma((8,)),
            dma((8,)),
            dma((8,)),
            dma((2, 2, MEM)),
            dma((2, 2, MEM)),
        ],
        compiler_params=pltpu.CompilerParams(collective_id=0, has_side_effects=True),
        name="smooth",
    )(potential, source, side_faces, end_faces)


def prolong_kernel(e, p, w_fine, w_plain, corrected, correction, wide, fine, coarse, sems, coarse_sems):
    groups = lax.axis_size("grp")
    device = lax.axis_index("grp") * MEM + lax.axis_index("mem")
    is_last = device == groups * MEM - 1
    blocks = CROWS // ROWS

    def by_column(part, red, black):
        even = lax.rem(iota(red.shape, 0) + part + device, 2) == 0
        return jnp.concatenate([jnp.where(even, red, black), jnp.where(even, black, red)], axis=1)

    def rows_of(part, c):
        here = [by_column(part, e[part, c * blocks + b, 0], e[part, c * blocks + b, 1]) for b in range(blocks)]
        if c == CHUNKS - 1:
            after = jnp.broadcast_to(here[-1][ROWS - 1 :, :], (8, NC))
        else:
            q = (c + 1) * blocks
            after = by_column(part, e[part, q, 0, 0:8, :], e[part, q, 1, 0:8, :])
        return jnp.concatenate(here + [after], axis=0)

    copies = []
    for c in range(CHUNKS):
        rows = rows_of(0, c)
        above = jnp.where(is_last, rows, 0.5 * (rows + rows_of(1, c)))
        out_rows = pl.ds(FINE * c, FINE)
        for plane, x in enumerate((rows, above)):
            refined = dot_exact(x, w_fine[...])
            for t in range(4):
                wide[plane, t] = refined[:, 128 * t : 128 * t + 128]
                here, after = wide[plane, t, 0:CROWS, :], wide[plane, t, 1 : CROWS + 1, :]
                even, odd = pl.ds(FINE * c, CROWS, stride=2), pl.ds(FINE * c + 1, CROWS, stride=2)
                p_even = p[plane, t, pl.ds(8 + FINE * c, CROWS, stride=2), :]
                p_odd = p[plane, t, pl.ds(9 + FINE * c, CROWS, stride=2), :]
                fine[plane, t, even, :] = p_even + here
                fine[plane, t, odd, :] = p_odd + 0.5 * (here + after)
                copy = pltpu.make_async_copy(
                    fine.at[plane, t, out_rows],
                    corrected.at[plane, out_rows, pl.ds(128 * t, 128)],
                    sems.at[c, plane, t],
                )
                copy.start()
                copies.append(copy)
        out_rows = pl.ds(CROWS * c, CROWS)
        coarse[out_rows, :] = dot_exact(rows[:CROWS], w_plain[...])
        copy = pltpu.make_async_copy(coarse.at[out_rows], correction.at[0, out_rows], coarse_sems.at[c])
        copy.start()
        copies.append(copy)
    for copy in copies:
        copy.wait()


def prolong(*values):
    vmem = pl.BlockSpec(memory_space=pltpu.VMEM)
    anyspace = pl.BlockSpec(memory_space=pl.ANY)
    return pl.pallas_call(
        prolong_kernel,
        out_shape=(
            jax.ShapeDtypeStruct((2, NF, NF), F32),
            jax.ShapeDtypeStruct((1, NC, NC), F32),
        ),
        in_specs=[vmem] * 4,
        out_specs=(anyspace, anyspace),
        scratch_shapes=[
            pltpu.VMEM((2, 4, CROWS + 8, 128), F32),
            pltpu.VMEM((2, 4, NF, 128), F32),
            pltpu.VMEM((NC, NC), F32),
            pltpu.SemaphoreType.DMA((CHUNKS, 2, 4)),
            pltpu.SemaphoreType.DMA((CHUNKS,)),
        ],
        compiler_params=pltpu.CompilerParams(vmem_limit_bytes=24 * 2**20),
        name="prolong",
    )(*(pltpu.with_memory_space_constraint(x, pltpu.VMEM) for x in values))


def per_device(potential, source, side_faces, end_faces):
    return prolong(*smooth(potential, source, side_faces, end_faces))


def solution(mesh):
    placed = P(("grp", "mem"), None, None)
    return jax.shard_map(
        per_device,
        mesh=mesh,
        in_specs=(placed, placed, placed, P()),
        out_specs=(placed, placed),
        check_vma=False,
    )
```

```python
import jax
import jax.numpy as jnp
from jax import lax
from jax.experimental import pallas as pl
from jax.experimental.pallas import tpu as pltpu
from jax.sharding import PartitionSpec as P

F32 = jnp.float32
BF16 = jnp.bfloat16
MESH = pl.DeviceIdType.MESH

NF = 512
NC = 256
MEM = 8
ROWS = NC // MEM
HALO = 8
SLOTS = MEM + 2 * HALO
FROWS = ROWS + 2 * HALO
VROWS = FROWS + 16
CHUNKS = 4
CROWS = NC // CHUNKS
FINE = 2 * CROWS


def iota(shape, dim):
    return lax.broadcasted_iota(jnp.int32, shape, dim)


def split3(x):
    high = x.astype(BF16)
    rest = x - high.astype(F32)
    middle = rest.astype(BF16)
    low = (rest - middle.astype(F32)).astype(BF16)
    return high, middle, low


def dot_exact(x, weights):
    rows = x.shape[0]
    parts = jnp.concatenate(split3(x), axis=0)
    out = jnp.dot(parts, weights, preferred_element_type=F32)
    return out[:rows] + (out[rows : 2 * rows] + out[2 * rows :])


def coarse_column(shape, dim):
    n = iota(shape, dim)
    return jnp.where(n < NC // 2, 2 * n, 2 * n - (NC - 1))


DIRECTIONS = tuple((dg, dm) for dg in (-1, 0, 1) for dm in (-1, 0, 1) if (dg, dm) != (0, 0))


def smooth_kernel(
    p_hbm, s_hbm, side, end_hbm, e_out, pb, w_fine, w_plain,
    sb, eb, w_rc, w_lr, w_perm, fields, partner, summed, fb, xb, vr, vk, vk2, scales,
    in_sems, end_sem, p_send, p_recv, f_send, f_recv, x_send, x_recv, h_send, h_recv, b_send, b_recv,
    e_send, e_recv,
):
    groups = lax.axis_size("grp")
    g = lax.axis_index("grp")
    m = lax.axis_index("mem")
    device = g * MEM + m
    is_first = device == 0
    is_last = device == groups * MEM - 1
    at_end = jnp.logical_or(is_first, is_last)

    def remote(src, dst, send, recv, tg, tm):
        return pltpu.make_async_remote_copy(
            src_ref=src, dst_ref=dst, send_sem=send, recv_sem=recv,
            device_id={"grp": tg, "mem": tm}, device_id_type=MESH,
        )

    in_copies = []
    for t in range(4):
        for a, (src, dst) in enumerate(((p_hbm, pb), (s_hbm, sb))):
            in_copies.append(
                pltpu.make_async_copy(
                    src.at[:, :, pl.ds(128 * t, 128)], dst.at[:, t, pl.ds(8, NF), :], in_sems.at[t, a]
                )
            )
    for copy in in_copies:
        copy.start()
    end_copy = pltpu.make_async_copy(end_hbm.at[jnp.where(is_last, 1, 0)], eb, end_sem)

    @pl.when(at_end)
    def _():
        end_copy.start()

    vk2[...] = jnp.zeros_like(vk2)
    fb[...] = jnp.zeros_like(fb)
    xb[...] = jnp.zeros_like(xb)

    barrier = pltpu.get_barrier_semaphore()
    for dg in (-1, 0, 1):
        exists = jnp.logical_and(g + dg >= 0, g + dg < groups)

        @pl.when(exists)
        def _():
            for i in range(1 if dg == 0 else 0, MEM):
                pl.semaphore_signal(
                    barrier, inc=1,
                    device_id={"grp": g + dg, "mem": lax.rem(m + i, MEM)}, device_id_type=MESH,
                )

    vr[...] = jnp.zeros_like(vr)
    vk[...] = jnp.zeros_like(vk)
    row = m * ROWS - HALO + iota((FROWS, 128), 0)
    inner = jnp.where(jnp.logical_and(row >= 0, row < NC), 1.0 / 6.0, 0.0)
    scales[0] = jnp.where(g > 0, inner, 0.0)
    scales[1] = inner
    scales[2] = jnp.where(g < groups - 1, inner, 0.0)

    zeros = jnp.zeros((2, 4, 8, 128), F32)
    pb[:, :, 0:8, :] = zeros
    pb[:, :, 8 + NF : 16 + NF, :] = zeros
    sb[:, :, 0:8, :] = zeros

    column = coarse_column((NF, NC), 1)
    step = jnp.abs(iota((NF, NC), 0) - 2 * column)
    w_rc[...] = jnp.where(step == 0, 0.5, jnp.where(step == 1, 0.25, 0.0)).astype(BF16)
    near = jnp.where(step == 0, jnp.where(column == 0, 0.25, 0.5), 0.5)
    w_lr[...] = jnp.where(step <= 1, near, jnp.where(step == 2, 0.25, 0.0)).astype(BF16)
    square = coarse_column((NC, NC), 1)
    w_perm[...] = jnp.where(iota((NC, NC), 0) == square, 1.0, 0.0).astype(BF16)

    front = dot_exact(jnp.broadcast_to(side[0, 0:1, :], (8, NC)), w_perm[...])[0:1]
    back = dot_exact(jnp.broadcast_to(side[0, 1:2, :], (8, NC)), w_perm[...])[0:1]
    own_weight = jnp.where(is_first, 0.25, 0.5)
    blocks = CROWS // ROWS

    def by_colour(value, shift):
        even = lax.rem(iota((CROWS, 128), 0) + device + shift, 2) == 0
        left, right = value[:, :128], value[:, 128:]
        return jnp.where(even, left, right), jnp.where(even, right, left)

    def restrict(c, first):
        lists = [[], [], [], [], []]
        row = CROWS * c + iota((CROWS, 128), 0)
        for t in range(4):
            if first:
                for copy in in_copies[2 * t : 2 * t + 2]:
                    copy.wait()

            def load(ref, plane, shift):
                return ref[plane, t, pl.ds(8 + FINE * c + shift, CROWS, stride=2), :]

            a, b = [], []
            for plane in (0, 1):
                p_before, p_here, p_after = (load(pb, plane, k) for k in (-1, 0, 1))
                outer = load(pb, plane, -2) + load(pb, plane, 2)
                odd = p_before + p_after
                s_part = 0.5 * load(sb, plane, 0) + 0.25 * (load(sb, plane, -1) + load(sb, plane, 1))
                value = s_part + (outer - 4.0 * odd - 10.0 * p_here)
                a.append(value - jnp.where(row == 0, p_here, 0.0))
                b.append(2.0 * p_here + odd)
            up = 0.25 * a[1] + 0.5 * b[1]
            lists[0].append(0.5 * a[0] + up + own_weight * b[0])
            lists[1].append(up + 0.25 * b[0])
            lists[2].append(0.25 * b[0])
            lists[3].append(0.5 * b[0] + 0.25 * b[1])
            lists[4].append(0.25 * b[1])
        wide = [jnp.concatenate(f, axis=1) for f in lists]
        plain = dot_exact(jnp.concatenate(wide[:3], axis=0), w_rc[...])
        cross = dot_exact(jnp.concatenate(wide[3:], axis=0), w_lr[...])
        local = plain[:CROWS] + cross[:CROWS]
        above = plain[CROWS : 2 * CROWS] + cross[CROWS:]
        below = plain[2 * CROWS :]
        row = CROWS * c + iota((CROWS, NC), 0)
        lane = iota((CROWS, NC), 1)
        left = jnp.sum(jnp.where(lane == row, side[0, 2:3, :], 0.0), axis=1, keepdims=True)
        right = jnp.sum(jnp.where(lane == row, side[0, 3:4, :], 0.0), axis=1, keepdims=True)
        local = local + jnp.where(lane == 0, left, jnp.where(lane == NC - 1, right, 0.0))
        local = local + jnp.where(row == 0, front, jnp.where(row == NC - 1, back, 0.0))
        for field, value in ((0, local), (1, above), (2, below)):
            for colour, part in enumerate(by_colour(value, int(field > 0))):
                for b in range(blocks):
                    fields[field, c * blocks + b, colour] = part[ROWS * b : ROWS * (b + 1)]

    def add_end_face(c):
        face = dot_exact(eb[pl.ds(pl.multiple_of(CROWS * c, CROWS), CROWS), :], w_perm[...])
        for colour, part in enumerate(by_colour(face, 0)):
            for b in range(blocks):
                q = c * blocks + b
                fields[0, q, colour] = fields[0, q, colour] + part[ROWS * b : ROWS * (b + 1)]

    odd = lax.rem(m, 2)
    x_group = g - jnp.where(m == 0, 1, 0) + jnp.where(m == MEM - 1, 1, 0)
    x_plane = lax.rem(m + jnp.where(odd == 1, 1, MEM - 1), MEM)
    x_field = 2 - odd
    x_valid = jnp.logical_and(x_group >= 0, x_group < groups)
    x_home = x_group == g
    own_rows = pl.ds(HALO, ROWS)
    sent = []

    def send_if(condition, copy):
        sent.append((condition, copy))

        @pl.when(condition)
        def _():
            copy.start()

    def send_x(i, c, colour):
        for b in range(blocks):
            q = c * blocks + b
            home = jnp.logical_and(x_home, q == m)
            send_if(
                jnp.logical_and(x_valid, jnp.logical_not(home)),
                remote(
                    fields.at[x_field, q, colour], xb.at[x_plane, colour],
                    x_send.at[i, b, colour], x_recv.at[x_plane, colour], x_group, q,
                ),
            )

            @pl.when(home)
            def _():
                xb[x_plane, colour] = fields[x_field, q, colour]

    def send_fields(i, c):
        part = pl.ds(c * blocks, blocks)
        copy = remote(
            fields.at[1 + odd, part], partner.at[part], p_send.at[i], p_recv.at[i], g, m + 1 - 2 * odd
        )
        copy.start()
        send_x(i, c, 0)
        return copy

    def send_sums(i, c, to_partner):
        to_partner.wait_recv()
        for b in range(blocks):
            q = c * blocks + b
            summed[q] = fields[0, q] + partner[q]

            @pl.when(q == m)
            def _():
                fb[HALO + m, :, HALO : HALO + ROWS, :] = summed[q]

        for colour in (0, 1):
            if colour == 1:
                send_x(i, c, 1)
            for b in range(blocks):
                q = c * blocks + b
                send_if(
                    q != m,
                    remote(
                        summed.at[q, colour], fb.at[HALO + m, colour, own_rows],
                        f_send.at[i, b, colour], f_recv.at[m, colour], g, q,
                    ),
                )

    @pl.when(at_end)
    def _():
        end_copy.wait()

    order = [lax.rem(m // blocks + k, CHUNKS) for k in (1, 3, 0, 2)]
    partners = []
    for i, c in enumerate(order):
        restrict(c, i == 0)

        @pl.when(at_end)
        def _():
            add_end_face(c)

        if i == 0:
            count = (MEM - 1) + jnp.where(g > 0, MEM, 0) + jnp.where(g < groups - 1, MEM, 0)
            pl.semaphore_wait(barrier, count)
        partners.append(send_fields(i, c))
        if i > 0:
            send_sums(i - 1, order[i - 1], partners[i - 1])
    send_sums(CHUNKS - 1, order[-1], partners[-1])

    def inside(dg, dm):
        ok = None
        for test in (
            (g + dg >= 0) if dg < 0 else (g + dg < groups) if dg > 0 else None,
            (m + dm >= 0) if dm < 0 else (m + dm < MEM) if dm > 0 else None,
        ):
            if test is not None:
                ok = test if ok is None else jnp.logical_and(ok, test)
        return ok

    def exchange(make):
        copies = []
        for o, (dg, dm) in enumerate(DIRECTIONS):
            copy = make(o, dg, dm)
            copies.append(copy)

            @pl.when(inside(dg, dm))
            def _():
                copy.start()
        return copies

    def arrive(copies):
        for o, (dg, dm) in enumerate(DIRECTIONS):
            @pl.when(inside(-dg, -dm))
            def _():
                copies[o].wait_recv()

    def row_parts(dm, base):
        if dm < 0:
            return pl.ds(base, HALO), pl.ds(base + ROWS, HALO)
        if dm > 0:
            return pl.ds(base + ROWS - HALO, HALO), pl.ds(base - HALO, HALO)
        return pl.ds(base, ROWS), pl.ds(base, ROWS)

    def plane_parts(dg, depth):
        if dg < 0:
            return pl.ds(HALO, depth), pl.ds(HALO + MEM, depth)
        if dg > 0:
            return pl.ds(HALO + MEM - depth, depth), pl.ds(HALO - depth, depth)
        return pl.ds(HALO, MEM), pl.ds(HALO, MEM)

    def forcing_copy(o, dg, dm, k=None, colour=0):
        src_rows, dst_rows = row_parts(dm, HALO)
        if k is None:
            src, dst = plane_parts(dg, HALO - 1 - abs(dm))
            colour = slice(None)
        else:
            src, dst = HALO + k, HALO + k - MEM * dg
        return remote(
            fb.at[src, colour, src_rows], fb.at[dst, colour, dst_rows], h_send.at[o], h_recv.at[o], g + dg, m + dm
        )

    def receive(n, carry):
        colour = lax.rem(n // 4, 2)
        item = n // 8 * 4 + lax.rem(n, 4)
        offset = jnp.where(item < 4, item - 1, jnp.where(item == 4, -2, item - 2))
        k = lax.rem(m // blocks * blocks + offset + MEM, MEM)

        @pl.when(m != k)
        def _():
            remote(
                summed.at[0, 0], fb.at[HALO + k, colour, own_rows],
                f_send.at[0, 0, 0], f_recv.at[k, colour], g, k,
            ).wait_recv()

        arrives = jnp.logical_not(jnp.logical_and(x_home, x_plane == k))
        arrives = jnp.logical_and(arrives, jnp.logical_or(k > 0, g > 0))
        arrives = jnp.logical_and(arrives, jnp.logical_or(k < MEM - 1, g < groups - 1))

        @pl.when(arrives)
        def _():
            remote(
                fields.at[0, 0, 0], xb.at[k, colour], x_send.at[0, 0, 0], x_recv.at[k, colour], g, k
            ).wait_recv()

        fb[HALO + k, colour, HALO : HALO + ROWS, :] = fb[HALO + k, colour, HALO : HALO + ROWS, :] + xb[k, colour]
        for o, (dg, dm) in enumerate(DIRECTIONS):
            depth = HALO - 1 - abs(dm)
            needed = inside(dg, dm)
            if dg < 0:
                needed = jnp.logical_and(needed, k < depth)
            if dg > 0:
                needed = jnp.logical_and(needed, k >= MEM - depth)

            @pl.when(needed)
            def _():
                forcing_copy(o, dg, dm, k, colour).start()
        return carry

    def black_copy(o, dg, dm):
        src_rows, dst_rows = row_parts(dm, HALO + 8)
        src_planes, dst_planes = plane_parts(dg, HALO - abs(dm))
        return remote(
            vk2.at[src_planes, src_rows], vk2.at[dst_planes, dst_rows],
            b_send.at[o], b_recv.at[o], g + dg, m + dm,
        )

    lax.fori_loop(0, 2 * MEM, receive, 0)
    column = coarse_column((NC, NF), 0)
    step = iota((NC, NF), 1) - 2 * column
    whole = jnp.logical_or(step == 0, jnp.logical_and(step == 1, column == NC - 1))
    half = jnp.abs(step) == 1
    w_fine[...] = jnp.where(whole, 1.0, jnp.where(half, 0.5, 0.0)).astype(BF16)
    w_plain[...] = jnp.where(iota((NC, NC), 1) == coarse_column((NC, NC), 0), 1.0, 0.0).astype(BF16)

    h_copies = [forcing_copy(o, dg, dm) for o, (dg, dm) in enumerate(DIRECTIONS)]
    arrive(h_copies)

    lane = iota((8, 128), 1)
    row_parity = lax.rem(iota((8, 128), 0), 2)
    from_left = [
        (jnp.logical_and(row_parity == flip, lane != 0), jnp.logical_and(row_parity != flip, lane != 127))
        for flip in (0, 1)
    ]

    def half_sweep(colour, t, target, source, first=0, tiles=FROWS // 8):
        at, n = 8 + 8 * first, 8 * tiles
        shape = (tiles, 8, 128)
        for slot in range(t, SLOTS - t):
            centre = source[slot, at : at + n, :].reshape(shape)
            keep_left, keep_right = from_left[(slot + colour) % 2]
            beside = jnp.where(
                jnp.broadcast_to(keep_left, shape), pltpu.roll(centre, 1, 2),
                jnp.where(jnp.broadcast_to(keep_right, shape), pltpu.roll(centre, 127, 2), 0.0),
            )
            rows = source[slot, at - 1 : at - 1 + n, :] + source[slot, at + 1 : at + 1 + n, :]
            depth = source[slot - 1, at : at + n, :] + source[slot + 1, at : at + n, :]
            side = 0 if slot < HALO else 2 if slot >= HALO + MEM else 1
            near = (depth + rows).reshape(shape) + (centre + beside)
            total = fb[slot, colour, 8 * first : 8 * first + n, :].reshape(shape) + near
            total = total * scales[side, 8 * first : 8 * first + n, :].reshape(shape)
            target[slot, at : at + n, :] = total.reshape(n, 128)

    def sweeps(black):
        for t in (1, 3, 5):
            half_sweep(0, t, vr, black)
            half_sweep(1, t + 1, black, vr)
        half_sweep(0, 7, vr, black)

    sweeps(vk)
    half_sweep(1, 8, vk2, vr, 1, ROWS // 8)
    b_copies = exchange(black_copy)
    arrive(b_copies)
    for o, (dg, dm) in enumerate(DIRECTIONS):
        @pl.when(inside(dg, dm))
        def _():
            b_copies[o].wait_send()
    sweeps(vk2)

    v_rows = pl.ds(HALO + 8, ROWS)
    e_copies = []

    def send_back(colour, values):
        for i in range(MEM):
            tm = lax.rem(m + i, MEM)
            if i == 0:
                e_out[0, m, colour] = values[HALO + m, HALO + 8 : HALO + 8 + ROWS, :]
            else:
                copy = remote(
                    values.at[HALO + tm, v_rows], e_out.at[0, m, colour],
                    e_send.at[0, colour, i], e_recv.at[0, colour, m], g, tm,
                )
                copy.start()
                e_copies.append((copy, None))
            wraps = tm == MEM - 1
            plane = HALO + jnp.where(wraps, 0, tm + 1)
            tg = g - jnp.where(wraps, 1, 0)
            copy = remote(
                values.at[plane, v_rows], e_out.at[1, m, colour],
                e_send.at[1, colour, i], e_recv.at[1, colour, m], tg, tm,
            )
            if i == 0:
                sends = jnp.logical_and(wraps, g > 0)

                @pl.when(jnp.logical_not(wraps))
                def _():
                    e_out[1, m, colour] = values[plane, HALO + 8 : HALO + 8 + ROWS, :]
            else:
                sends = jnp.logical_not(jnp.logical_and(wraps, g == 0))
            e_copies.append((copy, sends))

            @pl.when(sends)
            def _():
                copy.start()

    send_back(0, vr)
    half_sweep(1, 8, vk2, vr, 1, ROWS // 8)
    send_back(1, vk2)

    for copy in partners:
        copy.wait_send()
    for condition, copy in sent:
        @pl.when(condition)
        def _():
            copy.wait_send()
    for o, (dg, dm) in enumerate(DIRECTIONS):
        @pl.when(inside(dg, dm))
        def _():
            h_copies[o].wait_send()
    for colour, values in ((0, vr), (1, vk2)):
        for q in range(MEM):
            def wait_for(part):
                remote(
                    values.at[HALO, v_rows], e_out.at[part, q, colour],
                    e_send.at[part, colour, 0], e_recv.at[part, colour, q], g, q,
                ).wait_recv()

            @pl.when(m != q)
            def _():
                wait_for(0)

            last = m == MEM - 1
            arrives = jnp.logical_or(
                jnp.logical_and(jnp.logical_not(last), m != q), jnp.logical_and(last, g < groups - 1)
            )

            @pl.when(arrives)
            def _():
                wait_for(1)
    for copy, sends in e_copies:
        if sends is None:
            copy.wait_send()
        else:
            @pl.when(sends)
            def _():
                copy.wait_send()


def smooth(potential, source, side_faces, end_faces):
    dma = pltpu.SemaphoreType.DMA
    anyspace = pl.BlockSpec(memory_space=pltpu.HBM)
    return pl.pallas_call(
        smooth_kernel,
        out_shape=(
            pltpu.VMEM((2, MEM, 2, ROWS, 128), F32),
            pltpu.VMEM((2, 4, NF + 16, 128), F32),
            pltpu.VMEM((NC, NF), BF16),
            pltpu.VMEM((NC, NC), BF16),
        ),
        in_specs=[anyspace, anyspace, pl.BlockSpec(memory_space=pltpu.VMEM), anyspace],
        out_specs=(pl.BlockSpec(memory_space=pltpu.VMEM),) * 4,
        scratch_shapes=[
            pltpu.VMEM((2, 4, NF + 16, 128), F32),
            pltpu.VMEM((NC, NC), F32),
            pltpu.VMEM((NF, NC), BF16),
            pltpu.VMEM((NF, NC), BF16),
            pltpu.VMEM((NC, NC), BF16),
            pltpu.VMEM((3, MEM, 2, ROWS, 128), F32),
            pltpu.VMEM((MEM, 2, ROWS, 128), F32),
            pltpu.VMEM((MEM, 2, ROWS, 128), F32),
            pltpu.VMEM((SLOTS, 2, FROWS, 128), F32),
            pltpu.VMEM((MEM, 2, ROWS, 128), F32),
            pltpu.VMEM((SLOTS, VROWS, 128), F32),
            pltpu.VMEM((SLOTS, VROWS, 128), F32),
            pltpu.VMEM((SLOTS, VROWS, 128), F32),
            pltpu.VMEM((3, FROWS, 128), F32),
            dma((4, 2)),
            dma,
            dma((CHUNKS,)),
            dma((CHUNKS,)),
            dma((CHUNKS, 2, 2)),
            dma((MEM, 2)),
            dma((CHUNKS, 2, 2)),
            dma((MEM, 2)),
            dma((8,)),
            dma((8,)),
            dma((8,)),
            dma((8,)),
            dma((2, 2, MEM)),
            dma((2, 2, MEM)),
        ],
        compiler_params=pltpu.CompilerParams(collective_id=0, has_side_effects=True),
        name="smooth",
    )(potential, source, side_faces, end_faces)


def prolong_kernel(e, p, w_fine, w_plain, corrected, correction, wide, fine, coarse, sems, coarse_sems):
    groups = lax.axis_size("grp")
    device = lax.axis_index("grp") * MEM + lax.axis_index("mem")
    is_last = device == groups * MEM - 1
    blocks = CROWS // ROWS

    def by_column(part, red, black):
        even = lax.rem(iota(red.shape, 0) + part + device, 2) == 0
        return jnp.concatenate([jnp.where(even, red, black), jnp.where(even, black, red)], axis=1)

    def rows_of(part, c):
        here = [by_column(part, e[part, c * blocks + b, 0], e[part, c * blocks + b, 1]) for b in range(blocks)]
        if c == CHUNKS - 1:
            after = jnp.broadcast_to(here[-1][ROWS - 1 :, :], (8, NC))
        else:
            q = (c + 1) * blocks
            after = by_column(part, e[part, q, 0, 0:8, :], e[part, q, 1, 0:8, :])
        return jnp.concatenate(here + [after], axis=0)

    copies = []
    for c in range(CHUNKS):
        rows = rows_of(0, c)
        above = jnp.where(is_last, rows, 0.5 * (rows + rows_of(1, c)))
        out_rows = pl.ds(FINE * c, FINE)
        for plane, x in enumerate((rows, above)):
            refined = dot_exact(x, w_fine[...])
            for t in range(4):
                wide[plane, t] = refined[:, 128 * t : 128 * t + 128]
                here, after = wide[plane, t, 0:CROWS, :], wide[plane, t, 1 : CROWS + 1, :]
                even, odd = pl.ds(FINE * c, CROWS, stride=2), pl.ds(FINE * c + 1, CROWS, stride=2)
                p_even = p[plane, t, pl.ds(8 + FINE * c, CROWS, stride=2), :]
                p_odd = p[plane, t, pl.ds(9 + FINE * c, CROWS, stride=2), :]
                fine[plane, t, even, :] = p_even + here
                fine[plane, t, odd, :] = p_odd + 0.5 * (here + after)
                copy = pltpu.make_async_copy(
                    fine.at[plane, t, out_rows],
                    corrected.at[plane, out_rows, pl.ds(128 * t, 128)],
                    sems.at[c, plane, t],
                )
                copy.start()
                copies.append(copy)
        out_rows = pl.ds(CROWS * c, CROWS)
        coarse[out_rows, :] = dot_exact(rows[:CROWS], w_plain[...])
        copy = pltpu.make_async_copy(coarse.at[out_rows], correction.at[0, out_rows], coarse_sems.at[c])
        copy.start()
        copies.append(copy)
    for copy in copies:
        copy.wait()


def prolong(*values):
    vmem = pl.BlockSpec(memory_space=pltpu.VMEM)
    anyspace = pl.BlockSpec(memory_space=pl.ANY)
    return pl.pallas_call(
        prolong_kernel,
        out_shape=(
            jax.ShapeDtypeStruct((2, NF, NF), F32),
            jax.ShapeDtypeStruct((1, NC, NC), F32),
        ),
        in_specs=[vmem] * 4,
        out_specs=(anyspace, anyspace),
        scratch_shapes=[
            pltpu.VMEM((2, 4, CROWS + 8, 128), F32),
            pltpu.VMEM((2, 4, NF, 128), F32),
            pltpu.VMEM((NC, NC), F32),
            pltpu.SemaphoreType.DMA((CHUNKS, 2, 4)),
            pltpu.SemaphoreType.DMA((CHUNKS,)),
        ],
        compiler_params=pltpu.CompilerParams(vmem_limit_bytes=24 * 2**20),
        name="prolong",
    )(*(pltpu.with_memory_space_constraint(x, pltpu.VMEM) for x in values))


def per_device(potential, source, side_faces, end_faces):
    return prolong(*smooth(potential, source, side_faces, end_faces))


def solution(mesh):
    placed = P(("grp", "mem"), None, None)
    return jax.shard_map(
        per_device,
        mesh=mesh,
        in_specs=(placed, placed, placed, P()),
        out_specs=(placed, placed),
        check_vma=False,
    )
```

```python
import jax
import jax.numpy as jnp
from jax import lax
from jax.experimental import pallas as pl
from jax.experimental.pallas import tpu as pltpu
from jax.sharding import PartitionSpec as P

F32 = jnp.float32
BF16 = jnp.bfloat16
MESH = pl.DeviceIdType.MESH

NF = 512
NC = 256
MEM = 8
ROWS = NC // MEM
HALO = 8
SLOTS = MEM + 2 * HALO
FROWS = ROWS + 2 * HALO
VROWS = FROWS + 16
CHUNKS = 4
CROWS = NC // CHUNKS
FINE = 2 * CROWS


def iota(shape, dim):
    return lax.broadcasted_iota(jnp.int32, shape, dim)


def split3(x):
    high = x.astype(BF16)
    rest = x - high.astype(F32)
    middle = rest.astype(BF16)
    low = (rest - middle.astype(F32)).astype(BF16)
    return high, middle, low


def dot_exact(x, weights):
    rows = x.shape[0]
    parts = jnp.concatenate(split3(x), axis=0)
    out = jnp.dot(parts, weights, preferred_element_type=F32)
    return out[:rows] + (out[rows : 2 * rows] + out[2 * rows :])


def coarse_column(shape, dim):
    n = iota(shape, dim)
    return jnp.where(n < NC // 2, 2 * n, 2 * n - (NC - 1))


DIRECTIONS = tuple((dg, dm) for dg in (-1, 0, 1) for dm in (-1, 0, 1) if (dg, dm) != (0, 0))


def smooth_kernel(
    p_hbm, s_hbm, side, end_hbm, e_out, pb, w_fine, w_plain,
    sb, eb, w_rc, w_lr, w_perm, fields, partner, summed, fb, xb, vr, vk, vk2, scales,
    in_sems, end_sem, p_send, p_recv, f_send, f_recv, x_send, x_recv, h_send, h_recv, b_send, b_recv,
    e_send, e_recv, fwd_send,
):
    groups = lax.axis_size("grp")
    g = lax.axis_index("grp")
    m = lax.axis_index("mem")
    device = g * MEM + m
    is_first = device == 0
    is_last = device == groups * MEM - 1
    at_end = jnp.logical_or(is_first, is_last)

    def remote(src, dst, send, recv, tg, tm):
        return pltpu.make_async_remote_copy(
            src_ref=src, dst_ref=dst, send_sem=send, recv_sem=recv,
            device_id={"grp": tg, "mem": tm}, device_id_type=MESH,
        )

    in_copies = []
    for t in range(4):
        for a, (src, dst) in enumerate(((p_hbm, pb), (s_hbm, sb))):
            in_copies.append(
                pltpu.make_async_copy(
                    src.at[:, :, pl.ds(128 * t, 128)], dst.at[:, t, pl.ds(8, NF), :], in_sems.at[t, a]
                )
            )
    for copy in in_copies:
        copy.start()
    end_copy = pltpu.make_async_copy(end_hbm.at[jnp.where(is_last, 1, 0)], eb, end_sem)

    @pl.when(at_end)
    def _():
        end_copy.start()

    vk2[...] = jnp.zeros_like(vk2)
    fb[...] = jnp.zeros_like(fb)
    xb[...] = jnp.zeros_like(xb)

    barrier = pltpu.get_barrier_semaphore()
    for dg in (-1, 0, 1):
        exists = jnp.logical_and(g + dg >= 0, g + dg < groups)

        @pl.when(exists)
        def _():
            for i in range(1 if dg == 0 else 0, MEM):
                pl.semaphore_signal(
                    barrier, inc=1,
                    device_id={"grp": g + dg, "mem": lax.rem(m + i, MEM)}, device_id_type=MESH,
                )

    vr[...] = jnp.zeros_like(vr)
    vk[...] = jnp.zeros_like(vk)
    row = m * ROWS - HALO + iota((FROWS, 128), 0)
    inner = jnp.where(jnp.logical_and(row >= 0, row < NC), 1.0 / 6.0, 0.0)
    scales[0] = jnp.where(g > 0, inner, 0.0)
    scales[1] = inner
    scales[2] = jnp.where(g < groups - 1, inner, 0.0)

    zeros = jnp.zeros((2, 4, 8, 128), F32)
    pb[:, :, 0:8, :] = zeros
    pb[:, :, 8 + NF : 16 + NF, :] = zeros
    sb[:, :, 0:8, :] = zeros

    column = coarse_column((NF, NC), 1)
    step = jnp.abs(iota((NF, NC), 0) - 2 * column)
    w_rc[...] = jnp.where(step == 0, 0.5, jnp.where(step == 1, 0.25, 0.0)).astype(BF16)
    near = jnp.where(step == 0, jnp.where(column == 0, 0.25, 0.5), 0.5)
    w_lr[...] = jnp.where(step <= 1, near, jnp.where(step == 2, 0.25, 0.0)).astype(BF16)
    square = coarse_column((NC, NC), 1)
    w_perm[...] = jnp.where(iota((NC, NC), 0) == square, 1.0, 0.0).astype(BF16)

    front = dot_exact(jnp.broadcast_to(side[0, 0:1, :], (8, NC)), w_perm[...])[0:1]
    back = dot_exact(jnp.broadcast_to(side[0, 1:2, :], (8, NC)), w_perm[...])[0:1]
    own_weight = jnp.where(is_first, 0.25, 0.5)
    blocks = CROWS // ROWS

    def by_colour(value, shift):
        even = lax.rem(iota((CROWS, 128), 0) + device + shift, 2) == 0
        left, right = value[:, :128], value[:, 128:]
        return jnp.where(even, left, right), jnp.where(even, right, left)

    def restrict(c, first):
        lists = [[], [], [], [], []]
        row = CROWS * c + iota((CROWS, 128), 0)
        for t in range(4):
            if first:
                for copy in in_copies[2 * t : 2 * t + 2]:
                    copy.wait()

            def load(ref, plane, shift):
                return ref[plane, t, pl.ds(8 + FINE * c + shift, CROWS, stride=2), :]

            a, b = [], []
            for plane in (0, 1):
                p_before, p_here, p_after = (load(pb, plane, k) for k in (-1, 0, 1))
                outer = load(pb, plane, -2) + load(pb, plane, 2)
                odd = p_before + p_after
                s_part = 0.5 * load(sb, plane, 0) + 0.25 * (load(sb, plane, -1) + load(sb, plane, 1))
                value = s_part + (outer - 4.0 * odd - 10.0 * p_here)
                a.append(value - jnp.where(row == 0, p_here, 0.0))
                b.append(2.0 * p_here + odd)
            up = 0.25 * a[1] + 0.5 * b[1]
            lists[0].append(0.5 * a[0] + up + own_weight * b[0])
            lists[1].append(up + 0.25 * b[0])
            lists[2].append(0.25 * b[0])
            lists[3].append(0.5 * b[0] + 0.25 * b[1])
            lists[4].append(0.25 * b[1])
        wide = [jnp.concatenate(f, axis=1) for f in lists]
        plain = dot_exact(jnp.concatenate(wide[:3], axis=0), w_rc[...])
        cross = dot_exact(jnp.concatenate(wide[3:], axis=0), w_lr[...])
        local = plain[:CROWS] + cross[:CROWS]
        above = plain[CROWS : 2 * CROWS] + cross[CROWS:]
        below = plain[2 * CROWS :]
        row = CROWS * c + iota((CROWS, NC), 0)
        lane = iota((CROWS, NC), 1)
        left = jnp.sum(jnp.where(lane == row, side[0, 2:3, :], 0.0), axis=1, keepdims=True)
        right = jnp.sum(jnp.where(lane == row, side[0, 3:4, :], 0.0), axis=1, keepdims=True)
        local = local + jnp.where(lane == 0, left, jnp.where(lane == NC - 1, right, 0.0))
        local = local + jnp.where(row == 0, front, jnp.where(row == NC - 1, back, 0.0))
        for field, value in ((0, local), (1, above), (2, below)):
            for colour, part in enumerate(by_colour(value, int(field > 0))):
                for b in range(blocks):
                    fields[field, c * blocks + b, colour] = part[ROWS * b : ROWS * (b + 1)]

    def add_end_face(c):
        face = dot_exact(eb[pl.ds(pl.multiple_of(CROWS * c, CROWS), CROWS), :], w_perm[...])
        for colour, part in enumerate(by_colour(face, 0)):
            for b in range(blocks):
                q = c * blocks + b
                fields[0, q, colour] = fields[0, q, colour] + part[ROWS * b : ROWS * (b + 1)]

    odd = lax.rem(m, 2)
    x_group = g - jnp.where(m == 0, 1, 0) + jnp.where(m == MEM - 1, 1, 0)
    x_plane = lax.rem(m + jnp.where(odd == 1, 1, MEM - 1), MEM)
    x_field = 2 - odd
    x_valid = jnp.logical_and(x_group >= 0, x_group < groups)
    x_home = x_group == g
    own_rows = pl.ds(HALO, ROWS)
    sent = []

    def send_if(condition, copy):
        sent.append((condition, copy))

        @pl.when(condition)
        def _():
            copy.start()

    def send_x(i, c, colour):
        for b in range(blocks):
            q = c * blocks + b
            home = jnp.logical_and(x_home, q == m)
            send_if(
                jnp.logical_and(x_valid, jnp.logical_not(home)),
                remote(
                    fields.at[x_field, q, colour], xb.at[x_plane, colour],
                    x_send.at[i, b, colour], x_recv.at[x_plane, colour], x_group, q,
                ),
            )

            @pl.when(home)
            def _():
                xb[x_plane, colour] = fields[x_field, q, colour]

    def send_fields(i, c):
        part = pl.ds(c * blocks, blocks)
        copy = remote(
            fields.at[1 + odd, part], partner.at[part], p_send.at[i], p_recv.at[i], g, m + 1 - 2 * odd
        )
        copy.start()
        send_x(i, c, 0)
        return copy

    def send_sums(i, c, to_partner):
        to_partner.wait_recv()
        for b in range(blocks):
            q = c * blocks + b
            summed[q] = fields[0, q] + partner[q]

            @pl.when(q == m)
            def _():
                fb[HALO + m, :, HALO : HALO + ROWS, :] = summed[q]

        for colour in (0, 1):
            if colour == 1:
                send_x(i, c, 1)
            for b in range(blocks):
                q = c * blocks + b
                send_if(
                    q != m,
                    remote(
                        summed.at[q, colour], fb.at[HALO + m, colour, own_rows],
                        f_send.at[i, b, colour], f_recv.at[m, colour], g, q,
                    ),
                )

    @pl.when(at_end)
    def _():
        end_copy.wait()

    order = [lax.rem(m // blocks + k, CHUNKS) for k in (1, 3, 0, 2)]
    partners = []
    for i, c in enumerate(order):
        restrict(c, i == 0)

        @pl.when(at_end)
        def _():
            add_end_face(c)

        if i == 0:
            count = (MEM - 1) + jnp.where(g > 0, MEM, 0) + jnp.where(g < groups - 1, MEM, 0)
            pl.semaphore_wait(barrier, count)
        partners.append(send_fields(i, c))
        if i > 0:
            send_sums(i - 1, order[i - 1], partners[i - 1])
    send_sums(CHUNKS - 1, order[-1], partners[-1])

    def inside(dg, dm):
        ok = None
        for test in (
            (g + dg >= 0) if dg < 0 else (g + dg < groups) if dg > 0 else None,
            (m + dm >= 0) if dm < 0 else (m + dm < MEM) if dm > 0 else None,
        ):
            if test is not None:
                ok = test if ok is None else jnp.logical_and(ok, test)
        return ok

    def exchange(make):
        copies = []
        for o, (dg, dm) in enumerate(DIRECTIONS):
            copy = make(o, dg, dm)
            copies.append(copy)

            @pl.when(inside(dg, dm))
            def _():
                copy.start()
        return copies

    def arrive(copies):
        for o, (dg, dm) in enumerate(DIRECTIONS):
            @pl.when(inside(-dg, -dm))
            def _():
                copies[o].wait_recv()

    def row_parts(dm, base):
        if dm < 0:
            return pl.ds(base, HALO), pl.ds(base + ROWS, HALO)
        if dm > 0:
            return pl.ds(base + ROWS - HALO, HALO), pl.ds(base - HALO, HALO)
        return pl.ds(base, ROWS), pl.ds(base, ROWS)

    def plane_parts(dg, depth):
        if dg < 0:
            return pl.ds(HALO, depth), pl.ds(HALO + MEM, depth)
        if dg > 0:
            return pl.ds(HALO + MEM - depth, depth), pl.ds(HALO - depth, depth)
        return pl.ds(HALO, MEM), pl.ds(HALO, MEM)

    def forcing_copy(o, dg, dm, k=None, colour=0):
        src_rows, dst_rows = row_parts(dm, HALO)
        if k is None:
            src, dst = plane_parts(dg, HALO - 1 - abs(dm))
            colour = slice(None)
        else:
            src, dst = HALO + k, HALO + k - MEM * dg
        return remote(
            fb.at[src, colour, src_rows], fb.at[dst, colour, dst_rows], h_send.at[o], h_recv.at[o], g + dg, m + dm
        )

    def receive(n, carry):
        colour = lax.rem(n // 4, 2)
        item = n // 8 * 4 + lax.rem(n, 4)
        offset = jnp.where(item < 4, item - 1, jnp.where(item == 4, -2, item - 2))
        k = lax.rem(m // blocks * blocks + offset + MEM, MEM)

        @pl.when(m != k)
        def _():
            remote(
                summed.at[0, 0], fb.at[HALO + k, colour, own_rows],
                f_send.at[0, 0, 0], f_recv.at[k, colour], g, k,
            ).wait_recv()

        arrives = jnp.logical_not(jnp.logical_and(x_home, x_plane == k))
        arrives = jnp.logical_and(arrives, jnp.logical_or(k > 0, g > 0))
        arrives = jnp.logical_and(arrives, jnp.logical_or(k < MEM - 1, g < groups - 1))

        @pl.when(arrives)
        def _():
            remote(
                fields.at[0, 0, 0], xb.at[k, colour], x_send.at[0, 0, 0], x_recv.at[k, colour], g, k
            ).wait_recv()

        fb[HALO + k, colour, HALO : HALO + ROWS, :] = fb[HALO + k, colour, HALO : HALO + ROWS, :] + xb[k, colour]
        for o, (dg, dm) in enumerate(DIRECTIONS):
            depth = HALO - 1 - abs(dm)
            needed = inside(dg, dm)
            if dg < 0:
                needed = jnp.logical_and(needed, k < depth)
            if dg > 0:
                needed = jnp.logical_and(needed, k >= MEM - depth)

            @pl.when(needed)
            def _():
                forcing_copy(o, dg, dm, k, colour).start()
        return carry

    def black_copy(o, dg, dm):
        src_rows, dst_rows = row_parts(dm, HALO + 8)
        src_planes, dst_planes = plane_parts(dg, HALO - abs(dm))
        return remote(
            vk2.at[src_planes, src_rows], vk2.at[dst_planes, dst_rows],
            b_send.at[o], b_recv.at[o], g + dg, m + dm,
        )

    lax.fori_loop(0, 2 * MEM, receive, 0)
    column = coarse_column((NC, NF), 0)
    step = iota((NC, NF), 1) - 2 * column
    whole = jnp.logical_or(step == 0, jnp.logical_and(step == 1, column == NC - 1))
    half = jnp.abs(step) == 1
    w_fine[...] = jnp.where(whole, 1.0, jnp.where(half, 0.5, 0.0)).astype(BF16)
    w_plain[...] = jnp.where(iota((NC, NC), 1) == coarse_column((NC, NC), 0), 1.0, 0.0).astype(BF16)

    h_copies = [forcing_copy(o, dg, dm) for o, (dg, dm) in enumerate(DIRECTIONS)]
    arrive(h_copies)

    lane = iota((8, 128), 1)
    row_parity = lax.rem(iota((8, 128), 0), 2)
    from_left = [
        (jnp.logical_and(row_parity == flip, lane != 0), jnp.logical_and(row_parity != flip, lane != 127))
        for flip in (0, 1)
    ]

    def half_sweep(colour, t, target, source, first=0, tiles=FROWS // 8):
        at, n = 8 + 8 * first, 8 * tiles
        shape = (tiles, 8, 128)
        for slot in range(t, SLOTS - t):
            centre = source[slot, at : at + n, :].reshape(shape)
            keep_left, keep_right = from_left[(slot + colour) % 2]
            beside = jnp.where(
                jnp.broadcast_to(keep_left, shape), pltpu.roll(centre, 1, 2),
                jnp.where(jnp.broadcast_to(keep_right, shape), pltpu.roll(centre, 127, 2), 0.0),
            )
            rows = source[slot, at - 1 : at - 1 + n, :] + source[slot, at + 1 : at + 1 + n, :]
            depth = source[slot - 1, at : at + n, :] + source[slot + 1, at : at + n, :]
            side = 0 if slot < HALO else 2 if slot >= HALO + MEM else 1
            near = (depth + rows).reshape(shape) + (centre + beside)
            total = fb[slot, colour, 8 * first : 8 * first + n, :].reshape(shape) + near
            total = total * scales[side, 8 * first : 8 * first + n, :].reshape(shape)
            target[slot, at : at + n, :] = total.reshape(n, 128)

    def sweeps(black):
        for t in (1, 3, 5):
            half_sweep(0, t, vr, black)
            half_sweep(1, t + 1, black, vr)
        half_sweep(0, 7, vr, black)

    sweeps(vk)
    half_sweep(1, 8, vk2, vr, 1, ROWS // 8)
    b_copies = exchange(black_copy)
    arrive(b_copies)
    for o, (dg, dm) in enumerate(DIRECTIONS):
        @pl.when(inside(dg, dm))
        def _():
            b_copies[o].wait_send()
    sweeps(vk2)

    v_rows = pl.ds(HALO + 8, ROWS)
    e_copies = []

    def send_back(colour, values):
        e_out[0, m, colour] = values[HALO + m, HALO + 8 : HALO + 8 + ROWS, :]
        for i in range(1, MEM):
            tm = lax.rem(m + i, MEM)
            copy = remote(
                values.at[HALO + tm, v_rows], e_out.at[0, m, colour],
                e_send.at[0, colour, i], e_recv.at[0, colour, m], g, tm,
            )
            copy.start()
            e_copies.append((copy, None))
        for i in range(MEM):
            tm = lax.rem(m + i, MEM)
            wraps = tm == MEM - 1
            plane = HALO + jnp.where(wraps, 0, tm + 1)
            tg = g - jnp.where(wraps, 1, 0)
            copy = remote(
                values.at[plane, v_rows], e_out.at[1, m, colour],
                e_send.at[1, colour, i], e_recv.at[1, colour, m], tg, tm,
            )
            if i == 0:
                sends = jnp.logical_and(wraps, g > 0)

                @pl.when(jnp.logical_not(wraps))
                def _():
                    e_out[1, m, colour] = values[plane, HALO + 8 : HALO + 8 + ROWS, :]
            else:
                direct = jnp.logical_or(lax.rem(tm, 2) == 1, tm // blocks == m // blocks)
                sends = jnp.logical_and(direct, jnp.logical_not(jnp.logical_and(wraps, g == 0)))
            e_copies.append((copy, sends))

            @pl.when(sends)
            def _():
                copy.start()

    send_back(0, vr)
    half_sweep(1, 8, vk2, vr, 1, ROWS // 8)
    send_back(1, vk2)

    for copy in partners:
        copy.wait_send()
    for condition, copy in sent:
        @pl.when(condition)
        def _():
            copy.wait_send()
    for o, (dg, dm) in enumerate(DIRECTIONS):
        @pl.when(inside(dg, dm))
        def _():
            h_copies[o].wait_send()
    for colour, values in ((0, vr), (1, vk2)):
        def wait_for(part, q):
            remote(
                values.at[HALO, v_rows], e_out.at[part, q, colour],
                e_send.at[part, colour, 0], e_recv.at[part, colour, q], g, q,
            ).wait_recv()

        for j in range(1, MEM):
            q = lax.rem(m + MEM - j, MEM)
            wait_for(0, q)
            copy = remote(
                e_out.at[0, q, colour], e_out.at[1, q, colour],
                fwd_send.at[colour, j], e_recv.at[1, colour, q], g, m - odd,
            )
            sends = jnp.logical_and(odd == 1, q // blocks != m // blocks)
            e_copies.append((copy, sends))

            @pl.when(sends)
            def _():
                copy.start()

    for colour, values in ((0, vr), (1, vk2)):
        for q in range(MEM):
            last = m == MEM - 1
            arrives = jnp.logical_or(
                jnp.logical_and(jnp.logical_not(last), m != q), jnp.logical_and(last, g < groups - 1)
            )

            @pl.when(arrives)
            def _():
                remote(
                    values.at[HALO, v_rows], e_out.at[1, q, colour],
                    e_send.at[1, colour, 0], e_recv.at[1, colour, q], g, q,
                ).wait_recv()
    for copy, sends in e_copies:
        if sends is None:
            copy.wait_send()
        else:
            @pl.when(sends)
            def _():
                copy.wait_send()


def smooth(potential, source, side_faces, end_faces):
    dma = pltpu.SemaphoreType.DMA
    anyspace = pl.BlockSpec(memory_space=pltpu.HBM)
    return pl.pallas_call(
        smooth_kernel,
        out_shape=(
            pltpu.VMEM((2, MEM, 2, ROWS, 128), F32),
            pltpu.VMEM((2, 4, NF + 16, 128), F32),
            pltpu.VMEM((NC, NF), BF16),
            pltpu.VMEM((NC, NC), BF16),
        ),
        in_specs=[anyspace, anyspace, pl.BlockSpec(memory_space=pltpu.VMEM), anyspace],
        out_specs=(pl.BlockSpec(memory_space=pltpu.VMEM),) * 4,
        scratch_shapes=[
            pltpu.VMEM((2, 4, NF + 16, 128), F32),
            pltpu.VMEM((NC, NC), F32),
            pltpu.VMEM((NF, NC), BF16),
            pltpu.VMEM((NF, NC), BF16),
            pltpu.VMEM((NC, NC), BF16),
            pltpu.VMEM((3, MEM, 2, ROWS, 128), F32),
            pltpu.VMEM((MEM, 2, ROWS, 128), F32),
            pltpu.VMEM((MEM, 2, ROWS, 128), F32),
            pltpu.VMEM((SLOTS, 2, FROWS, 128), F32),
            pltpu.VMEM((MEM, 2, ROWS, 128), F32),
            pltpu.VMEM((SLOTS, VROWS, 128), F32),
            pltpu.VMEM((SLOTS, VROWS, 128), F32),
            pltpu.VMEM((SLOTS, VROWS, 128), F32),
            pltpu.VMEM((3, FROWS, 128), F32),
            dma((4, 2)),
            dma,
            dma((CHUNKS,)),
            dma((CHUNKS,)),
            dma((CHUNKS, 2, 2)),
            dma((MEM, 2)),
            dma((CHUNKS, 2, 2)),
            dma((MEM, 2)),
            dma((8,)),
            dma((8,)),
            dma((8,)),
            dma((8,)),
            dma((2, 2, MEM)),
            dma((2, 2, MEM)),
            dma((2, MEM)),
        ],
        compiler_params=pltpu.CompilerParams(collective_id=0, has_side_effects=True),
        name="smooth",
    )(potential, source, side_faces, end_faces)


def prolong_kernel(e, p, w_fine, w_plain, corrected, correction, wide, fine, coarse, sems, coarse_sems):
    groups = lax.axis_size("grp")
    device = lax.axis_index("grp") * MEM + lax.axis_index("mem")
    is_last = device == groups * MEM - 1
    blocks = CROWS // ROWS

    def by_column(part, red, black):
        even = lax.rem(iota(red.shape, 0) + part + device, 2) == 0
        return jnp.concatenate([jnp.where(even, red, black), jnp.where(even, black, red)], axis=1)

    def rows_of(part, c):
        here = [by_column(part, e[part, c * blocks + b, 0], e[part, c * blocks + b, 1]) for b in range(blocks)]
        if c == CHUNKS - 1:
            after = jnp.broadcast_to(here[-1][ROWS - 1 :, :], (8, NC))
        else:
            q = (c + 1) * blocks
            after = by_column(part, e[part, q, 0, 0:8, :], e[part, q, 1, 0:8, :])
        return jnp.concatenate(here + [after], axis=0)

    copies = []
    for c in range(CHUNKS):
        rows = rows_of(0, c)
        above = jnp.where(is_last, rows, 0.5 * (rows + rows_of(1, c)))
        out_rows = pl.ds(FINE * c, FINE)
        for plane, x in enumerate((rows, above)):
            refined = dot_exact(x, w_fine[...])
            for t in range(4):
                wide[plane, t] = refined[:, 128 * t : 128 * t + 128]
                here, after = wide[plane, t, 0:CROWS, :], wide[plane, t, 1 : CROWS + 1, :]
                even, odd = pl.ds(FINE * c, CROWS, stride=2), pl.ds(FINE * c + 1, CROWS, stride=2)
                p_even = p[plane, t, pl.ds(8 + FINE * c, CROWS, stride=2), :]
                p_odd = p[plane, t, pl.ds(9 + FINE * c, CROWS, stride=2), :]
                fine[plane, t, even, :] = p_even + here
                fine[plane, t, odd, :] = p_odd + 0.5 * (here + after)
                copy = pltpu.make_async_copy(
                    fine.at[plane, t, out_rows],
                    corrected.at[plane, out_rows, pl.ds(128 * t, 128)],
                    sems.at[c, plane, t],
                )
                copy.start()
                copies.append(copy)
        out_rows = pl.ds(CROWS * c, CROWS)
        coarse[out_rows, :] = dot_exact(rows[:CROWS], w_plain[...])
        copy = pltpu.make_async_copy(coarse.at[out_rows], correction.at[0, out_rows], coarse_sems.at[c])
        copy.start()
        copies.append(copy)
    for copy in copies:
        copy.wait()


def prolong(*values):
    vmem = pl.BlockSpec(memory_space=pltpu.VMEM)
    anyspace = pl.BlockSpec(memory_space=pl.ANY)
    return pl.pallas_call(
        prolong_kernel,
        out_shape=(
            jax.ShapeDtypeStruct((2, NF, NF), F32),
            jax.ShapeDtypeStruct((1, NC, NC), F32),
        ),
        in_specs=[vmem] * 4,
        out_specs=(anyspace, anyspace),
        scratch_shapes=[
            pltpu.VMEM((2, 4, CROWS + 8, 128), F32),
            pltpu.VMEM((2, 4, NF, 128), F32),
            pltpu.VMEM((NC, NC), F32),
            pltpu.SemaphoreType.DMA((CHUNKS, 2, 4)),
            pltpu.SemaphoreType.DMA((CHUNKS,)),
        ],
        compiler_params=pltpu.CompilerParams(vmem_limit_bytes=24 * 2**20),
        name="prolong",
    )(*(pltpu.with_memory_space_constraint(x, pltpu.VMEM) for x in values))


def per_device(potential, source, side_faces, end_faces):
    return prolong(*smooth(potential, source, side_faces, end_faces))


def solution(mesh):
    placed = P(("grp", "mem"), None, None)
    return jax.shard_map(
        per_device,
        mesh=mesh,
        in_specs=(placed, placed, placed, P()),
        out_specs=(placed, placed),
        check_vma=False,
    )
```

```python
import jax
import jax.numpy as jnp
from jax import lax
from jax.experimental import pallas as pl
from jax.experimental.pallas import tpu as pltpu
from jax.sharding import PartitionSpec as P

F32 = jnp.float32
BF16 = jnp.bfloat16
MESH = pl.DeviceIdType.MESH

NF = 512
NC = 256
MEM = 8
ROWS = NC // MEM
HALO = 8
SLOTS = MEM + 2 * HALO
FROWS = ROWS + 2 * HALO
VROWS = FROWS + 16
CHUNKS = 4
CROWS = NC // CHUNKS
FINE = 2 * CROWS


def iota(shape, dim):
    return lax.broadcasted_iota(jnp.int32, shape, dim)


def split3(x):
    high = x.astype(BF16)
    rest = x - high.astype(F32)
    middle = rest.astype(BF16)
    low = (rest - middle.astype(F32)).astype(BF16)
    return high, middle, low


def dot_exact(x, weights):
    rows = x.shape[0]
    parts = jnp.concatenate(split3(x), axis=0)
    out = jnp.dot(parts, weights, preferred_element_type=F32)
    return out[:rows] + (out[rows : 2 * rows] + out[2 * rows :])


def coarse_column(shape, dim):
    n = iota(shape, dim)
    return jnp.where(n < NC // 2, 2 * n, 2 * n - (NC - 1))


DIRECTIONS = tuple((dg, dm) for dg in (-1, 0, 1) for dm in (-1, 0, 1) if (dg, dm) != (0, 0))


def smooth_kernel(
    p_hbm, s_hbm, side, end_hbm, e_out, pb, w_fine, w_plain,
    sb, eb, w_rc, w_lr, w_perm, fields, partner, summed, fb, xb, vr, vk, vk2, scales,
    in_sems, end_sem, p_send, p_recv, f_send, f_recv, x_send, x_recv, h_send, h_recv, b_send, b_recv,
    e_send, e_recv, fwd_send,
):
    groups = lax.axis_size("grp")
    g = lax.axis_index("grp")
    m = lax.axis_index("mem")
    device = g * MEM + m
    is_first = device == 0
    is_last = device == groups * MEM - 1
    at_end = jnp.logical_or(is_first, is_last)

    def remote(src, dst, send, recv, tg, tm):
        return pltpu.make_async_remote_copy(
            src_ref=src, dst_ref=dst, send_sem=send, recv_sem=recv,
            device_id={"grp": tg, "mem": tm}, device_id_type=MESH,
        )

    in_copies = []
    for t in range(4):
        for a, (src, dst) in enumerate(((p_hbm, pb), (s_hbm, sb))):
            in_copies.append(
                pltpu.make_async_copy(
                    src.at[:, :, pl.ds(128 * t, 128)], dst.at[:, t, pl.ds(8, NF), :], in_sems.at[t, a]
                )
            )
    for copy in in_copies:
        copy.start()
    end_copy = pltpu.make_async_copy(end_hbm.at[jnp.where(is_last, 1, 0)], eb, end_sem)

    @pl.when(at_end)
    def _():
        end_copy.start()

    vk2[...] = jnp.zeros_like(vk2)
    fb[...] = jnp.zeros_like(fb)
    xb[...] = jnp.zeros_like(xb)

    barrier = pltpu.get_barrier_semaphore()
    for dg in (-1, 0, 1):
        exists = jnp.logical_and(g + dg >= 0, g + dg < groups)

        @pl.when(exists)
        def _():
            for i in range(1 if dg == 0 else 0, MEM):
                pl.semaphore_signal(
                    barrier, inc=1,
                    device_id={"grp": g + dg, "mem": lax.rem(m + i, MEM)}, device_id_type=MESH,
                )

    vr[...] = jnp.zeros_like(vr)
    vk[...] = jnp.zeros_like(vk)
    row = m * ROWS - HALO + iota((FROWS, 128), 0)
    inner = jnp.where(jnp.logical_and(row >= 0, row < NC), 1.0 / 6.0, 0.0)
    scales[0] = jnp.where(g > 0, inner, 0.0)
    scales[1] = inner
    scales[2] = jnp.where(g < groups - 1, inner, 0.0)

    zeros = jnp.zeros((2, 4, 8, 128), F32)
    pb[:, :, 0:8, :] = zeros
    pb[:, :, 8 + NF : 16 + NF, :] = zeros
    sb[:, :, 0:8, :] = zeros

    column = coarse_column((NF, NC), 1)
    step = jnp.abs(iota((NF, NC), 0) - 2 * column)
    w_rc[...] = jnp.where(step == 0, 0.5, jnp.where(step == 1, 0.25, 0.0)).astype(BF16)
    near = jnp.where(step == 0, jnp.where(column == 0, 0.25, 0.5), 0.5)
    w_lr[...] = jnp.where(step <= 1, near, jnp.where(step == 2, 0.25, 0.0)).astype(BF16)
    square = coarse_column((NC, NC), 1)
    w_perm[...] = jnp.where(iota((NC, NC), 0) == square, 1.0, 0.0).astype(BF16)

    front = dot_exact(jnp.broadcast_to(side[0, 0:1, :], (8, NC)), w_perm[...])[0:1]
    back = dot_exact(jnp.broadcast_to(side[0, 1:2, :], (8, NC)), w_perm[...])[0:1]
    own_weight = jnp.where(is_first, 0.25, 0.5)
    blocks = CROWS // ROWS

    def by_colour(value, shift):
        even = lax.rem(iota((CROWS, 128), 0) + device + shift, 2) == 0
        left, right = value[:, :128], value[:, 128:]
        return jnp.where(even, left, right), jnp.where(even, right, left)

    def restrict(c, first):
        lists = [[], [], [], [], []]
        row = CROWS * c + iota((CROWS, 128), 0)
        for t in range(4):
            if first:
                for copy in in_copies[2 * t : 2 * t + 2]:
                    copy.wait()

            def load(ref, plane, shift):
                return ref[plane, t, pl.ds(8 + FINE * c + shift, CROWS, stride=2), :]

            a, b = [], []
            for plane in (0, 1):
                p_before, p_here, p_after = (load(pb, plane, k) for k in (-1, 0, 1))
                outer = load(pb, plane, -2) + load(pb, plane, 2)
                odd = p_before + p_after
                s_part = 0.5 * load(sb, plane, 0) + 0.25 * (load(sb, plane, -1) + load(sb, plane, 1))
                value = s_part + (outer - 4.0 * odd - 10.0 * p_here)
                a.append(value - jnp.where(row == 0, p_here, 0.0))
                b.append(2.0 * p_here + odd)
            up = 0.25 * a[1] + 0.5 * b[1]
            lists[0].append(0.5 * a[0] + up + own_weight * b[0])
            lists[1].append(up + 0.25 * b[0])
            lists[2].append(0.25 * b[0])
            lists[3].append(0.5 * b[0] + 0.25 * b[1])
            lists[4].append(0.25 * b[1])
        wide = [jnp.concatenate(f, axis=1) for f in lists]
        plain = dot_exact(jnp.concatenate(wide[:3], axis=0), w_rc[...])
        cross = dot_exact(jnp.concatenate(wide[3:], axis=0), w_lr[...])
        local = plain[:CROWS] + cross[:CROWS]
        above = plain[CROWS : 2 * CROWS] + cross[CROWS:]
        below = plain[2 * CROWS :]
        row = CROWS * c + iota((CROWS, NC), 0)
        lane = iota((CROWS, NC), 1)
        left = jnp.sum(jnp.where(lane == row, side[0, 2:3, :], 0.0), axis=1, keepdims=True)
        right = jnp.sum(jnp.where(lane == row, side[0, 3:4, :], 0.0), axis=1, keepdims=True)
        local = local + jnp.where(lane == 0, left, jnp.where(lane == NC - 1, right, 0.0))
        local = local + jnp.where(row == 0, front, jnp.where(row == NC - 1, back, 0.0))
        for field, value in ((0, local), (1, above), (2, below)):
            for colour, part in enumerate(by_colour(value, int(field > 0))):
                for b in range(blocks):
                    fields[field, c * blocks + b, colour] = part[ROWS * b : ROWS * (b + 1)]

    def add_end_face(c):
        face = dot_exact(eb[pl.ds(pl.multiple_of(CROWS * c, CROWS), CROWS), :], w_perm[...])
        for colour, part in enumerate(by_colour(face, 0)):
            for b in range(blocks):
                q = c * blocks + b
                fields[0, q, colour] = fields[0, q, colour] + part[ROWS * b : ROWS * (b + 1)]

    odd = lax.rem(m, 2)
    x_group = g - jnp.where(m == 0, 1, 0) + jnp.where(m == MEM - 1, 1, 0)
    x_plane = lax.rem(m + jnp.where(odd == 1, 1, MEM - 1), MEM)
    x_field = 2 - odd
    x_valid = jnp.logical_and(x_group >= 0, x_group < groups)
    x_home = x_group == g
    own_rows = pl.ds(HALO, ROWS)
    sent = []

    def send_if(condition, copy):
        sent.append((condition, copy))

        @pl.when(condition)
        def _():
            copy.start()

    def send_x(i, c, colour):
        for b in range(blocks):
            q = c * blocks + b
            home = jnp.logical_and(x_home, q == m)
            send_if(
                jnp.logical_and(x_valid, jnp.logical_not(home)),
                remote(
                    fields.at[x_field, q, colour], xb.at[x_plane, colour],
                    x_send.at[i, b, colour], x_recv.at[x_plane, colour], x_group, q,
                ),
            )

            @pl.when(home)
            def _():
                xb[x_plane, colour] = fields[x_field, q, colour]

    def send_fields(i, c):
        part = pl.ds(c * blocks, blocks)
        copy = remote(
            fields.at[1 + odd, part], partner.at[part], p_send.at[i], p_recv.at[i], g, m + 1 - 2 * odd
        )
        copy.start()
        send_x(i, c, 0)
        return copy

    def send_sums(i, c, to_partner):
        to_partner.wait_recv()
        for b in range(blocks):
            q = c * blocks + b
            summed[q] = fields[0, q] + partner[q]

            @pl.when(q == m)
            def _():
                fb[HALO + m, :, HALO : HALO + ROWS, :] = summed[q]

        for colour in (0, 1):
            if colour == 1:
                send_x(i, c, 1)
            for b in range(blocks):
                q = c * blocks + b
                send_if(
                    q != m,
                    remote(
                        summed.at[q, colour], fb.at[HALO + m, colour, own_rows],
                        f_send.at[i, b, colour], f_recv.at[m, colour], g, q,
                    ),
                )

    @pl.when(at_end)
    def _():
        end_copy.wait()

    order = [lax.rem(m // blocks + k, CHUNKS) for k in (1, 3, 0, 2)]
    partners = []
    for i, c in enumerate(order):
        restrict(c, i == 0)

        @pl.when(at_end)
        def _():
            add_end_face(c)

        if i == 0:
            count = (MEM - 1) + jnp.where(g > 0, MEM, 0) + jnp.where(g < groups - 1, MEM, 0)
            pl.semaphore_wait(barrier, count)
        partners.append(send_fields(i, c))
        if i > 0:
            send_sums(i - 1, order[i - 1], partners[i - 1])
    send_sums(CHUNKS - 1, order[-1], partners[-1])

    def inside(dg, dm):
        ok = None
        for test in (
            (g + dg >= 0) if dg < 0 else (g + dg < groups) if dg > 0 else None,
            (m + dm >= 0) if dm < 0 else (m + dm < MEM) if dm > 0 else None,
        ):
            if test is not None:
                ok = test if ok is None else jnp.logical_and(ok, test)
        return ok

    def exchange(make):
        copies = []
        for o, (dg, dm) in enumerate(DIRECTIONS):
            copy = make(o, dg, dm)
            copies.append(copy)

            @pl.when(inside(dg, dm))
            def _():
                copy.start()
        return copies

    def arrive(copies):
        for o, (dg, dm) in enumerate(DIRECTIONS):
            @pl.when(inside(-dg, -dm))
            def _():
                copies[o].wait_recv()

    def row_parts(dm, base):
        if dm < 0:
            return pl.ds(base, HALO), pl.ds(base + ROWS, HALO)
        if dm > 0:
            return pl.ds(base + ROWS - HALO, HALO), pl.ds(base - HALO, HALO)
        return pl.ds(base, ROWS), pl.ds(base, ROWS)

    def plane_parts(dg, depth):
        if dg < 0:
            return pl.ds(HALO, depth), pl.ds(HALO + MEM, depth)
        if dg > 0:
            return pl.ds(HALO + MEM - depth, depth), pl.ds(HALO - depth, depth)
        return pl.ds(HALO, MEM), pl.ds(HALO, MEM)

    def forcing_copy(o, dg, dm, k=None, colour=0):
        src_rows, dst_rows = row_parts(dm, HALO)
        if k is None:
            src, dst = plane_parts(dg, HALO - 1 - abs(dm))
            colour = slice(None)
        else:
            src, dst = HALO + k, HALO + k - MEM * dg
        return remote(
            fb.at[src, colour, src_rows], fb.at[dst, colour, dst_rows], h_send.at[o], h_recv.at[o], g + dg, m + dm
        )

    def receive(n, carry):
        colour = lax.rem(n // 4, 2)
        item = n // 8 * 4 + lax.rem(n, 4)
        offset = jnp.where(item < 4, item - 1, jnp.where(item == 4, -2, item - 2))
        k = lax.rem(m // blocks * blocks + offset + MEM, MEM)

        @pl.when(m != k)
        def _():
            remote(
                summed.at[0, 0], fb.at[HALO + k, colour, own_rows],
                f_send.at[0, 0, 0], f_recv.at[k, colour], g, k,
            ).wait_recv()

        arrives = jnp.logical_not(jnp.logical_and(x_home, x_plane == k))
        arrives = jnp.logical_and(arrives, jnp.logical_or(k > 0, g > 0))
        arrives = jnp.logical_and(arrives, jnp.logical_or(k < MEM - 1, g < groups - 1))

        @pl.when(arrives)
        def _():
            remote(
                fields.at[0, 0, 0], xb.at[k, colour], x_send.at[0, 0, 0], x_recv.at[k, colour], g, k
            ).wait_recv()

        fb[HALO + k, colour, HALO : HALO + ROWS, :] = fb[HALO + k, colour, HALO : HALO + ROWS, :] + xb[k, colour]
        for o, (dg, dm) in enumerate(DIRECTIONS):
            depth = HALO - 1 - abs(dm)
            needed = inside(dg, dm)
            if dg < 0:
                needed = jnp.logical_and(needed, k < depth)
            if dg > 0:
                needed = jnp.logical_and(needed, k >= MEM - depth)

            @pl.when(needed)
            def _():
                forcing_copy(o, dg, dm, k, colour).start()
        return carry

    def black_copy(o, dg, dm):
        src_rows, dst_rows = row_parts(dm, HALO + 8)
        src_planes, dst_planes = plane_parts(dg, HALO - abs(dm))
        return remote(
            vk2.at[src_planes, src_rows], vk2.at[dst_planes, dst_rows],
            b_send.at[o], b_recv.at[o], g + dg, m + dm,
        )

    lax.fori_loop(0, 2 * MEM, receive, 0)
    column = coarse_column((NC, NF), 0)
    step = iota((NC, NF), 1) - 2 * column
    whole = jnp.logical_or(step == 0, jnp.logical_and(step == 1, column == NC - 1))
    half = jnp.abs(step) == 1
    w_fine[...] = jnp.where(whole, 1.0, jnp.where(half, 0.5, 0.0)).astype(BF16)
    w_plain[...] = jnp.where(iota((NC, NC), 1) == coarse_column((NC, NC), 0), 1.0, 0.0).astype(BF16)

    h_copies = [forcing_copy(o, dg, dm) for o, (dg, dm) in enumerate(DIRECTIONS)]
    arrive(h_copies)

    lane = iota((8, 128), 1)
    row_parity = lax.rem(iota((8, 128), 0), 2)
    from_left = [
        (jnp.logical_and(row_parity == flip, lane != 0), jnp.logical_and(row_parity != flip, lane != 127))
        for flip in (0, 1)
    ]

    def half_sweep(colour, t, target, source, first=0, tiles=FROWS // 8):
        at, n = 8 + 8 * first, 8 * tiles
        shape = (tiles, 8, 128)
        for slot in range(t, SLOTS - t):
            centre = source[slot, at : at + n, :].reshape(shape)
            keep_left, keep_right = from_left[(slot + colour) % 2]
            beside = jnp.where(
                jnp.broadcast_to(keep_left, shape), pltpu.roll(centre, 1, 2),
                jnp.where(jnp.broadcast_to(keep_right, shape), pltpu.roll(centre, 127, 2), 0.0),
            )
            rows = source[slot, at - 1 : at - 1 + n, :] + source[slot, at + 1 : at + 1 + n, :]
            depth = source[slot - 1, at : at + n, :] + source[slot + 1, at : at + n, :]
            side = 0 if slot < HALO else 2 if slot >= HALO + MEM else 1
            near = (depth + rows).reshape(shape) + (centre + beside)
            total = fb[slot, colour, 8 * first : 8 * first + n, :].reshape(shape) + near
            total = total * scales[side, 8 * first : 8 * first + n, :].reshape(shape)
            target[slot, at : at + n, :] = total.reshape(n, 128)

    def sweeps(black):
        for t in (1, 3, 5):
            half_sweep(0, t, vr, black)
            half_sweep(1, t + 1, black, vr)
        half_sweep(0, 7, vr, black)

    sweeps(vk)
    half_sweep(1, 8, vk2, vr, 1, ROWS // 8)
    b_copies = exchange(black_copy)
    arrive(b_copies)
    for o, (dg, dm) in enumerate(DIRECTIONS):
        @pl.when(inside(dg, dm))
        def _():
            b_copies[o].wait_send()
    sweeps(vk2)

    v_rows = pl.ds(HALO + 8, ROWS)
    e_copies = []

    def send_back(colour, values):
        e_out[0, m, colour] = values[HALO + m, HALO + 8 : HALO + 8 + ROWS, :]
        for i in range(1, MEM):
            tm = lax.rem(m + i, MEM)
            copy = remote(
                values.at[HALO + tm, v_rows], e_out.at[0, m, colour],
                e_send.at[0, colour, i], e_recv.at[0, colour, m], g, tm,
            )
            copy.start()
            e_copies.append((copy, None))
        for i in range(MEM):
            tm = lax.rem(m + i, MEM)
            wraps = tm == MEM - 1
            plane = HALO + jnp.where(wraps, 0, tm + 1)
            tg = g - jnp.where(wraps, 1, 0)
            copy = remote(
                values.at[plane, v_rows], e_out.at[1, m, colour],
                e_send.at[1, colour, i], e_recv.at[1, colour, m], tg, tm,
            )
            if i == 0:
                sends = jnp.logical_and(wraps, g > 0)

                @pl.when(jnp.logical_not(wraps))
                def _():
                    e_out[1, m, colour] = values[plane, HALO + 8 : HALO + 8 + ROWS, :]
            else:
                direct = jnp.logical_or(lax.rem(tm, 2) == 1, tm // blocks == m // blocks)
                sends = jnp.logical_and(direct, jnp.logical_not(jnp.logical_and(wraps, g == 0)))
            e_copies.append((copy, sends))

            @pl.when(sends)
            def _():
                copy.start()

    send_back(0, vr)
    half_sweep(1, 8, vk2, vr, 1, ROWS // 8)
    send_back(1, vk2)

    for copy in partners:
        copy.wait_send()
    for condition, copy in sent:
        @pl.when(condition)
        def _():
            copy.wait_send()
    for o, (dg, dm) in enumerate(DIRECTIONS):
        @pl.when(inside(dg, dm))
        def _():
            h_copies[o].wait_send()
    for colour, values in ((0, vr), (1, vk2)):
        def wait_for(part, q):
            remote(
                values.at[HALO, v_rows], e_out.at[part, q, colour],
                e_send.at[part, colour, 0], e_recv.at[part, colour, q], g, q,
            ).wait_recv()

        for j in range(1, MEM):
            q = lax.rem(m + MEM - j, MEM)
            wait_for(0, q)
            copy = remote(
                e_out.at[0, q, colour], e_out.at[1, q, colour],
                fwd_send.at[colour, j], e_recv.at[1, colour, q], g, m - odd,
            )
            sends = jnp.logical_and(odd == 1, q // blocks != m // blocks)
            e_copies.append((copy, sends))

            @pl.when(sends)
            def _():
                copy.start()

    for colour, values in ((0, vr), (1, vk2)):
        for q in range(MEM):
            last = m == MEM - 1
            arrives = jnp.logical_or(
                jnp.logical_and(jnp.logical_not(last), m != q), jnp.logical_and(last, g < groups - 1)
            )

            @pl.when(arrives)
            def _():
                remote(
                    values.at[HALO, v_rows], e_out.at[1, q, colour],
                    e_send.at[1, colour, 0], e_recv.at[1, colour, q], g, q,
                ).wait_recv()
    for copy, sends in e_copies:
        if sends is None:
            copy.wait_send()
        else:
            @pl.when(sends)
            def _():
                copy.wait_send()


def smooth(potential, source, side_faces, end_faces):
    dma = pltpu.SemaphoreType.DMA
    anyspace = pl.BlockSpec(memory_space=pltpu.HBM)
    return pl.pallas_call(
        smooth_kernel,
        out_shape=(
            pltpu.VMEM((2, MEM, 2, ROWS, 128), F32),
            pltpu.VMEM((2, 4, NF + 16, 128), F32),
            pltpu.VMEM((NC, NF), BF16),
            pltpu.VMEM((NC, NC), BF16),
        ),
        in_specs=[anyspace, anyspace, pl.BlockSpec(memory_space=pltpu.VMEM), anyspace],
        out_specs=(pl.BlockSpec(memory_space=pltpu.VMEM),) * 4,
        scratch_shapes=[
            pltpu.VMEM((2, 4, NF + 16, 128), F32),
            pltpu.VMEM((NC, NC), F32),
            pltpu.VMEM((NF, NC), BF16),
            pltpu.VMEM((NF, NC), BF16),
            pltpu.VMEM((NC, NC), BF16),
            pltpu.VMEM((3, MEM, 2, ROWS, 128), F32),
            pltpu.VMEM((MEM, 2, ROWS, 128), F32),
            pltpu.VMEM((MEM, 2, ROWS, 128), F32),
            pltpu.VMEM((SLOTS, 2, FROWS, 128), F32),
            pltpu.VMEM((MEM, 2, ROWS, 128), F32),
            pltpu.VMEM((SLOTS, VROWS, 128), F32),
            pltpu.VMEM((SLOTS, VROWS, 128), F32),
            pltpu.VMEM((SLOTS, VROWS, 128), F32),
            pltpu.VMEM((3, FROWS, 128), F32),
            dma((4, 2)),
            dma,
            dma((CHUNKS,)),
            dma((CHUNKS,)),
            dma((CHUNKS, 2, 2)),
            dma((MEM, 2)),
            dma((CHUNKS, 2, 2)),
            dma((MEM, 2)),
            dma((8,)),
            dma((8,)),
            dma((8,)),
            dma((8,)),
            dma((2, 2, MEM)),
            dma((2, 2, MEM)),
            dma((2, MEM)),
        ],
        compiler_params=pltpu.CompilerParams(collective_id=0, has_side_effects=True),
        name="smooth",
    )(potential, source, side_faces, end_faces)


def prolong_kernel(e, p, w_fine, w_plain, corrected, correction, wide, fine, coarse, sems, coarse_sems):
    groups = lax.axis_size("grp")
    device = lax.axis_index("grp") * MEM + lax.axis_index("mem")
    is_last = device == groups * MEM - 1
    blocks = CROWS // ROWS

    def by_column(part, red, black):
        even = lax.rem(iota(red.shape, 0) + part + device, 2) == 0
        return jnp.concatenate([jnp.where(even, red, black), jnp.where(even, black, red)], axis=1)

    def rows_of(part, c):
        here = [by_column(part, e[part, c * blocks + b, 0], e[part, c * blocks + b, 1]) for b in range(blocks)]
        if c == CHUNKS - 1:
            after = jnp.broadcast_to(here[-1][ROWS - 1 :, :], (8, NC))
        else:
            q = (c + 1) * blocks
            after = by_column(part, e[part, q, 0, 0:8, :], e[part, q, 1, 0:8, :])
        return jnp.concatenate(here + [after], axis=0)

    copies = []
    for c in range(CHUNKS):
        rows = rows_of(0, c)
        above = jnp.where(is_last, rows, 0.5 * (rows + rows_of(1, c)))
        out_rows = pl.ds(FINE * c, FINE)
        for plane, x in enumerate((rows, above)):
            refined = dot_exact(x, w_fine[...])
            for t in range(4):
                wide[plane, t] = refined[:, 128 * t : 128 * t + 128]
                here, after = wide[plane, t, 0:CROWS, :], wide[plane, t, 1 : CROWS + 1, :]
                even, odd = pl.ds(FINE * c, CROWS, stride=2), pl.ds(FINE * c + 1, CROWS, stride=2)
                p_even = p[plane, t, pl.ds(8 + FINE * c, CROWS, stride=2), :]
                p_odd = p[plane, t, pl.ds(9 + FINE * c, CROWS, stride=2), :]
                fine[plane, t, even, :] = p_even + here
                fine[plane, t, odd, :] = p_odd + 0.5 * (here + after)
                copy = pltpu.make_async_copy(
                    fine.at[plane, t, out_rows],
                    corrected.at[plane, out_rows, pl.ds(128 * t, 128)],
                    sems.at[c, plane, t],
                )
                copy.start()
                copies.append(copy)
        out_rows = pl.ds(CROWS * c, CROWS)
        coarse[out_rows, :] = dot_exact(rows[:CROWS], w_plain[...])
        copy = pltpu.make_async_copy(coarse.at[out_rows], correction.at[0, out_rows], coarse_sems.at[c])
        copy.start()
        copies.append(copy)
    for copy in copies:
        copy.wait()


def prolong(*values):
    vmem = pl.BlockSpec(memory_space=pltpu.VMEM)
    anyspace = pl.BlockSpec(memory_space=pl.ANY)
    return pl.pallas_call(
        prolong_kernel,
        out_shape=(
            jax.ShapeDtypeStruct((2, NF, NF), F32),
            jax.ShapeDtypeStruct((1, NC, NC), F32),
        ),
        in_specs=[vmem] * 4,
        out_specs=(anyspace, anyspace),
        scratch_shapes=[
            pltpu.VMEM((2, 4, CROWS + 8, 128), F32),
            pltpu.VMEM((2, 4, NF + 16, 128), F32),
            pltpu.VMEM((NC, NC), F32),
            pltpu.SemaphoreType.DMA((CHUNKS, 2, 4)),
            pltpu.SemaphoreType.DMA((CHUNKS,)),
        ],
        compiler_params=pltpu.CompilerParams(vmem_limit_bytes=24 * 2**20),
        name="prolong",
    )(*(pltpu.with_memory_space_constraint(x, pltpu.VMEM) for x in values))


def per_device(potential, source, side_faces, end_faces):
    return prolong(*smooth(potential, source, side_faces, end_faces))


def solution(mesh):
    placed = P(("grp", "mem"), None, None)
    return jax.shard_map(
        per_device,
        mesh=mesh,
        in_specs=(placed, placed, placed, P()),
        out_specs=(placed, placed),
        check_vma=False,
    )
```
